64 devices in a mesh: data: 4 (over x, y), model: 16 (over z, core).
Axes of the slice: x: 2, y: 2, z: 8, core: 2. Of those that a mesh axis runs over, the one named last changes fastest.
The devices are a block of a 4x4x8 slice.
Arguments:
- x_in: bfloat16 [16384, 2048], P(('data', 'model')), parts along dimension 0
- dy_in: bfloat16 [16384, 2048], P(('data', 'model')), parts along dimension 0
- w_query: bfloat16 [2048, 16, 128], P(None, 'model')
- w_key: bfloat16 [2048, 128], replicated
- w_value: bfloat16 [2048, 128], replicated
- w_out: bfloat16 [16, 128, 2048], P('model')
Outputs:
- output 1: bfloat16 [16384, 2048], P(('data', 'model')), parts along dimension 0
- output 2: float32 [8192, 16, 128], P('data', 'model'), parts along dimension 0
- output 3: float32 [8192, 128], P(('data', 'model')), parts along dimension 0
- output 4: float32 [8192, 128], P(('data', 'model')), parts along dimension 0
- output 5: float32 [64, 128, 2048], P(('data', 'model')), parts along dimension 0
There are 4 independent parts. The reference program is written for one: setup_inputs(seed, part) draws one part's arguments, and reference() takes and returns one part's arrays. A program takes and returns all parts, laid end to end along the dimension named above; an argument that names none is the same for every part.
All inputs are finite; a program needn't handle non-finite values.
Results may differ from the reference program's by a relative error of at most 0.00907.
Values are sent between devices in bfloat16 or wider.
A program may use at most 768 MiB of HBM per device.

```python
import math
import jax
import jax.numpy as jnp
from jax import lax

SEQ_LEN = 4096
D_MODEL = 2048
NUM_HEADS = 16
HEAD_DIM = 128


def setup_inputs(seed: int = 0, part: int = 0) -> dict:
    part_key = jax.random.fold_in(jax.random.key(seed), part)
    act_keys = jax.random.split(part_key, 2)
    weight_keys = jax.random.split(jax.random.key(seed + 1), 4)
    in_scale = D_MODEL ** -0.5
    x_in = jax.random.normal(act_keys[0], (SEQ_LEN, D_MODEL), jnp.float32).astype(jnp.bfloat16)
    dy_in = jax.random.normal(act_keys[1], (SEQ_LEN, D_MODEL), jnp.float32).astype(jnp.bfloat16)
    w_query = (jax.random.normal(weight_keys[0], (D_MODEL, NUM_HEADS, HEAD_DIM), jnp.float32) * in_scale).astype(jnp.bfloat16)
    w_key = (jax.random.normal(weight_keys[1], (D_MODEL, HEAD_DIM), jnp.float32) * in_scale).astype(jnp.bfloat16)
    w_value = (jax.random.normal(weight_keys[2], (D_MODEL, HEAD_DIM), jnp.float32) * in_scale).astype(jnp.bfloat16)
    w_out = (jax.random.normal(weight_keys[3], (NUM_HEADS, HEAD_DIM, D_MODEL), jnp.float32) * in_scale).astype(jnp.bfloat16)
    return {"x_in": x_in, "dy_in": dy_in, "w_query": w_query, "w_key": w_key, "w_value": w_value, "w_out": w_out}


def reference(x_in, dy_in, w_query, w_key, w_value, w_out):
    score_scale = 1.0 / math.sqrt(HEAD_DIM)
    keys_all = jnp.dot(x_in, w_key, preferred_element_type=jnp.float32).astype(jnp.bfloat16)
    values_all = jnp.dot(x_in, w_value, preferred_element_type=jnp.float32).astype(jnp.bfloat16)
    causal = jnp.arange(SEQ_LEN)[:, None] >= jnp.arange(SEQ_LEN)[None, :]

    def head_step(carry_in, head_weights):
        dk_sum, dv_sum, dx_sum = carry_in
        wq_head, wo_head = head_weights
        query_rows = jnp.dot(x_in, wq_head, preferred_element_type=jnp.float32).astype(jnp.bfloat16)
        scores = jnp.dot(query_rows, keys_all.T, preferred_element_type=jnp.float32) * score_scale
        scores = jnp.where(causal, scores, -jnp.inf)
        probs_f32 = jax.nn.softmax(scores, axis=-1)
        probs_bf = probs_f32.astype(jnp.bfloat16)
        attn_rows = jnp.dot(probs_bf, values_all, preferred_element_type=jnp.float32).astype(jnp.bfloat16)
        dw_out_head = jnp.dot(attn_rows.T, dy_in, preferred_element_type=jnp.float32)
        d_attn = jnp.dot(dy_in, wo_head.T, preferred_element_type=jnp.float32).astype(jnp.bfloat16)
        d_probs = jnp.dot(d_attn, values_all.T, preferred_element_type=jnp.float32)
        row_dot = jnp.sum(d_attn.astype(jnp.float32) * attn_rows.astype(jnp.float32), axis=-1, keepdims=True)
        d_scores = (probs_f32 * (d_probs - row_dot) * score_scale).astype(jnp.bfloat16)
        d_query = jnp.dot(d_scores, keys_all, preferred_element_type=jnp.float32).astype(jnp.bfloat16)
        d_keys_part = jnp.dot(d_scores.T, query_rows, preferred_element_type=jnp.float32)
        d_values_part = jnp.dot(probs_bf.T, d_attn, preferred_element_type=jnp.float32)
        dw_query_head = jnp.dot(x_in.T, d_query, preferred_element_type=jnp.float32)
        dx_part = jnp.dot(d_query, wq_head.T, preferred_element_type=jnp.float32)
        carry_out = (dk_sum + d_keys_part, dv_sum + d_values_part, dx_sum + dx_part)
        return carry_out, (dw_query_head, dw_out_head)

    carry_init = (jnp.zeros((SEQ_LEN, HEAD_DIM), jnp.float32), jnp.zeros((SEQ_LEN, HEAD_DIM), jnp.float32), jnp.zeros((SEQ_LEN, D_MODEL), jnp.float32))
    wq_heads = jnp.transpose(w_query, (1, 0, 2))
    sums_out, grads_out = lax.scan(head_step, carry_init, (wq_heads, w_out))
    dk_sum, dv_sum, dx_sum = sums_out
    dwq_heads, dw_out = grads_out
    d_keys = dk_sum.astype(jnp.bfloat16)
    d_values = dv_sum.astype(jnp.bfloat16)
    dw_key = jnp.dot(x_in.T, d_keys, preferred_element_type=jnp.float32)
    dw_value = jnp.dot(x_in.T, d_values, preferred_element_type=jnp.float32)
    dx_total = dx_sum + jnp.dot(d_keys, w_key.T, preferred_element_type=jnp.float32) + jnp.dot(d_values, w_value.T, preferred_element_type=jnp.float32)
    dx_out = dx_total.astype(jnp.bfloat16)
    dw_query = jnp.transpose(dwq_heads, (1, 0, 2))
    return (dx_out, dw_query, dw_key, dw_value, dw_out)
```

```python
import math

import jax
import jax.numpy as jnp
from jax import lax
from jax.experimental import pallas as pl
from jax.experimental.pallas import tpu as pltpu
from jax.sharding import PartitionSpec as P

BF16 = jnp.bfloat16
F32 = jnp.float32
MESH = pl.DeviceIdType.MESH
RX, RY, RW, RG = range(4)


def dot(a, b):
    return jnp.dot(a, b, preferred_element_type=F32)


def dot_nt(a, b):
    return lax.dot_general(a, b, (((1,), (1,)), ((), ())), preferred_element_type=F32)


def dot_tn(a, b):
    return lax.dot_general(a, b, (((0,), (0,)), ((), ())), preferred_element_type=F32)


def rowfold(x, op):
    y = x.reshape(x.shape[0] // 8, 8, x.shape[1])
    return jnp.max(y, axis=0) if op == "max" else jnp.sum(y, axis=0)


def make_kernel(n):
    chips = n // 2
    hops = chips // 2
    last = 2 * (hops - 1)
    arrivals = last + 1

    def kernel(
        x_hbm, dy_hbm, wq_hbm, wk_hbm, wv_hbm, wo_hbm,
        dx_hbm, dwq_hbm, dwk_hbm, dwv_hbm, dwo_hbm, wq_all,
        x_all, dy_all, q_all, k_all, v_all, kt_all, vt_all, wqkv, wo,
        dkv, part, sums, gkv, dq_out, dq_in, dwqt, dwo_acc, st, wq_st,
        ot, dqt, dot_s, qt_s, do_s, dwkv, dwq_st,
        ring_r, ring_s, pair_r, pair_s, dq_r, dq_s, px_r, px_s, rs_r, rs_s, loc,
    ):
        rows, width = x_hbm.shape
        dim = wk_hbm.shape[1]
        cols = width // n
        tiles = width // rows
        scale = 1.0 / math.sqrt(dim)
        m = lax.axis_index("model")
        c = lax.div(m, 2)
        k = lax.rem(m, 2)
        mate = m + 1 - 2 * k
        nbr = (lax.rem(m + 2, n), lax.rem(m + n - 2, n))

        def remote(src, dst, ssem, rsem, dev):
            return pltpu.make_async_remote_copy(
                src_ref=src, dst_ref=dst, send_sem=ssem, recv_sem=rsem,
                device_id={"model": dev}, device_id_type=MESH,
            )

        bufs = (x_all, dy_all, wq_all, gkv)
        owns = (x_hbm, dy_hbm, wq_hbm, None)

        def half(ref, h):
            size = ref.shape[0] // 2
            return ref.at[pl.ds(pl.multiple_of(h * size, size), size), :]

        def start_own(r):
            own = gkv.at[m] if owns[r] is None else owns[r]
            for p in (0, 1):
                for d in (0, 1):
                    h = p if d == 0 else 1 - p
                    remote(half(own, h), half(bufs[r].at[m], h), ring_s.at[r, d, p], ring_r.at[r, d, p], nbr[d]).start()
            for h in (0, 1):
                remote(half(own, h), half(bufs[r].at[m], h), pair_s.at[r, h], pair_r.at[r, h], mate).start()

        def service(r, a):
            step = lax.div(a, 2) + 1
            p = lax.rem(a, 2)
            for d in (0, 1):
                blk = lax.rem(m + (n - 2 * step if d == 0 else 2 * step), n)
                chunk = half(bufs[r].at[blk], p if d == 0 else 1 - p)
                remote(chunk, chunk, ring_s.at[r, d, 0], ring_r.at[r, d, a], nbr[d]).wait_recv()

                @pl.when(a <= last - 2)
                def _():
                    remote(chunk, chunk, ring_s.at[r, d, 2 + a], ring_r.at[r, d, a + 2], nbr[d]).start()

                i = 2 + d * arrivals + a
                remote(chunk, chunk, pair_s.at[r, i], pair_r.at[r, i], mate).start()

        def chip_at(u):
            step = lax.div(u + 1, 2)
            odd = lax.rem(u, 2)
            return lax.rem(c + odd * (chips - step) + (1 - odd) * step, chips)

        def wait_pair(r, u):
            blk = bufs[r].at[2 * chip_at(u) + 1 - k]

            def wait(h, i):
                chunk = half(blk, h)
                remote(chunk, chunk, pair_s.at[r, 0], pair_r.at[r, i], mate).wait_recv()

            @pl.when(u == 0)
            def _():
                wait(0, 0)
                wait(1, 1)

            @pl.when(u > 0)
            def _():
                d = 1 - lax.rem(u, 2)
                i = 2 + d * arrivals + 2 * (lax.div(u + 1, 2) - 1)
                wait(d, i)
                wait(1 - d, i + 1 + lax.div(u, chips - 1) * last)

        def wait_sends(r):
            own = gkv.at[m] if owns[r] is None else owns[r]
            chunk = half(own, 0)
            for d in (0, 1):
                for i in range(last + 1):
                    remote(chunk, chunk, ring_s.at[r, d, i], ring_r.at[r, d, 0], nbr[d]).wait_send()
            for i in range(2 + 2 * arrivals):
                remote(chunk, chunk, pair_s.at[r, i], pair_r.at[r, 0], mate).wait_send()

        def local(src, dst, i):
            return pltpu.make_async_copy(src, dst, loc.at[i])

        loads = [
            local(x_hbm, x_all.at[m], 0),
            local(wq_hbm, wqkv.at[:, pl.ds(0, dim)], 1),
            local(wk_hbm, wqkv.at[:, pl.ds(dim, dim)], 2),
            local(wv_hbm, wqkv.at[:, pl.ds(2 * dim, dim)], 3),
            local(wo_hbm, wo, 4),
            local(dy_hbm, dy_all.at[m], 5),
        ]
        for load in loads:
            load.start()
        barrier = pltpu.get_barrier_semaphore()
        for i in range(1, n):
            pl.semaphore_signal(barrier, inc=1, device_id={"model": lax.rem(m + i, n)}, device_id_type=MESH)
        pl.semaphore_wait(barrier, n - 1)
        start_own(RX)
        dwqt[...] = jnp.zeros_like(dwqt)
        dwo_acc[...] = jnp.zeros_like(dwo_acc)
        dwkv[...] = jnp.zeros_like(dwkv)

        def clear(j, _):
            dkv[j] = jnp.zeros(dkv.shape[1:], F32)
            return 0

        lax.fori_loop(0, n, clear, 0)
        for load in loads:
            load.wait()

        def project(blk):
            qkv = dot(x_all[blk], wqkv[...]).astype(BF16)
            q_all[blk] = qkv[:, :dim]
            k_all[blk] = qkv[:, dim : 2 * dim]
            v_all[blk] = qkv[:, 2 * dim :]
            kt_all[blk] = qkv[:, dim : 2 * dim].T
            vt_all[blk] = qkv[:, 2 * dim :].T

        def steps(r, follow, work, extra=None):
            def body(v, _):
                u = lax.div(v, 2)
                kk = lax.rem(v, 2)

                @pl.when(v == 2)
                def _():
                    service(r, 0)

                @pl.when((kk == 0) & (u >= 1) & (u <= last))
                def _():
                    service(r, u)

                @pl.when(v == 2 * (last - 2))
                def _():
                    start_own(follow)

                @pl.when(kk == 1)
                def _():
                    wait_pair(r, u)

                if extra is not None:
                    extra(v)
                work(2 * chip_at(u) + lax.rem(k + kk, 2))
                return 0

            lax.fori_loop(0, n, body, 0)

        steps(RX, RY, project)

        def attend(blk):
            q = q_all[blk]
            do = dot_nt(dy_all[blk], wo[...]).astype(BF16)
            do_s[...] = do
            dot_s[...] = do.T
            qt_s[...] = q.T

            def scores(j, top):
                s = dot(k_all[j], qt_s[...])
                st[j] = s
                return jnp.maximum(top, rowfold(s, "max"))

            top = lax.fori_loop(0, blk, scores, jnp.full((8, rows), -jnp.inf, F32))
            s = dot(k_all[blk], qt_s[...])
            key = lax.broadcasted_iota(jnp.int32, (rows, rows), 0)
            query = lax.broadcasted_iota(jnp.int32, (rows, rows), 1)
            s = jnp.where(key <= query, s, -jnp.inf)
            st[blk] = s
            top = jnp.max(jnp.maximum(top, rowfold(s, "max")), axis=0, keepdims=True)
            factor = scale * math.log2(math.e)

            def weights(j, total):
                p = jnp.exp2((st[j] - top) * factor)
                st[j] = p
                return total + rowfold(p, "sum")

            total = lax.fori_loop(0, blk + 1, weights, jnp.zeros((8, rows), F32))
            inv = 1.0 / jnp.sum(total, axis=0, keepdims=True)
            ot[...] = jnp.zeros_like(ot)
            dqt[...] = jnp.zeros_like(dqt)

            def outputs(j, _):
                p = (st[j] * inv).astype(BF16)
                ot[...] += dot(vt_all[j], p)
                dkv[j, 1] += dot(p, do_s[...])
                return 0

            lax.fori_loop(0, blk + 1, outputs, 0)
            o = ot[...].astype(BF16)
            row = jnp.sum(dot_s[...].astype(F32) * o.astype(F32), axis=0, keepdims=True)

            def grads(j, _):
                dp = dot(v_all[j], dot_s[...])
                g = ((st[j] * inv) * (dp - row) * scale).astype(BF16)
                dqt[...] += dot(kt_all[j], g)
                dkv[j, 0] += dot(g, q_all[blk])
                return 0

            lax.fori_loop(0, blk + 1, grads, 0)
            dq = dqt[...].astype(BF16)
            dq_out[blk] = dq.T

            @pl.when(blk != m)
            def _():
                remote(dq_out.at[blk], dq_in.at[m], dq_s.at[blk], dq_r.at[m], blk).start()

            for t in range(tiles):
                at = pl.ds(t * rows, rows)
                dwqt[:, at] += dot(dq, x_all[blk, :, at])
                dwo_acc[:, at] += dot(o, dy_all[blk, :, at])

        def extra(v):
            @pl.when(v == n - 2)
            def _():
                service(RW, 0)

            @pl.when(v == n - 1)
            def _():
                service(RW, 1)

        steps(RY, RW, attend, extra)

        order = [hops]
        for step in range(hops - 1, 0, -1):
            order += [step, -step]
        order.append(0)

        def chip_off(off):
            return lax.rem(c + off + chips, chips)

        def px(i):
            chip = chip_off(order[i])
            return remote(dkv.at[2 * chip + 1 - k], part.at[chip], px_s.at[i], px_r.at[i], mate)

        for i in range(chips):
            px(i).start()
        dwo_out = local(dwo_acc, dwo_hbm, 0)
        dwo_out.start()
        for t in range(tiles):
            at = pl.ds(t * rows, rows)
            dwq_st[at, :] = dwqt[:, at].T
            st[t] = jnp.zeros((rows, rows), F32)
        dwq_out = local(dwq_st, dwq_hbm, 1)
        dwq_out.start()

        def add_dx(dq, w_ref):
            for t in range(tiles):
                st[t] += dot_nt(dq, w_ref[pl.ds(t * rows, rows), :])

        def dx_heads(lo, hi):
            def body(v, _):
                u = lax.div(v, 2)
                kk = lax.rem(v, 2)
                h = 2 * chip_at(u) + lax.rem(k + kk, 2)

                @pl.when(kk == 1)
                def _():
                    wait_pair(RW, u)

                fetch = local(wq_all.at[h], wq_st.at[0], 2)
                fetch.start()
                remote(dq_in.at[h], dq_in.at[h], dq_s.at[h], dq_r.at[h], mate).wait_recv()
                fetch.wait()
                add_dx(dq_in[h], wq_st.at[0])
                return 0

            lax.fori_loop(lo, hi, body, 0)

        def gather(i):
            px(i).wait_recv()
            chip = chip_off(order[i])
            part[chip] += dkv[2 * chip + k]

        def rs(d, t, h, src):
            return remote(src, sums.at[d, t - 1, h], rs_s.at[d, t - 1, h], rs_r.at[d, t - 1, h], nbr[d])

        sent = []

        def hop(t):
            for d in (0, 1):
                chip = chip_off((hops + 1 - t) * (1 - 2 * d))
                for h in (d, 1 - d):
                    if t == 1 and h != d:
                        continue
                    if t == 1 or (t == 2 and h != d):
                        copy = rs(d, t, h, part.at[chip, h])
                    else:
                        held = sums.at[d, t - 2, h]
                        rs(d, t - 1, h, held).wait_recv()
                        held[...] += part[chip, h]
                        copy = rs(d, t, h, held)
                    copy.start()
                    sent.append(copy)

        service(RW, 2)
        gather(0)
        hop(1)
        service(RW, 3)
        gather(1)
        gather(2)
        hop(2)
        add_dx(dq_out[m], wqkv.at[:, pl.ds(0, dim)])
        dx_heads(1, 2)
        for i in range(3, chips):
            gather(i)
        done = 2
        for t in range(3, hops + 1):
            hop(t)
            service(RW, t + 1)
            dx_heads(done, done + 4)
            done += 4
        for t in range(hops + 2, last + 1):
            service(RW, t)
        for h in (0, 1):
            total = part[c, h]
            for d in (0, 1):
                held = sums.at[d, hops - 1, h]
                rs(d, hops, h, held).wait_recv()
                total += held[...]
            gkv[m, :, pl.ds(h * dim, dim)] = total.astype(BF16)
        start_own(RG)
        for t in range(tiles):
            at = pl.ds(t * rows, rows)
            st[t] += dot_nt(gkv[m], wqkv[at, pl.ds(dim, 2 * dim)])
        dx_heads(done, n)
        wait_sends(RY)
        for t in range(tiles):
            dy_all[0, :, pl.ds(t * rows, rows)] = st[t].astype(BF16)
        dx_out = local(dy_all.at[0], dx_hbm, 2)
        dx_out.start()

        def key_grads(blk):
            xs = x_all[blk, :, pl.ds(pl.multiple_of(m * cols, cols), cols)]
            dwkv[...] += dot_tn(xs, gkv[blk])

        def last_steps(v, _):
            u = lax.div(v, 2)
            kk = lax.rem(v, 2)

            @pl.when(v == 2)
            def _():
                service(RG, 0)

            @pl.when((kk == 0) & (u >= 1) & (u <= last))
            def _():
                service(RG, u)

            @pl.when(kk == 1)
            def _():
                wait_pair(RG, u)

            key_grads(2 * chip_at(u) + lax.rem(k + kk, 2))
            return 0

        lax.fori_loop(0, n, last_steps, 0)
        outs = [
            local(dwkv.at[:, pl.ds(0, dim)], dwk_hbm, 3),
            local(dwkv.at[:, pl.ds(dim, dim)], dwv_hbm, 4),
        ]
        for out in outs:
            out.start()
        for out in (dwo_out, dwq_out, dx_out, *outs):
            out.wait()

        for r in (RX, RW, RG):
            wait_sends(r)
        for i in range(chips):
            px(i).wait_send()
        for copy in sent:
            copy.wait_send()

        def sent_dq(h, _):
            @pl.when(h != m)
            def _():
                remote(dq_out.at[h], dq_in.at[h], dq_s.at[h], dq_r.at[h], h).wait_send()

            return 0

        lax.fori_loop(0, n, sent_dq, 0)

    return kernel


def solution(mesh):
    n = mesh.shape["model"]
    chips = n // 2
    hops = chips // 2
    tok_spec = P(("data", "model"), None)

    def local_step(x_loc, dy_loc, wq_loc, w_key, w_value, wo_loc):
        rows, width = x_loc.shape
        dim = w_key.shape[1]
        cols = width // n
        sds = jax.ShapeDtypeStruct
        vmem = pltpu.VMEM
        dma = pltpu.SemaphoreType.DMA
        arrivals = 2 * hops - 1
        outs = pl.pallas_call(
            make_kernel(n),
            name="mqa_backward",
            out_shape=(
                sds((rows, width), BF16),
                sds((width, dim), F32),
                sds((cols, dim), F32),
                sds((cols, dim), F32),
                sds((dim, width), F32),
                sds((n, width, dim), BF16),
            ),
            in_specs=[pl.BlockSpec(memory_space=pl.ANY)] * 6,
            out_specs=[pl.BlockSpec(memory_space=pl.ANY)] * 6,
            scratch_shapes=[
                vmem((n, rows, width), BF16),
                vmem((n, rows, width), BF16),
                vmem((n, rows, dim), BF16),
                vmem((n, rows, dim), BF16),
                vmem((n, rows, dim), BF16),
                vmem((n, dim, rows), BF16),
                vmem((n, dim, rows), BF16),
                vmem((width, 3 * dim), BF16),
                vmem((dim, width), BF16),
                vmem((n, 2, rows, dim), F32),
                vmem((chips, 2, rows, dim), F32),
                vmem((2, hops, 2, rows, dim), F32),
                vmem((n, rows, 2 * dim), BF16),
                vmem((n, rows, dim), BF16),
                vmem((n, rows, dim), BF16),
                vmem((dim, width), F32),
                vmem((dim, width), F32),
                vmem((n, rows, rows), F32),
                vmem((1, width, dim), BF16),
                vmem((dim, rows), F32),
                vmem((dim, rows), F32),
                vmem((dim, rows), BF16),
                vmem((dim, rows), BF16),
                vmem((rows, dim), BF16),
                vmem((cols, 2 * dim), F32),
                vmem((width, dim), F32),
                dma((4, 2, arrivals)),
                dma((4, 2, arrivals)),
                dma((4, 2 + 2 * arrivals)),
                dma((4, 2 + 2 * arrivals)),
                dma((n,)),
                dma((n,)),
                dma((chips,)),
                dma((chips,)),
                dma((2, hops, 2)),
                dma((2, hops, 2)),
                dma((6,)),
            ],
            compiler_params=pltpu.CompilerParams(
                collective_id=0, has_side_effects=True, vmem_limit_bytes=67043328
            ),
        )(
            x_loc,
            dy_loc,
            wq_loc.reshape(width, dim),
            w_key,
            w_value,
            wo_loc.reshape(dim, width),
        )
        dx, dwq, dwk, dwv, dwo, _ = outs
        return dx, dwq.reshape(width, 1, dim), dwk, dwv, dwo.reshape(1, dim, width)

    return jax.shard_map(
        local_step,
        mesh=mesh,
        in_specs=(tok_spec, tok_spec, P(None, "model", None), P(None, None), P(None, None), P("model", None, None)),
        out_specs=(tok_spec, P("data", "model", None), tok_spec, tok_spec, P(("data", "model"), None, None)),
        check_vma=False,
    )
```

```python
import math

import jax
import jax.numpy as jnp
from jax import lax
from jax.experimental import pallas as pl
from jax.experimental.pallas import tpu as pltpu
from jax.sharding import PartitionSpec as P

BF16 = jnp.bfloat16
F32 = jnp.float32
MESH = pl.DeviceIdType.MESH
RX, RY, RW, RG = range(4)


def dot(a, b):
    return jnp.dot(a, b, preferred_element_type=F32)


def dot_nt(a, b):
    return lax.dot_general(a, b, (((1,), (1,)), ((), ())), preferred_element_type=F32)


def dot_tn(a, b):
    return lax.dot_general(a, b, (((0,), (0,)), ((), ())), preferred_element_type=F32)


def rowfold(x, op):
    y = x.reshape(x.shape[0] // 8, 8, x.shape[1])
    return jnp.max(y, axis=0) if op == "max" else jnp.sum(y, axis=0)


def make_kernel(n):
    chips = n // 2
    hops = chips // 2
    last = 2 * (hops - 1)
    arrivals = last + 1

    def kernel(
        x_hbm, dy_hbm, wq_hbm, wk_hbm, wv_hbm, wo_hbm,
        dx_hbm, dwq_hbm, dwk_hbm, dwv_hbm, dwo_hbm, wq_all,
        x_all, dy_all, q_all, kv_all, kt_all, vt_all, wqkv, wo,
        dkv, part, sums, dq_in, dwqt, dwo_acc, st, wq_st,
        ot, dqt, dot_s, qt_s, do_s, dwkv,
        ring_r, ring_s, pair_r, pair_s, dq_r, dq_s, px_r, px_s, rs_r, rs_s, loc,
    ):
        rows, width = x_hbm.shape
        dim = wk_hbm.shape[1]
        cols = width // n
        tiles = width // rows
        scale = 1.0 / math.sqrt(dim)
        m = lax.axis_index("model")
        c = lax.div(m, 2)
        k = lax.rem(m, 2)
        mate = m + 1 - 2 * k
        nbr = (lax.rem(m + 2, n), lax.rem(m + n - 2, n))

        def remote(src, dst, ssem, rsem, dev):
            return pltpu.make_async_remote_copy(
                src_ref=src, dst_ref=dst, send_sem=ssem, recv_sem=rsem,
                device_id={"model": dev}, device_id_type=MESH,
            )

        bufs = (x_all, dy_all, wq_all)
        owns = (x_hbm, dy_hbm, wq_hbm)

        def half(ref, h):
            size = ref.shape[0] // 2
            return ref.at[pl.ds(pl.multiple_of(h * size, size), size), :]

        def chunk_at(r, blk, h):
            if r == RG:
                at = pl.ds(pl.multiple_of(lax.rem(blk, 2) * rows, rows), rows)
                return kv_all.at[h, lax.div(blk, 2), at, :]
            return half(bufs[r].at[blk], h)

        def own_at(r, h):
            return chunk_at(r, m, h) if r == RG else half(owns[r], h)

        def start_own(r):
            for p in (0, 1):
                for d in (0, 1):
                    h = p if d == 0 else 1 - p
                    remote(own_at(r, h), chunk_at(r, m, h), ring_s.at[r, d, p], ring_r.at[r, d, p], nbr[d]).start()
            for h in (0, 1):
                remote(own_at(r, h), chunk_at(r, m, h), pair_s.at[r, h], pair_r.at[r, h], mate).start()

        def service(r, a):
            step = lax.div(a, 2) + 1
            p = lax.rem(a, 2)
            for d in (0, 1):
                blk = lax.rem(m + (n - 2 * step if d == 0 else 2 * step), n)
                chunk = chunk_at(r, blk, p if d == 0 else 1 - p)
                remote(chunk, chunk, ring_s.at[r, d, 0], ring_r.at[r, d, a], nbr[d]).wait_recv()

                @pl.when(a <= last - 2)
                def _():
                    remote(chunk, chunk, ring_s.at[r, d, 2 + a], ring_r.at[r, d, a + 2], nbr[d]).start()

                i = 2 + d * arrivals + a
                remote(chunk, chunk, pair_s.at[r, i], pair_r.at[r, i], mate).start()

        def chip_at(u):
            step = lax.div(u + 1, 2)
            odd = lax.rem(u, 2)
            return lax.rem(c + odd * (chips - step) + (1 - odd) * step, chips)

        def wait_pair(r, u):
            blk = 2 * chip_at(u) + 1 - k

            def wait(h, i):
                chunk = chunk_at(r, blk, h)
                remote(chunk, chunk, pair_s.at[r, 0], pair_r.at[r, i], mate).wait_recv()

            @pl.when(u == 0)
            def _():
                wait(0, 0)
                wait(1, 1)

            @pl.when(u > 0)
            def _():
                d = 1 - lax.rem(u, 2)
                i = 2 + d * arrivals + 2 * (lax.div(u + 1, 2) - 1)
                wait(d, i)
                wait(1 - d, i + 1 + lax.div(u, chips - 1) * last)

        def wait_sends(r):
            chunk = own_at(r, 0)
            for d in (0, 1):
                for i in range(last + 1):
                    remote(chunk, chunk, ring_s.at[r, d, i], ring_r.at[r, d, 0], nbr[d]).wait_send()
            for i in range(2 + 2 * arrivals):
                remote(chunk, chunk, pair_s.at[r, i], pair_r.at[r, 0], mate).wait_send()

        def local(src, dst, i):
            return pltpu.make_async_copy(src, dst, loc.at[i])

        loads = [
            local(x_hbm, x_all.at[m], 0),
            local(wq_hbm, wqkv.at[:, pl.ds(0, dim)], 1),
            local(wk_hbm, wqkv.at[:, pl.ds(dim, dim)], 2),
            local(wv_hbm, wqkv.at[:, pl.ds(2 * dim, dim)], 3),
            local(wo_hbm, wo, 4),
            local(dy_hbm, dy_all.at[m], 5),
        ]
        for load in loads:
            load.start()
        barrier = pltpu.get_barrier_semaphore()
        for i in range(1, n):
            pl.semaphore_signal(barrier, inc=1, device_id={"model": lax.rem(m + i, n)}, device_id_type=MESH)
        pl.semaphore_wait(barrier, n - 1)
        start_own(RX)
        dwqt[...] = jnp.zeros_like(dwqt)
        dwo_acc[...] = jnp.zeros_like(dwo_acc)
        dwkv[...] = jnp.zeros_like(dwkv)

        def clear(j, _):
            dkv[j] = jnp.zeros(dkv.shape[1:], F32)
            return 0

        lax.fori_loop(0, n, clear, 0)
        for load in loads:
            load.wait()

        def project(ch):
            for i in (0, 1):
                at = pl.ds(i * rows, rows)
                qkv = dot(x_all[2 * ch + i], wqkv[...]).astype(BF16)
                q_all[ch, at, :] = qkv[:, :dim]
                kv_all[0, ch, at, :] = qkv[:, dim : 2 * dim]
                kv_all[1, ch, at, :] = qkv[:, 2 * dim :]
                kt_all[ch, :, at] = qkv[:, dim : 2 * dim].T
                vt_all[ch, :, at] = qkv[:, 2 * dim :].T

        def gathered(u, _):
            @pl.when(u == 1)
            def _():
                service(RX, 0)

            @pl.when((u >= 1) & (u <= last))
            def _():
                service(RX, u)

            @pl.when(u == last - 2)
            def _():
                start_own(RW)

            @pl.when(u == last)
            def _():
                start_own(RY)

            wait_pair(RX, u)
            project(chip_at(u))
            return 0

        lax.fori_loop(0, chips, gathered, 0)

        pair = 2 * rows
        factor = scale * math.log2(math.e)
        halves = [pl.ds(i * rows, rows) for i in (0, 1)]

        def attend(ch):
            for i in (0, 1):
                do_s[halves[i], :] = dot_nt(dy_all[2 * ch + i], wo[...]).astype(BF16)
            dot_s[...] = do_s[...].T
            qt_s[...] = q_all[ch].T

            def scores(j, top):
                for at in halves:
                    s = dot(kv_all[0, j, at, :], qt_s[...])
                    st[j, at, :] = s
                    top = jnp.maximum(top, rowfold(s, "max"))
                return top

            top = lax.fori_loop(0, ch, scores, jnp.full((8, pair), -jnp.inf, F32))
            for i in (0, 1):
                s = dot(kv_all[0, ch, halves[i], :], qt_s[...])
                key = lax.broadcasted_iota(jnp.int32, (rows, pair), 0) + i * rows
                query = lax.broadcasted_iota(jnp.int32, (rows, pair), 1)
                s = jnp.where(key <= query, s, -jnp.inf)
                st[ch, halves[i], :] = s
                top = jnp.maximum(top, rowfold(s, "max"))
            top = jnp.max(top, axis=0, keepdims=True)

            def weights(j, total):
                for at in halves:
                    p = jnp.exp2((st[j, at, :] - top) * factor)
                    st[j, at, :] = p
                    total += rowfold(p, "sum")
                return total

            total = lax.fori_loop(0, ch + 1, weights, jnp.zeros((8, pair), F32))
            inv = 1.0 / jnp.sum(total, axis=0, keepdims=True)
            ot[...] = jnp.zeros_like(ot)
            dqt[...] = jnp.zeros_like(dqt)

            def outputs(j, _):
                p = (st[j] * inv).astype(BF16)
                ot[...] += dot(vt_all[j], p)
                dv = dot(p, do_s[...])
                for i in (0, 1):
                    dkv[2 * j + i, 1] += dv[i * rows : (i + 1) * rows]
                return 0

            lax.fori_loop(0, ch + 1, outputs, 0)
            o = ot[...].astype(BF16)
            row = jnp.sum(dot_s[...].astype(F32) * o.astype(F32), axis=0, keepdims=True)
            inv_scale = inv * scale

            def grads(j, _):
                dp = dot(kv_all[1, j], dot_s[...])
                g = ((st[j] * inv_scale) * (dp - row)).astype(BF16)
                dqt[...] += dot(kt_all[j], g)
                dk = dot(g, q_all[ch])
                for i in (0, 1):
                    dkv[2 * j + i, 0] += dk[i * rows : (i + 1) * rows]
                return 0

            lax.fori_loop(0, ch + 1, grads, 0)
            dq = dqt[...].astype(BF16)
            q_all[ch] = dq.T
            for i in (0, 1):
                blk = 2 * ch + i

                @pl.when(blk != m)
                def _():
                    remote(q_all.at[ch, halves[i], :], dq_in.at[m], dq_s.at[blk], dq_r.at[m], blk).start()

            for t in range(tiles):
                at = pl.ds(t * rows, rows)
                add_q = dot(dq[:, :rows], x_all[2 * ch, :, at])
                add_o = dot(o[:, :rows], dy_all[2 * ch, :, at])
                dwqt[:, at] += add_q + dot(dq[:, rows:], x_all[2 * ch + 1, :, at])
                dwo_acc[:, at] += add_o + dot(o[:, rows:], dy_all[2 * ch + 1, :, at])

        def attended(u, _):
            @pl.when(u == 1)
            def _():
                for a in range(1, last - 3):
                    service(RW, a)
                service(RY, 0)

            @pl.when((u >= 1) & (u <= last))
            def _():
                service(RY, u)

            @pl.when(u == last - 2)
            def _():
                service(RW, last - 3)
                service(RW, last - 2)

            wait_pair(RY, u)
            attend(chip_at(u))
            return 0

        service(RW, 0)
        lax.fori_loop(0, chips, attended, 0)

        order = [hops]
        for step in range(hops - 1, 0, -1):
            order += [step, -step]
        order.append(0)

        def chip_off(off):
            return lax.rem(c + off + chips, chips)

        def px(i):
            chip = chip_off(order[i])
            return remote(dkv.at[2 * chip + 1 - k], part.at[chip], px_s.at[i], px_r.at[i], mate)

        for i in range(chips):
            px(i).start()
        dwo_out = local(dwo_acc, dwo_hbm, 0)
        dwo_out.start()
        spare = width // pair
        dwq_out = []
        for t in range(spare):
            at = pl.ds(t * pair, pair)
            staged = st.at[spare + t, :, pl.ds(0, dim)]
            staged[...] = dwqt[:, at].T
            out = local(staged, dwq_hbm.at[at, :], 6 + t)
            out.start()
            dwq_out.append(out)
            st[t, pl.ds(0, rows), :] = jnp.zeros((rows, pair), F32)

        def add_dx(dq, w_ref):
            for t in range(spare):
                st[t, pl.ds(0, rows), :] += dot_nt(dq, w_ref[pl.ds(t * pair, pair), :])

        def head_at(v):
            return 2 * chip_at(lax.div(v, 2)) + lax.rem(k + lax.rem(v, 2), 2)

        def fetch(v):
            slot = lax.rem(v, 2)
            return local(wq_all.at[head_at(v)], wq_st.at[slot], 2 + slot)

        def dx_head(v):
            h = head_at(v)
            fetch(v).wait()
            remote(dq_in.at[h], dq_in.at[h], dq_s.at[h], dq_r.at[h], mate).wait_recv()
            add_dx(dq_in[h], wq_st.at[lax.rem(v, 2)])

        def dx_heads(lo, hi):
            def body(v, _):
                @pl.when(lax.rem(v, 2) == 1)
                def _():
                    wait_pair(RW, lax.div(v, 2))

                fetch(v).start()

                @pl.when(v > 1)
                def _():
                    dx_head(v - 1)

                return 0

            lax.fori_loop(lo, hi, body, 0)

        def gather(i):
            px(i).wait_recv()
            chip = chip_off(order[i])
            part[chip] += dkv[2 * chip + k]

        def rs(d, t, h, src):
            return remote(src, sums.at[d, t - 1, h], rs_s.at[d, t - 1, h], rs_r.at[d, t - 1, h], nbr[d])

        sent = []

        def hop(t):
            for d in (0, 1):
                chip = chip_off((hops + 1 - t) * (1 - 2 * d))
                for h in (d, 1 - d):
                    if t == 1 and h != d:
                        continue
                    if t == 1 or (t == 2 and h != d):
                        copy = rs(d, t, h, part.at[chip, h])
                    else:
                        held = sums.at[d, t - 2, h]
                        rs(d, t - 1, h, held).wait_recv()
                        held[...] += part[chip, h]
                        copy = rs(d, t, h, held)
                    copy.start()
                    sent.append(copy)

        gather(0)
        hop(1)
        add_dx(q_all[c, pl.ds(pl.multiple_of(k * rows, rows), rows), :], wqkv.at[:, pl.ds(0, dim)])
        dx_heads(1, 3)
        gather(1)
        gather(2)
        hop(2)
        dx_heads(3, 5)
        for i in range(3, chips):
            gather(i)
        done = 5
        for t in range(3, hops + 1):
            hop(t)
            service(RW, last - hops + t)
            dx_heads(done, done + 4)
            done += 4

        def turn(j, _):
            for i in (0, 1):
                xs = x_all[2 * j + i, :, pl.ds(pl.multiple_of(m * cols, cols), cols)]
                kt_all[j, pl.ds(0, cols), halves[i]] = xs.T
            return 0

        lax.fori_loop(0, chips, turn, 0)
        for h in (0, 1):
            total = part[c, h]
            for d in (0, 1):
                held = sums.at[d, hops - 1, h]
                rs(d, hops, h, held).wait_recv()
                total += held[...]
            chunk_at(RG, m, h)[...] = total.astype(BF16)
        start_own(RG)
        own_kv = [chunk_at(RG, m, h)[...] for h in (0, 1)]
        for t in range(spare):
            at = pl.ds(t * pair, pair)
            add = dot_nt(own_kv[0], wqkv[at, pl.ds(dim, dim)])
            add += dot_nt(own_kv[1], wqkv[at, pl.ds(2 * dim, dim)])
            st[t, pl.ds(0, rows), :] += add
        dx_heads(done, n)
        dx_head(n - 1)
        wait_sends(RY)
        for t in range(spare):
            dy_all[0, :, pl.ds(t * pair, pair)] = st[t, pl.ds(0, rows), :].astype(BF16)
        dx_out = local(dy_all.at[0], dx_hbm, 4)
        dx_out.start()

        def last_steps(u, _):
            @pl.when(u == 1)
            def _():
                service(RG, 0)

            @pl.when((u >= 1) & (u <= last))
            def _():
                service(RG, u)

            wait_pair(RG, u)
            ch = chip_at(u)
            for h in (0, 1):
                dwkv[h] += dot(kt_all[ch, pl.ds(0, cols), :], kv_all[h, ch])
            return 0

        lax.fori_loop(0, chips, last_steps, 0)
        outs = [
            local(dwkv.at[0], dwk_hbm, 2),
            local(dwkv.at[1], dwv_hbm, 3),
        ]
        for out in outs:
            out.start()
        for out in (dwo_out, *dwq_out, dx_out, *outs):
            out.wait()

        for r in (RX, RW, RG):
            wait_sends(r)
        for i in range(chips):
            px(i).wait_send()
        for copy in sent:
            copy.wait_send()

        def sent_dq(h, _):
            @pl.when(h != m)
            def _():
                remote(dq_in.at[h], dq_in.at[h], dq_s.at[h], dq_r.at[h], h).wait_send()

            return 0

        lax.fori_loop(0, n, sent_dq, 0)

    return kernel


def hand_on(*refs):
    count = (len(refs) - 2) // 3
    srcs, dsts, bufs = refs[:count], refs[count : 2 * count], refs[2 * count : 3 * count]
    sems_in, sems_out = refs[3 * count :]
    pieces = []
    for src, dst, buf in zip(srcs, dsts, bufs):
        parts = max(1, src.shape[0] * src.shape[1] // (1 << 16))
        size = src.shape[0] // parts
        for i in range(parts):
            at = pl.ds(i * size, size)
            pieces.append((src.at[at, :], buf.at[at, :], dst.at[at, :]))
    ins = [pltpu.make_async_copy(a, b, sems_in.at[i]) for i, (a, b, _) in enumerate(pieces)]
    outs = [pltpu.make_async_copy(b, c, sems_out.at[i]) for i, (_, b, c) in enumerate(pieces)]
    for copy in ins:
        copy.start()
    for got, put in zip(ins, outs):
        got.wait()
        put.start()
    for put in outs:
        put.wait()


def solution(mesh):
    n = mesh.shape["model"]
    chips = n // 2
    hops = chips // 2
    tok_spec = P(("data", "model"), None)

    def local_step(x_loc, dy_loc, wq_loc, w_key, w_value, wo_loc):
        rows, width = x_loc.shape
        dim = w_key.shape[1]
        cols = width // n
        sds = jax.ShapeDtypeStruct
        vmem = pltpu.VMEM
        dma = pltpu.SemaphoreType.DMA
        arrivals = 2 * hops - 1
        outs = pl.pallas_call(
            make_kernel(n),
            name="mqa_backward",
            out_shape=(
                sds((rows, width), BF16),
                sds((width, dim), F32),
                sds((cols, dim), F32),
                sds((cols, dim), F32),
                sds((dim, width), F32),
                sds((n, width, dim), BF16),
            ),
            in_specs=[pl.BlockSpec(memory_space=pl.ANY)] * 6,
            out_specs=[pl.BlockSpec(memory_space=pl.ANY)] * 6,
            scratch_shapes=[
                vmem((n, rows, width), BF16),
                vmem((n, rows, width), BF16),
                vmem((chips, 2 * rows, dim), BF16),
                vmem((2, chips, 2 * rows, dim), BF16),
                vmem((chips, dim, 2 * rows), BF16),
                vmem((chips, dim, 2 * rows), BF16),
                vmem((width, 3 * dim), BF16),
                vmem((dim, width), BF16),
                vmem((n, 2, rows, dim), F32),
                vmem((chips, 2, rows, dim), F32),
                vmem((2, hops, 2, rows, dim), F32),
                vmem((n, rows, dim), BF16),
                vmem((dim, width), F32),
                vmem((dim, width), F32),
                vmem((chips, 2 * rows, 2 * rows), F32),
                vmem((2, width, dim), BF16),
                vmem((dim, 2 * rows), F32),
                vmem((dim, 2 * rows), F32),
                vmem((dim, 2 * rows), BF16),
                vmem((dim, 2 * rows), BF16),
                vmem((2 * rows, dim), BF16),
                vmem((2, cols, dim), F32),
                dma((4, 2, arrivals)),
                dma((4, 2, arrivals)),
                dma((4, 2 + 2 * arrivals)),
                dma((4, 2 + 2 * arrivals)),
                dma((n,)),
                dma((n,)),
                dma((chips,)),
                dma((chips,)),
                dma((2, hops, 2)),
                dma((2, hops, 2)),
                dma((6 + width // (2 * rows),)),
            ],
            compiler_params=pltpu.CompilerParams(
                collective_id=0, has_side_effects=True, vmem_limit_bytes=67043328
            ),
        )(
            x_loc,
            dy_loc,
            wq_loc.reshape(width, dim),
            w_key,
            w_value,
            wo_loc.reshape(dim, width),
        )
        results = outs[:5]
        any_spec = [pl.BlockSpec(memory_space=pl.ANY)] * 5
        dx, dwq, dwk, dwv, dwo = pl.pallas_call(
            hand_on,
            name="hand_on",
            out_shape=tuple(sds(o.shape, o.dtype) for o in results),
            in_specs=any_spec,
            out_specs=any_spec,
            scratch_shapes=[vmem(o.shape, o.dtype) for o in results] + [dma((64,)), dma((64,))],
        )(*results)
        return dx, dwq.reshape(width, 1, dim), dwk, dwv, dwo.reshape(1, dim, width)

    return jax.shard_map(
        local_step,
        mesh=mesh,
        in_specs=(tok_spec, tok_spec, P(None, "model", None), P(None, None), P(None, None), P("model", None, None)),
        out_specs=(tok_spec, P("data", "model", None), tok_spec, tok_spec, P(("data", "model"), None, None)),
        check_vma=False,
    )
```

```python
import math

import jax
import jax.numpy as jnp
from jax import lax
from jax.experimental import pallas as pl
from jax.experimental.pallas import tpu as pltpu
from jax.sharding import PartitionSpec as P

BF16 = jnp.bfloat16
F32 = jnp.float32
MESH = pl.DeviceIdType.MESH
RX, RY, RW, RG = range(4)


def dot(a, b):
    return jnp.dot(a, b, preferred_element_type=F32)


def dot_nt(a, b):
    return lax.dot_general(a, b, (((1,), (1,)), ((), ())), preferred_element_type=F32)


def dot_tn(a, b):
    return lax.dot_general(a, b, (((0,), (0,)), ((), ())), preferred_element_type=F32)


def rowfold(x, op):
    y = x.reshape(x.shape[0] // 8, 8, x.shape[1])
    return jnp.max(y, axis=0) if op == "max" else jnp.sum(y, axis=0)


def make_kernel(n):
    chips = n // 2
    hops = chips // 2
    last = 2 * (hops - 1)
    arrivals = last + 1

    def kernel(
        x_hbm, dy_hbm, wq_hbm, wk_hbm, wv_hbm, wo_hbm,
        dx_hbm, dwq_hbm, dwk_hbm, dwv_hbm, dwo_hbm, wq_all,
        x_all, dy_all, q_all, kv_all, kt_all, vt_all, o_all, lse, wqkv, wo, wot,
        dkv, part, sums, dq_in, dwqt, dwo_acc, st, wq_st,
        ot, dqt, dot_s, qt_s, do_s, dwkv,
        ring_r, ring_s, pair_r, pair_s, dq_r, dq_s, px_r, px_s, rs_r, rs_s, loc,
    ):
        rows, width = x_hbm.shape
        dim = wk_hbm.shape[1]
        cols = width // n
        scale = 1.0 / math.sqrt(dim)
        m = lax.axis_index("model")
        c = lax.div(m, 2)
        k = lax.rem(m, 2)
        mate = m + 1 - 2 * k
        nbr = (lax.rem(m + 2, n), lax.rem(m + n - 2, n))

        def remote(src, dst, ssem, rsem, dev):
            return pltpu.make_async_remote_copy(
                src_ref=src, dst_ref=dst, send_sem=ssem, recv_sem=rsem,
                device_id={"model": dev}, device_id_type=MESH,
            )

        bufs = (x_all, dy_all)
        owns = (x_hbm, dy_hbm, wq_hbm)

        def half(ref, h, size, base=0):
            return ref.at[pl.ds(pl.multiple_of(base + h * size, size), size), :]

        def chunk_at(r, blk, h):
            chip = lax.div(blk, 2)
            base = lax.rem(blk, 2) * rows
            if r == RG:
                return kv_all.at[h, chip, pl.ds(pl.multiple_of(base, rows), rows), :]
            if r == RW:
                return half(wq_all.at[blk], h, width // 2)
            return half(bufs[r].at[chip], h, rows // 2, base)

        def own_at(r, h):
            return chunk_at(r, m, h) if r == RG else half(owns[r], h, owns[r].shape[0] // 2)

        def start_own(r):
            for p in (0, 1):
                for d in (0, 1):
                    h = p if d == 0 else 1 - p
                    remote(own_at(r, h), chunk_at(r, m, h), ring_s.at[r, d, p], ring_r.at[r, d, p], nbr[d]).start()
            for h in (0, 1):
                remote(own_at(r, h), chunk_at(r, m, h), pair_s.at[r, h], pair_r.at[r, h], mate).start()

        def service(r, a):
            step = lax.div(a, 2) + 1
            p = lax.rem(a, 2)
            for d in (0, 1):
                blk = lax.rem(m + (n - 2 * step if d == 0 else 2 * step), n)
                chunk = chunk_at(r, blk, p if d == 0 else 1 - p)
                remote(chunk, chunk, ring_s.at[r, d, 0], ring_r.at[r, d, a], nbr[d]).wait_recv()

                @pl.when(a <= last - 2)
                def _():
                    remote(chunk, chunk, ring_s.at[r, d, 2 + a], ring_r.at[r, d, a + 2], nbr[d]).start()

                i = 2 + d * arrivals + a
                remote(chunk, chunk, pair_s.at[r, i], pair_r.at[r, i], mate).start()

        def chip_at(u):
            step = lax.div(u + 1, 2)
            odd = lax.rem(u, 2)
            return lax.rem(c + odd * (chips - step) + (1 - odd) * step, chips)

        def wait_pair(r, u):
            blk = 2 * chip_at(u) + 1 - k

            def wait(h, i):
                chunk = chunk_at(r, blk, h)
                remote(chunk, chunk, pair_s.at[r, 0], pair_r.at[r, i], mate).wait_recv()

            @pl.when(u == 0)
            def _():
                wait(0, 0)
                wait(1, 1)

            @pl.when(u > 0)
            def _():
                d = 1 - lax.rem(u, 2)
                i = 2 + d * arrivals + 2 * (lax.div(u + 1, 2) - 1)
                wait(d, i)
                wait(1 - d, i + 1 + lax.div(u, chips - 1) * last)

        def wait_sends(r):
            chunk = own_at(r, 0)
            for d in (0, 1):
                for i in range(last + 1):
                    remote(chunk, chunk, ring_s.at[r, d, i], ring_r.at[r, d, 0], nbr[d]).wait_send()
            for i in range(2 + 2 * arrivals):
                remote(chunk, chunk, pair_s.at[r, i], pair_r.at[r, 0], mate).wait_send()

        def local(src, dst, i):
            return pltpu.make_async_copy(src, dst, loc.at[i])

        own_rows = pl.ds(pl.multiple_of(k * rows, rows), rows)
        loads = [
            local(x_hbm, x_all.at[c, own_rows, :], 0),
            local(wq_hbm, wqkv.at[:, pl.ds(0, dim)], 1),
            local(wk_hbm, wqkv.at[:, pl.ds(dim, dim)], 2),
            local(wv_hbm, wqkv.at[:, pl.ds(2 * dim, dim)], 3),
            local(wo_hbm, wo, 4),
            local(dy_hbm, dy_all.at[c, own_rows, :], 5),
        ]
        for load in loads:
            load.start()
        barrier = pltpu.get_barrier_semaphore()
        for dev in (*nbr, mate):
            pl.semaphore_signal(barrier, inc=1, device_id={"model": dev}, device_id_type=MESH)
        pl.semaphore_wait(barrier, 3)
        start_own(RX)
        dwqt[...] = jnp.zeros_like(dwqt)
        dwo_acc[...] = jnp.zeros_like(dwo_acc)
        dwkv[...] = jnp.zeros_like(dwkv)

        def clear(j, _):
            dkv[j] = jnp.zeros(dkv.shape[1:], F32)
            return 0

        lax.fori_loop(0, n, clear, 0)
        for load in loads:
            load.wait()
        wot[...] = wo[...].T

        def project(ch):
            qkv = dot(x_all[ch], wqkv[...]).astype(BF16)
            q_all[ch] = qkv[:, :dim]
            kv_all[0, ch] = qkv[:, dim : 2 * dim]
            kv_all[1, ch] = qkv[:, 2 * dim :]
            kt_all[ch] = qkv[:, dim : 2 * dim].T
            vt_all[ch] = qkv[:, 2 * dim :].T

        def gathered(u, _):
            @pl.when(u == 1)
            def _():
                service(RX, 0)

            @pl.when((u >= 1) & (u <= last))
            def _():
                service(RX, u)

            @pl.when(u == last - 2)
            def _():
                start_own(RW)

            @pl.when(u == last)
            def _():
                start_own(RY)

            wait_pair(RX, u)
            project(chip_at(u))
            return 0

        lax.fori_loop(0, chips, gathered, 0)

        pair = 2 * rows
        factor = scale * math.log2(math.e)
        halves = [pl.ds(i * rows, rows) for i in (0, 1)]

        def causal(i):
            key = lax.broadcasted_iota(jnp.int32, (rows, pair), 0) + i * rows
            return key <= lax.broadcasted_iota(jnp.int32, (rows, pair), 1)

        def forward(ch):
            qt_s[...] = q_all[ch].T

            def scores(j, top):
                for at in halves:
                    s = dot(kv_all[0, j, at, :], qt_s[...])
                    st[j, at, :] = s
                    top = jnp.maximum(top, rowfold(s, "max"))
                return top

            top = lax.fori_loop(0, ch, scores, jnp.full((8, pair), -jnp.inf, F32))
            for i in (0, 1):
                s = dot(kv_all[0, ch, halves[i], :], qt_s[...])
                s = jnp.where(causal(i), s, -jnp.inf)
                st[ch, halves[i], :] = s
                top = jnp.maximum(top, rowfold(s, "max"))
            top = jnp.max(top, axis=0, keepdims=True)

            def weights(j, total):
                for at in halves:
                    p = jnp.exp2((st[j, at, :] - top) * factor)
                    st[j, at, :] = p
                    total += rowfold(p, "sum")
                return total

            total = lax.fori_loop(0, ch + 1, weights, jnp.zeros((8, pair), F32))
            total = jnp.sum(total, axis=0, keepdims=True)
            lse[ch] = jnp.broadcast_to(top * factor + jnp.log2(total), (8, pair))
            inv = 1.0 / total
            ot[...] = jnp.zeros_like(ot)

            def outputs(j, _):
                ot[...] += dot(vt_all[j], (st[j] * inv).astype(BF16))
                return 0

            lax.fori_loop(0, ch + 1, outputs, 0)
            o_all[ch] = ot[...].astype(BF16)

        def forwarded(u, _):
            @pl.when(u == hops)
            def _():
                service(RW, 1)

            forward(chip_at(u))
            return 0

        service(RW, 0)
        lax.fori_loop(0, chips, forwarded, 0)

        def attend(ch):
            do_s[...] = dot(dy_all[ch], wot[...]).astype(BF16)
            dot_s[...] = do_s[...].T
            qt_s[...] = q_all[ch].T
            row = jnp.sum(dot_s[...].astype(F32) * o_all[ch].astype(F32), axis=0, keepdims=True)
            shift = lse[ch, 0:1, :]
            dqt[...] = jnp.zeros_like(dqt)

            def tile(j, masked):
                add_q = 0.0
                for i in (0, 1):
                    at = halves[i]
                    s = dot(kv_all[0, j, at, :], qt_s[...])
                    p = jnp.exp2(s * factor - shift)
                    if masked:
                        p = jnp.where(causal(i), p, 0.0)
                    dp = dot(kv_all[1, j, at, :], dot_s[...])
                    g = (p * (dp - row) * scale).astype(BF16)
                    dkv[2 * j + i, 1] += dot(p.astype(BF16), do_s[...])
                    dkv[2 * j + i, 0] += dot(g, q_all[ch])
                    add_q += dot(kt_all[j, :, at], g)
                dqt[...] += add_q

            def grads(j, _):
                tile(j, False)
                return 0

            lax.fori_loop(0, ch, grads, 0)
            tile(ch, True)
            dq = dqt[...].astype(BF16)
            q_all[ch] = dq.T
            for i in (0, 1):
                blk = 2 * ch + i

                @pl.when(blk != m)
                def _():
                    remote(q_all.at[ch, halves[i], :], dq_in.at[m], dq_s.at[blk], dq_r.at[m], blk).start()

            for t in range(width // pair):
                at = pl.ds(t * pair, pair)
                dwqt[:, at] += dot(dq, x_all[ch, :, at])
                dwo_acc[:, at] += dot(o_all[ch], dy_all[ch, :, at])

        def attended(u, _):
            @pl.when(u == 1)
            def _():
                for a in range(2, last - 3):
                    service(RW, a)
                service(RY, 0)

            @pl.when((u >= 1) & (u < last))
            def _():
                service(RY, u)

            @pl.when(u == last - 2)
            def _():
                service(RW, last - 3)
                service(RW, last - 2)

            @pl.when(u == chips - 1)
            def _():
                service(RY, last)

            wait_pair(RY, u)
            attend(chip_at(u))
            return 0

        lax.fori_loop(0, chips, attended, 0)

        order = [hops]
        for step in range(hops - 1, 0, -1):
            order += [step, -step]
        order.append(0)

        def chip_off(off):
            return lax.rem(c + off + chips, chips)

        def px(i):
            chip = chip_off(order[i])
            return remote(dkv.at[2 * chip + 1 - k], part.at[chip], px_s.at[i], px_r.at[i], mate)

        for i in range(chips):
            px(i).start()
        dwo_out = local(dwo_acc, dwo_hbm, 0)
        dwo_out.start()
        spare = width // pair
        dwq_out = []
        for t in range(spare):
            at = pl.ds(t * pair, pair)
            staged = st.at[spare + t, :, pl.ds(0, dim)]
            staged[...] = dwqt[:, at].T
            out = local(staged, dwq_hbm.at[at, :], 6 + t)
            out.start()
            dwq_out.append(out)
            st[t, pl.ds(0, rows), :] = jnp.zeros((rows, pair), F32)

        def add_dx(dq, w_ref):
            for t in range(spare):
                st[t, pl.ds(0, rows), :] += dot_nt(dq, w_ref[pl.ds(t * pair, pair), :])

        def head_at(v):
            return 2 * chip_at(lax.div(v, 2)) + lax.rem(k + lax.rem(v, 2), 2)

        def fetch(v):
            slot = lax.rem(v, 2)
            return local(wq_all.at[head_at(v)], wq_st.at[slot], 2 + slot)

        def dx_head(v):
            h = head_at(v)
            fetch(v).wait()
            remote(dq_in.at[h], dq_in.at[h], dq_s.at[h], dq_r.at[h], mate).wait_recv()
            add_dx(dq_in[h], wq_st.at[lax.rem(v, 2)])

        def dx_heads(lo, hi):
            def body(v, _):
                @pl.when(lax.rem(v, 2) == 1)
                def _():
                    wait_pair(RW, lax.div(v, 2))

                fetch(v).start()

                @pl.when(v > 1)
                def _():
                    dx_head(v - 1)

                return 0

            lax.fori_loop(lo, hi, body, 0)

        def gather(i):
            px(i).wait_recv()
            chip = chip_off(order[i])
            part[chip] += dkv[2 * chip + k]

        def rs(d, t, h, src):
            return remote(src, sums.at[d, t - 1, h], rs_s.at[d, t - 1, h], rs_r.at[d, t - 1, h], nbr[d])

        sent = []

        def hop(t):
            for d in (0, 1):
                chip = chip_off((hops + 1 - t) * (1 - 2 * d))
                for h in (d, 1 - d):
                    if t == 1 and h != d:
                        continue
                    if t == 1 or (t == 2 and h != d):
                        copy = rs(d, t, h, part.at[chip, h])
                    else:
                        held = sums.at[d, t - 2, h]
                        rs(d, t - 1, h, held).wait_recv()
                        held[...] += part[chip, h]
                        copy = rs(d, t, h, held)
                    copy.start()
                    sent.append(copy)

        gather(0)
        hop(1)
        add_dx(q_all[c, own_rows, :], wqkv.at[:, pl.ds(0, dim)])
        dx_heads(1, 3)
        gather(1)
        gather(2)
        hop(2)
        dx_heads(3, 5)
        for i in range(3, chips):
            gather(i)
        done = 5
        for t in range(3, hops + 1):
            hop(t)
            service(RW, last - hops + t)
            dx_heads(done, done + 4)
            done += 4

        def turn(j, _):
            xs = x_all[j, :, pl.ds(pl.multiple_of(m * cols, cols), cols)]
            kt_all[j, pl.ds(0, cols), :] = xs.T
            return 0

        lax.fori_loop(0, chips, turn, 0)
        for h in (0, 1):
            total = part[c, h]
            for d in (0, 1):
                held = sums.at[d, hops - 1, h]
                rs(d, hops, h, held).wait_recv()
                total += held[...]
            chunk_at(RG, m, h)[...] = total.astype(BF16)
        start_own(RG)
        own_kv = [chunk_at(RG, m, h)[...] for h in (0, 1)]
        for t in range(spare):
            at = pl.ds(t * pair, pair)
            add = dot_nt(own_kv[0], wqkv[at, pl.ds(dim, dim)])
            add += dot_nt(own_kv[1], wqkv[at, pl.ds(2 * dim, dim)])
            st[t, pl.ds(0, rows), :] += add
        dx_heads(done, n)
        dx_head(n - 1)
        wait_sends(RY)
        for t in range(spare):
            dy_all[0, pl.ds(0, rows), pl.ds(t * pair, pair)] = st[t, pl.ds(0, rows), :].astype(BF16)
        dx_out = local(dy_all.at[0, pl.ds(0, rows), :], dx_hbm, 4)
        dx_out.start()

        def last_steps(u, _):
            @pl.when(u == 1)
            def _():
                service(RG, 0)

            @pl.when((u >= 1) & (u <= last))
            def _():
                service(RG, u)

            wait_pair(RG, u)
            ch = chip_at(u)
            for h in (0, 1):
                dwkv[h] += dot(kt_all[ch, pl.ds(0, cols), :], kv_all[h, ch])
            return 0

        lax.fori_loop(0, chips, last_steps, 0)
        outs = [
            local(dwkv.at[0], dwk_hbm, 2),
            local(dwkv.at[1], dwv_hbm, 3),
        ]
        for out in outs:
            out.start()
        for out in (dwo_out, *dwq_out, dx_out, *outs):
            out.wait()

        for r in (RX, RW, RG):
            wait_sends(r)
        for i in range(chips):
            px(i).wait_send()
        for copy in sent:
            copy.wait_send()

        def sent_dq(h, _):
            @pl.when(h != m)
            def _():
                remote(dq_in.at[h], dq_in.at[h], dq_s.at[h], dq_r.at[h], h).wait_send()

            return 0

        lax.fori_loop(0, n, sent_dq, 0)

    return kernel


def hand_on(*refs):
    count = (len(refs) - 2) // 3
    srcs, dsts, bufs = refs[:count], refs[count : 2 * count], refs[2 * count : 3 * count]
    sems_in, sems_out = refs[3 * count :]
    pieces = []
    for src, dst, buf in zip(srcs, dsts, bufs):
        parts = max(1, src.shape[0] * src.shape[1] // (1 << 16))
        size = src.shape[0] // parts
        for i in range(parts):
            at = pl.ds(i * size, size)
            pieces.append((src.at[at, :], buf.at[at, :], dst.at[at, :]))
    ins = [pltpu.make_async_copy(a, b, sems_in.at[i]) for i, (a, b, _) in enumerate(pieces)]
    outs = [pltpu.make_async_copy(b, c, sems_out.at[i]) for i, (_, b, c) in enumerate(pieces)]
    for copy in ins:
        copy.start()
    for got, put in zip(ins, outs):
        got.wait()
        put.start()
    for put in outs:
        put.wait()


def solution(mesh):
    n = mesh.shape["model"]
    chips = n // 2
    hops = chips // 2
    tok_spec = P(("data", "model"), None)

    def local_step(x_loc, dy_loc, wq_loc, w_key, w_value, wo_loc):
        rows, width = x_loc.shape
        dim = w_key.shape[1]
        cols = width // n
        sds = jax.ShapeDtypeStruct
        vmem = pltpu.VMEM
        dma = pltpu.SemaphoreType.DMA
        arrivals = 2 * hops - 1
        outs = pl.pallas_call(
            make_kernel(n),
            name="mqa_backward",
            out_shape=(
                sds((rows, width), BF16),
                sds((width, dim), F32),
                sds((cols, dim), F32),
                sds((cols, dim), F32),
                sds((dim, width), F32),
                sds((n, width, dim), BF16),
            ),
            in_specs=[pl.BlockSpec(memory_space=pl.ANY)] * 6,
            out_specs=[pl.BlockSpec(memory_space=pl.ANY)] * 6,
            scratch_shapes=[
                vmem((chips, 2 * rows, width), BF16),
                vmem((chips, 2 * rows, width), BF16),
                vmem((chips, 2 * rows, dim), BF16),
                vmem((2, chips, 2 * rows, dim), BF16),
                vmem((chips, dim, 2 * rows), BF16),
                vmem((chips, dim, 2 * rows), BF16),
                vmem((chips, dim, 2 * rows), BF16),
                vmem((chips, 8, 2 * rows), F32),
                vmem((width, 3 * dim), BF16),
                vmem((dim, width), BF16),
                vmem((width, dim), BF16),
                vmem((n, 2, rows, dim), F32),
                vmem((chips, 2, rows, dim), F32),
                vmem((2, hops, 2, rows, dim), F32),
                vmem((n, rows, dim), BF16),
                vmem((dim, width), F32),
                vmem((dim, width), F32),
                vmem((chips, 2 * rows, 2 * rows), F32),
                vmem((2, width, dim), BF16),
                vmem((dim, 2 * rows), F32),
                vmem((dim, 2 * rows), F32),
                vmem((dim, 2 * rows), BF16),
                vmem((dim, 2 * rows), BF16),
                vmem((2 * rows, dim), BF16),
                vmem((2, cols, dim), F32),
                dma((4, 2, arrivals)),
                dma((4, 2, arrivals)),
                dma((4, 2 + 2 * arrivals)),
                dma((4, 2 + 2 * arrivals)),
                dma((n,)),
                dma((n,)),
                dma((chips,)),
                dma((chips,)),
                dma((2, hops, 2)),
                dma((2, hops, 2)),
                dma((6 + width // (2 * rows),)),
            ],
            compiler_params=pltpu.CompilerParams(
                collective_id=0, has_side_effects=True, vmem_limit_bytes=67043328
            ),
        )(
            x_loc,
            dy_loc,
            wq_loc.reshape(width, dim),
            w_key,
            w_value,
            wo_loc.reshape(dim, width),
        )
        results = outs[:5]
        any_spec = [pl.BlockSpec(memory_space=pl.ANY)] * 5
        dx, dwq, dwk, dwv, dwo = pl.pallas_call(
            hand_on,
            name="hand_on",
            out_shape=tuple(sds(o.shape, o.dtype) for o in results),
            in_specs=any_spec,
            out_specs=any_spec,
            scratch_shapes=[vmem(o.shape, o.dtype) for o in results] + [dma((64,)), dma((64,))],
        )(*results)
        return dx, dwq.reshape(width, 1, dim), dwk, dwv, dwo.reshape(1, dim, width)

    return jax.shard_map(
        local_step,
        mesh=mesh,
        in_specs=(tok_spec, tok_spec, P(None, "model", None), P(None, None), P(None, None), P("model", None, None)),
        out_specs=(tok_spec, P("data", "model", None), tok_spec, tok_spec, P(("data", "model"), None, None)),
        check_vma=False,
    )
```

```python
import math

import jax
import jax.numpy as jnp
from jax import lax
from jax.experimental import pallas as pl
from jax.experimental.pallas import tpu as pltpu
from jax.sharding import PartitionSpec as P

BF16 = jnp.bfloat16
F32 = jnp.float32
MESH = pl.DeviceIdType.MESH
RX, RY, RW = range(3)


def dot(a, b):
    return jnp.dot(a, b, preferred_element_type=F32)


def dot_nt(a, b):
    return lax.dot_general(a, b, (((1,), (1,)), ((), ())), preferred_element_type=F32)


def dot_tn(a, b):
    return lax.dot_general(a, b, (((0,), (0,)), ((), ())), preferred_element_type=F32)


def rowfold(x, op):
    y = x.reshape(x.shape[0] // 8, 8, x.shape[1])
    return jnp.max(y, axis=0) if op == "max" else jnp.sum(y, axis=0)


def make_kernel(n):
    chips = n // 2
    hops = chips // 2
    last = 2 * (hops - 1)
    arrivals = last + 1

    def kernel(
        x_hbm, dy_hbm, wq_hbm, wk_hbm, wv_hbm, wo_hbm,
        dx_hbm, dwq_hbm, dwk_hbm, dwv_hbm, dwo_hbm, wq_all,
        x_all, dy_all, q_all, kv_all, kt_all, vt_all, o_all, lse, wqkv, wo, wot,
        dkv, part, sums, dq_in, dwqt, dwo_acc, st, wq_st,
        ot, dqt, dot_s, qt_s, thin, kv_rows, dw_out, dw_in, dw_t,
        ring_r, ring_s, pair_r, pair_s, dq_r, dq_s, px_r, px_s, rs_r, rs_s,
        kv_r, kv_s, dw_r, dw_s, loc,
    ):
        rows, width = x_hbm.shape
        dim = wk_hbm.shape[1]
        cols = width // n
        slim = 2 * dim // n
        quarter = chips // 2
        scale = 1.0 / math.sqrt(dim)
        m = lax.axis_index("model")
        c = lax.div(m, 2)
        k = lax.rem(m, 2)
        mate = m + 1 - 2 * k
        nbr = (lax.rem(m + 2, n), lax.rem(m + n - 2, n))

        def remote(src, dst, ssem, rsem, dev):
            return pltpu.make_async_remote_copy(
                src_ref=src, dst_ref=dst, send_sem=ssem, recv_sem=rsem,
                device_id={"model": dev}, device_id_type=MESH,
            )

        bufs = (x_all, dy_all)
        owns = (x_hbm, dy_hbm, wq_hbm)

        def half(ref, h, size, base=0):
            return ref.at[pl.ds(pl.multiple_of(base + h * size, size), size), :]

        def chunk_at(r, blk, h):
            chip = lax.div(blk, 2)
            base = lax.rem(blk, 2) * rows
            if r == RW:
                return half(wq_all.at[blk], h, width // 2)
            return half(bufs[r].at[chip], h, rows // 2, base)

        def own_at(r, h):
            return half(owns[r], h, owns[r].shape[0] // 2)

        def start_own(r):
            for p in (0, 1):
                for d in (0, 1):
                    h = p if d == 0 else 1 - p
                    remote(own_at(r, h), chunk_at(r, m, h), ring_s.at[r, d, p], ring_r.at[r, d, p], nbr[d]).start()
            for h in (0, 1):
                remote(own_at(r, h), chunk_at(r, m, h), pair_s.at[r, h], pair_r.at[r, h], mate).start()

        def service(r, a):
            step = lax.div(a, 2) + 1
            p = lax.rem(a, 2)
            for d in (0, 1):
                blk = lax.rem(m + (n - 2 * step if d == 0 else 2 * step), n)
                chunk = chunk_at(r, blk, p if d == 0 else 1 - p)
                remote(chunk, chunk, ring_s.at[r, d, 0], ring_r.at[r, d, a], nbr[d]).wait_recv()

                @pl.when(a <= last - 2)
                def _():
                    remote(chunk, chunk, ring_s.at[r, d, 2 + a], ring_r.at[r, d, a + 2], nbr[d]).start()

                i = 2 + d * arrivals + a
                remote(chunk, chunk, pair_s.at[r, i], pair_r.at[r, i], mate).start()

        def chip_at(u):
            step = lax.div(u + 1, 2)
            odd = lax.rem(u, 2)
            return lax.rem(c + odd * (chips - step) + (1 - odd) * step, chips)

        def wait_pair(r, u):
            blk = 2 * chip_at(u) + 1 - k

            def wait(h, i):
                chunk = chunk_at(r, blk, h)
                remote(chunk, chunk, pair_s.at[r, 0], pair_r.at[r, i], mate).wait_recv()

            @pl.when(u == 0)
            def _():
                wait(0, 0)
                wait(1, 1)

            @pl.when(u > 0)
            def _():
                d = 1 - lax.rem(u, 2)
                i = 2 + d * arrivals + 2 * (lax.div(u + 1, 2) - 1)
                wait(d, i)
                wait(1 - d, i + 1 + lax.div(u, chips - 1) * last)

        def wait_sends(r):
            chunk = own_at(r, 0)
            for d in (0, 1):
                for i in range(last + 1):
                    remote(chunk, chunk, ring_s.at[r, d, i], ring_r.at[r, d, 0], nbr[d]).wait_send()
            for i in range(2 + 2 * arrivals):
                remote(chunk, chunk, pair_s.at[r, i], pair_r.at[r, 0], mate).wait_send()

        def local(src, dst, i):
            return pltpu.make_async_copy(src, dst, loc.at[i])

        own_rows = pl.ds(pl.multiple_of(k * rows, rows), rows)
        loads = [
            local(x_hbm, x_all.at[c, own_rows, :], 0),
            local(wq_hbm, wqkv.at[:, pl.ds(0, dim)], 1),
            local(wk_hbm, wqkv.at[:, pl.ds(dim, dim)], 2),
            local(wv_hbm, wqkv.at[:, pl.ds(2 * dim, dim)], 3),
            local(wo_hbm, wo, 4),
            local(dy_hbm, dy_all.at[c, own_rows, :], 5),
        ]
        for load in loads:
            load.start()
        barrier = pltpu.get_barrier_semaphore()
        for dev in (*nbr, mate):
            pl.semaphore_signal(barrier, inc=1, device_id={"model": dev}, device_id_type=MESH)
        pl.semaphore_wait(barrier, 3)
        start_own(RX)
        dwqt[...] = jnp.zeros_like(dwqt)
        dwo_acc[...] = jnp.zeros_like(dwo_acc)

        def clear(j, _):
            for kind in (0, 1):
                for hi in (0, 1):
                    dkv[kind, hi, j] = jnp.zeros(dkv.shape[3:], F32)
            return 0

        lax.fori_loop(0, quarter, clear, 0)
        for load in loads:
            load.wait()
        wot[...] = wo[...].T

        def project(ch):
            qkv = dot(x_all[ch], wqkv[...]).astype(BF16)
            q_all[ch] = qkv[:, :dim]
            kv_all[0, ch] = qkv[:, dim : 2 * dim]
            kv_all[1, ch] = qkv[:, 2 * dim :]
            kt_all[ch] = qkv[:, dim : 2 * dim].T
            vt_all[ch] = qkv[:, 2 * dim :].T

        def gathered(u, _):
            @pl.when(u == 1)
            def _():
                service(RX, 0)

            @pl.when((u >= 1) & (u <= last))
            def _():
                service(RX, u)

            @pl.when(u == last - 2)
            def _():
                start_own(RW)

            @pl.when(u == last)
            def _():
                start_own(RY)

            wait_pair(RX, u)
            project(chip_at(u))
            return 0

        lax.fori_loop(0, chips, gathered, 0)

        pair = 2 * rows
        factor = scale * math.log2(math.e)
        halves = [pl.ds(i * rows, rows) for i in (0, 1)]

        def causal(i):
            key = lax.broadcasted_iota(jnp.int32, (rows, pair), 0) + i * rows
            return key <= lax.broadcasted_iota(jnp.int32, (rows, pair), 1)

        def forward(ch):
            qt_s[...] = q_all[ch].T

            def scores(j, top):
                for at in halves:
                    s = dot(kv_all[0, j, at, :], qt_s[...])
                    st[j, at, :] = s
                    top = jnp.maximum(top, rowfold(s, "max"))
                return top

            top = lax.fori_loop(0, ch, scores, jnp.full((8, pair), -jnp.inf, F32))
            for i in (0, 1):
                s = dot(kv_all[0, ch, halves[i], :], qt_s[...])
                s = jnp.where(causal(i), s, -jnp.inf)
                st[ch, halves[i], :] = s
                top = jnp.maximum(top, rowfold(s, "max"))
            top = jnp.max(top, axis=0, keepdims=True)

            def weights(j, total):
                for at in halves:
                    p = jnp.exp2((st[j, at, :] - top) * factor)
                    st[j, at, :] = p
                    total += rowfold(p, "sum")
                return total

            total = lax.fori_loop(0, ch + 1, weights, jnp.zeros((8, pair), F32))
            total = jnp.sum(total, axis=0, keepdims=True)
            lse[ch] = jnp.broadcast_to(top * factor + jnp.log2(total), (8, pair))
            inv = 1.0 / total
            ot[...] = jnp.zeros_like(ot)

            def outputs(j, _):
                ot[...] += dot(vt_all[j], (st[j] * inv).astype(BF16))
                return 0

            lax.fori_loop(0, ch + 1, outputs, 0)
            o_all[ch] = ot[...].astype(BF16)

        def forwarded(u, _):
            @pl.when(u == hops)
            def _():
                service(RW, 1)

            forward(chip_at(u))
            return 0

        service(RW, 0)
        lax.fori_loop(0, chips, forwarded, 0)

        def attend(ch):
            dot_s[...] = dot(dy_all[ch], wot[...]).astype(BF16).T
            qt_s[...] = q_all[ch].T
            row = jnp.sum(dot_s[...].astype(F32) * o_all[ch].astype(F32), axis=0, keepdims=True)
            shift = lse[ch, 0:1, :]
            dqt[...] = jnp.zeros_like(dqt)

            def tile(j, masked):
                add_q = 0.0
                hi, lo = lax.div(j, quarter), lax.rem(j, quarter)
                for i in (0, 1):
                    at = halves[i]
                    s = dot(kv_all[0, j, at, :], qt_s[...])
                    p = jnp.exp2(s * factor - shift)
                    if masked:
                        p = jnp.where(causal(i), p, 0.0)
                    dp = dot(kv_all[1, j, at, :], dot_s[...])
                    g = (p * (dp - row) * scale).astype(BF16)
                    dkv[1, hi, lo, :, at] += dot_nt(dot_s[...], p.astype(BF16))
                    dkv[0, hi, lo, :, at] += dot_nt(qt_s[...], g)
                    add_q += dot(kt_all[j, :, at], g)
                dqt[...] += add_q

            def grads(j, _):
                tile(j, False)
                return 0

            lax.fori_loop(0, ch, grads, 0)
            tile(ch, True)
            dq = dqt[...].astype(BF16)
            q_all[ch] = dq.T
            for t in range(width // pair):
                at = pl.ds(t * pair, pair)
                dwqt[:, at] += dot(dq, x_all[ch, :, at])
                dwo_acc[:, at] += dot(o_all[ch], dy_all[ch, :, at])

        def send_dq(u, i):
            ch = chip_at(u)
            blk = 2 * ch + i

            @pl.when(blk != m)
            def _():
                remote(q_all.at[ch, halves[i], :], dq_in.at[m], dq_s.at[blk], dq_r.at[m], blk).start()

        late = chips - 1

        def attended(u, _):
            @pl.when(u == 1)
            def _():
                for a in range(2, last - 1 - 2):
                    service(RW, a)
                service(RY, 0)

            @pl.when((u >= 1) & (u < last))
            def _():
                service(RY, u)

            @pl.when(u == last - 2)
            def _():
                service(RW, last - 2 - 1)
                service(RW, last - 2 - 0)

            @pl.when(u == chips - 1)
            def _():
                service(RY, last)

            wait_pair(RY, u)
            attend(chip_at(u))

            @pl.when(u < late)
            def _():
                send_dq(u, 0)
                send_dq(u, 1)

            return 0

        lax.fori_loop(0, chips, attended, 0)

        order = [hops]
        for step in range(hops - 1, 0, -1):
            order += [step, -step]
        order.append(0)

        def chip_off(off):
            return lax.rem(c + off + chips, chips)

        def slice_of(dev):
            row = pl.multiple_of(lax.rem(dev, chips) * slim, slim)
            return dkv.at[lax.div(dev, chips), :, :, pl.ds(row, slim), :]

        def px(i):
            chip = chip_off(order[i])
            return remote(slice_of(2 * chip + 1 - k), part.at[chip], px_s.at[i], px_r.at[i], mate)

        for i in range(chips):
            px(i).start()
        dwo_out = local(dwo_acc, dwo_hbm, 0)
        dwo_out.start()
        spare = width // pair
        dwq_out = []
        for t in range(spare):
            at = pl.ds(t * pair, pair)
            staged = st.at[spare + t, :, pl.ds(0, dim)]
            staged[...] = dwqt[:, at].T
            out = local(staged, dwq_hbm.at[at, :], 6 + t)
            out.start()
            dwq_out.append(out)
            st[t, pl.ds(0, rows), :] = jnp.zeros((rows, pair), F32)

        def add_dx(dq, w_ref):
            for t in range(spare):
                st[t, pl.ds(0, rows), :] += dot_nt(dq, w_ref[pl.ds(t * pair, pair), :])

        def head_at(v):
            return 2 * chip_at(lax.div(v, 2)) + lax.rem(k + lax.rem(v, 2), 2)

        def fetch(v):
            slot = lax.rem(v, 2)
            return local(wq_all.at[head_at(v)], wq_st.at[slot], 2 + slot)

        def dx_head(v):
            h = head_at(v)
            fetch(v).wait()
            remote(dq_in.at[h], dq_in.at[h], dq_s.at[h], dq_r.at[h], mate).wait_recv()
            add_dx(dq_in[h], wq_st.at[lax.rem(v, 2)])

        def dx_heads(lo, hi):
            def body(v, _):
                @pl.when(lax.rem(v, 2) == 1)
                def _():
                    wait_pair(RW, lax.div(v, 2))

                fetch(v).start()

                @pl.when(v > 1)
                def _():
                    dx_head(v - 1)

                return 0

            lax.fori_loop(lo, hi, body, 0)

        def gather(i):
            px(i).wait_recv()
            chip = chip_off(order[i])
            part[chip] += slice_of(2 * chip + k)[...]

        def rs(d, t, h, src):
            return remote(src, sums.at[d, t - 1, h], rs_s.at[d, t - 1, h], rs_r.at[d, t - 1, h], nbr[d])

        sent = []

        def hop(t):
            for first in (True, False):
                for d in (0, 1):
                    h = d if first else 1 - d
                    chip = chip_off((hops + 1 - t) * (1 - 2 * d))
                    if t == 1 and not first:
                        continue
                    if t == 1 or (t == 2 and not first):
                        copy = rs(d, t, h, part.at[chip, h])
                    else:
                        held = sums.at[d, t - 2, h]
                        rs(d, t - 1, h, held).wait_recv()
                        held[...] += part[chip, h]
                        copy = rs(d, t, h, held)
                    copy.start()
                    sent.append(copy)

        gather(0)
        hop(1)
        add_dx(q_all[c, own_rows, :], wqkv.at[:, pl.ds(0, dim)])
        dx_heads(1, 3)
        gather(1)
        gather(2)
        hop(2)
        for i in range(3, chips):
            gather(i)
        dx_heads(3, 5)
        done = 5
        for t in range(3, hops + 1):
            hop(t)
            service(RW, last - hops + t)
            send_dq(chips - 1, t - hops + 1)
            dx_heads(done, done + 2)
            done += 2

        for h in (0, 1):
            total = part[c, h]
            for d in (0, 1):
                held = sums.at[d, hops - 1, h]
                rs(d, hops, h, held).wait_recv()
                total += held[...]
            thin[h] = total.astype(BF16)

        def tokens_of(dev):
            chip = lax.div(dev, 2)
            at = pl.ds(pl.multiple_of(lax.rem(dev, 2) * rows, rows), rows)
            return thin.at[lax.div(chip, quarter), lax.rem(chip, quarter), :, at]

        def kv_copy(i):
            dev = lax.rem(m + i, n)
            return remote(tokens_of(dev), kv_rows.at[m], kv_s.at[i], kv_r.at[i], dev)

        far = sorted(range(1, n), key=lambda i: -min(i, n - i))
        for i in far:
            kv_copy(i).start()
        kv_rows[m] = tokens_of(m)[...]

        def dw_copy(dev):
            return remote(dw_out.at[dev], dw_in.at[m], dw_s.at[dev], dw_r.at[m], dev)

        per = pair // cols

        def key_grads(t, _):
            at = pl.ds(pl.multiple_of(t * pair, pair), pair)
            add = dot(thin[0, 0], x_all[0, :, at])
            for j in range(1, chips):
                add += dot(thin[j // quarter, j % quarter], x_all[j, :, at])
            for i in range(per):
                dw_out[t * per + i] = add[:, i * cols : (i + 1) * cols]
            for i in range(per):
                dev = t * per + i

                @pl.when(dev != m)
                def _():
                    dw_copy(dev).start()

            return 0

        lax.fori_loop(0, width // pair, key_grads, 0)
        dx_heads(done, n)
        dx_head(n - 1)
        for i in far:
            kv_copy(i).wait_recv()
        own_kv = kv_rows[...].reshape(2 * dim, rows).T
        wait_sends(RY)
        for t in range(spare):
            at = pl.ds(t * pair, pair)
            add = dot_nt(own_kv, wqkv[at, pl.ds(dim, 2 * dim)])
            dy_all[0, pl.ds(0, rows), at] = (st[t, pl.ds(0, rows), :] + add).astype(BF16)
        dx_out = local(dy_all.at[0, pl.ds(0, rows), :], dx_hbm, 4)
        dx_out.start()
        dw_in[m] = dw_out[m]

        def arrived(dev, _):
            @pl.when(dev != m)
            def _():
                dw_copy(dev).wait_send()
                remote(dw_in.at[dev], dw_in.at[dev], dw_s.at[dev], dw_r.at[dev], mate).wait_recv()

            return 0

        lax.fori_loop(0, n, arrived, 0)
        turned = dw_in[...].reshape(2 * dim, cols)
        dw_t[0] = turned[:dim].T
        dw_t[1] = turned[dim:].T
        outs = [local(dw_t.at[0], dwk_hbm, 2), local(dw_t.at[1], dwv_hbm, 3)]
        for out in outs:
            out.start()
        for out in (dwo_out, *dwq_out, dx_out, *outs):
            out.wait()

        for r in (RX, RW):
            wait_sends(r)
        for i in far:
            kv_copy(i).wait_send()
        for i in range(chips):
            px(i).wait_send()
        for copy in sent:
            copy.wait_send()

        def sent_dq(h, _):
            @pl.when(h != m)
            def _():
                remote(dq_in.at[h], dq_in.at[h], dq_s.at[h], dq_r.at[h], h).wait_send()

            return 0

        lax.fori_loop(0, n, sent_dq, 0)

    return kernel


def hand_on(*refs):
    count = (len(refs) - 2) // 3
    srcs, dsts, bufs = refs[:count], refs[count : 2 * count], refs[2 * count : 3 * count]
    sems_in, sems_out = refs[3 * count :]
    pieces = []
    for src, dst, buf in zip(srcs, dsts, bufs):
        parts = max(1, src.shape[0] * src.shape[1] // (1 << 16))
        size = src.shape[0] // parts
        for i in range(parts):
            at = pl.ds(i * size, size)
            pieces.append((src.at[at, :], buf.at[at, :], dst.at[at, :]))
    ins = [pltpu.make_async_copy(a, b, sems_in.at[i]) for i, (a, b, _) in enumerate(pieces)]
    outs = [pltpu.make_async_copy(b, c, sems_out.at[i]) for i, (_, b, c) in enumerate(pieces)]
    for copy in ins:
        copy.start()
    for got, put in zip(ins, outs):
        got.wait()
        put.start()
    for put in outs:
        put.wait()


def solution(mesh):
    n = mesh.shape["model"]
    chips = n // 2
    hops = chips // 2
    tok_spec = P(("data", "model"), None)

    def local_step(x_loc, dy_loc, wq_loc, w_key, w_value, wo_loc):
        rows, width = x_loc.shape
        dim = w_key.shape[1]
        cols = width // n
        sds = jax.ShapeDtypeStruct
        vmem = pltpu.VMEM
        dma = pltpu.SemaphoreType.DMA
        arrivals = 2 * hops - 1
        slim = 2 * dim // n
        outs = pl.pallas_call(
            make_kernel(n),
            name="mqa_backward",
            out_shape=(
                sds((rows, width), BF16),
                sds((width, dim), F32),
                sds((cols, dim), F32),
                sds((cols, dim), F32),
                sds((dim, width), F32),
                sds((n, width, dim), BF16),
            ),
            in_specs=[pl.BlockSpec(memory_space=pl.ANY)] * 6,
            out_specs=[pl.BlockSpec(memory_space=pl.ANY)] * 6,
            scratch_shapes=[
                vmem((chips, 2 * rows, width), BF16),
                vmem((chips, 2 * rows, width), BF16),
                vmem((chips, 2 * rows, dim), BF16),
                vmem((2, chips, 2 * rows, dim), BF16),
                vmem((chips, dim, 2 * rows), BF16),
                vmem((chips, dim, 2 * rows), BF16),
                vmem((chips, dim, 2 * rows), BF16),
                vmem((chips, 8, 2 * rows), F32),
                vmem((width, 3 * dim), BF16),
                vmem((dim, width), BF16),
                vmem((width, dim), BF16),
                vmem((2, 2, hops, dim, 2 * rows), F32),
                vmem((chips, 2, hops, slim, 2 * rows), F32),
                vmem((2, hops, 2, hops, slim, 2 * rows), F32),
                vmem((n, rows, dim), BF16),
                vmem((dim, width), F32),
                vmem((dim, width), F32),
                vmem((chips, 2 * rows, 2 * rows), F32),
                vmem((2, width, dim), BF16),
                vmem((dim, 2 * rows), F32),
                vmem((dim, 2 * rows), F32),
                vmem((dim, 2 * rows), BF16),
                vmem((dim, 2 * rows), BF16),
                vmem((2, hops, slim, 2 * rows), BF16),
                vmem((n, slim, rows), BF16),
                vmem((n, slim, cols), F32),
                vmem((n, slim, cols), F32),
                vmem((2, cols, dim), F32),
                dma((3, 2, arrivals)),
                dma((3, 2, arrivals)),
                dma((3, 2 + 2 * arrivals)),
                dma((3, 2 + 2 * arrivals)),
                dma((n,)),
                dma((n,)),
                dma((chips,)),
                dma((chips,)),
                dma((2, hops, 2)),
                dma((2, hops, 2)),
                dma((n,)),
                dma((n,)),
                dma((n,)),
                dma((n,)),
                dma((6 + width // (2 * rows),)),
            ],
            compiler_params=pltpu.CompilerParams(
                collective_id=0, has_side_effects=True, vmem_limit_bytes=67043328
            ),
        )(
            x_loc,
            dy_loc,
            wq_loc.reshape(width, dim),
            w_key,
            w_value,
            wo_loc.reshape(dim, width),
        )
        results = outs[:5]
        any_spec = [pl.BlockSpec(memory_space=pl.ANY)] * 5
        dx, dwq, dwk, dwv, dwo = pl.pallas_call(
            hand_on,
            name="hand_on",
            out_shape=tuple(sds(o.shape, o.dtype) for o in results),
            in_specs=any_spec,
            out_specs=any_spec,
            scratch_shapes=[vmem(o.shape, o.dtype) for o in results] + [dma((64,)), dma((64,))],
        )(*results)
        return dx, dwq.reshape(width, 1, dim), dwk, dwv, dwo.reshape(1, dim, width)

    return jax.shard_map(
        local_step,
        mesh=mesh,
        in_specs=(tok_spec, tok_spec, P(None, "model", None), P(None, None), P(None, None), P("model", None, None)),
        out_specs=(tok_spec, P("data", "model", None), tok_spec, tok_spec, P(("data", "model"), None, None)),
        check_vma=False,
    )
```

```python
import math

import jax
import jax.numpy as jnp
from jax import lax
from jax.experimental import pallas as pl
from jax.experimental.pallas import tpu as pltpu
from jax.sharding import PartitionSpec as P

BF16 = jnp.bfloat16
F32 = jnp.float32
MESH = pl.DeviceIdType.MESH
RX, RY, RW = range(3)


def dot(a, b):
    return jnp.dot(a, b, preferred_element_type=F32)


def dot_nt(a, b):
    return lax.dot_general(a, b, (((1,), (1,)), ((), ())), preferred_element_type=F32)


def dot_tn(a, b):
    return lax.dot_general(a, b, (((0,), (0,)), ((), ())), preferred_element_type=F32)


def rowfold(x, op):
    y = x.reshape(x.shape[0] // 8, 8, x.shape[1])
    return jnp.max(y, axis=0) if op == "max" else jnp.sum(y, axis=0)


def make_kernel(n):
    chips = n // 2
    hops = chips // 2
    last = 2 * (hops - 1)
    arrivals = last + 1

    def kernel(
        x_hbm, dy_hbm, wq_hbm, wk_hbm, wv_hbm, wo_hbm,
        dx_hbm, dwq_hbm, dwk_hbm, dwv_hbm, dwo_hbm, wq_all,
        x_all, dy_all, q_all, kv_all, kt_all, vt_all, o_all, lse, wqkv, wo, wot,
        dkv, part, sums, dq_in, dwqt, dwo_acc, st, wq_st,
        ot, dqt, dot_s, qt_s, thin, kv_rows, dw_out, dw_in, dw_t,
        ring_r, ring_s, pair_r, pair_s, dq_r, dq_s, px_r, px_s, rs_r, rs_s,
        kv_r, kv_s, dw_r, dw_s, loc,
    ):
        rows, width = x_hbm.shape
        dim = wk_hbm.shape[1]
        cols = width // n
        slim = 2 * dim // n
        quarter = chips // 2
        scale = 1.0 / math.sqrt(dim)
        m = lax.axis_index("model")
        c = lax.div(m, 2)
        k = lax.rem(m, 2)
        mate = m + 1 - 2 * k
        nbr = (lax.rem(m + 2, n), lax.rem(m + n - 2, n))

        def remote(src, dst, ssem, rsem, dev):
            return pltpu.make_async_remote_copy(
                src_ref=src, dst_ref=dst, send_sem=ssem, recv_sem=rsem,
                device_id={"model": dev}, device_id_type=MESH,
            )

        bufs = (x_all, dy_all)
        owns = (x_hbm, dy_hbm, wq_hbm)

        def half(ref, h, size, base=0):
            return ref.at[pl.ds(pl.multiple_of(base + h * size, size), size), :]

        def chunk_at(r, blk, h):
            chip = lax.div(blk, 2)
            base = lax.rem(blk, 2) * rows
            if r == RW:
                return half(wq_all.at[blk], h, width // 2)
            return half(bufs[r].at[chip], h, rows // 2, base)

        def own_at(r, h):
            return half(owns[r], h, owns[r].shape[0] // 2)

        def start_own(r):
            for p in (0, 1):
                for d in (0, 1):
                    h = p if d == 0 else 1 - p
                    remote(own_at(r, h), chunk_at(r, m, h), ring_s.at[r, d, p], ring_r.at[r, d, p], nbr[d]).start()
            for h in (0, 1):
                remote(own_at(r, h), chunk_at(r, m, h), pair_s.at[r, h], pair_r.at[r, h], mate).start()

        def service(r, a):
            step = lax.div(a, 2) + 1
            p = lax.rem(a, 2)
            for d in (0, 1):
                blk = lax.rem(m + (n - 2 * step if d == 0 else 2 * step), n)
                chunk = chunk_at(r, blk, p if d == 0 else 1 - p)
                remote(chunk, chunk, ring_s.at[r, d, 0], ring_r.at[r, d, a], nbr[d]).wait_recv()

                @pl.when(a <= last - 2)
                def _():
                    remote(chunk, chunk, ring_s.at[r, d, 2 + a], ring_r.at[r, d, a + 2], nbr[d]).start()

                i = 2 + d * arrivals + a
                remote(chunk, chunk, pair_s.at[r, i], pair_r.at[r, i], mate).start()

        def chip_at(u):
            step = lax.div(u + 1, 2)
            odd = lax.rem(u, 2)
            return lax.rem(c + odd * (chips - step) + (1 - odd) * step, chips)

        def wait_pair(r, u):
            blk = 2 * chip_at(u) + 1 - k

            def wait(h, i):
                chunk = chunk_at(r, blk, h)
                remote(chunk, chunk, pair_s.at[r, 0], pair_r.at[r, i], mate).wait_recv()

            @pl.when(u == 0)
            def _():
                wait(0, 0)
                wait(1, 1)

            @pl.when(u > 0)
            def _():
                d = 1 - lax.rem(u, 2)
                i = 2 + d * arrivals + 2 * (lax.div(u + 1, 2) - 1)
                wait(d, i)
                wait(1 - d, i + 1 + lax.div(u, chips - 1) * last)

        def wait_sends(r):
            chunk = own_at(r, 0)
            for d in (0, 1):
                for i in range(last + 1):
                    remote(chunk, chunk, ring_s.at[r, d, i], ring_r.at[r, d, 0], nbr[d]).wait_send()
            for i in range(2 + 2 * arrivals):
                remote(chunk, chunk, pair_s.at[r, i], pair_r.at[r, 0], mate).wait_send()

        def local(src, dst, i):
            return pltpu.make_async_copy(src, dst, loc.at[i])

        own_rows = pl.ds(pl.multiple_of(k * rows, rows), rows)
        loads = [
            local(x_hbm, x_all.at[c, own_rows, :], 0),
            local(wq_hbm, wqkv.at[:, pl.ds(0, dim)], 1),
            local(wk_hbm, wqkv.at[:, pl.ds(dim, dim)], 2),
            local(wv_hbm, wqkv.at[:, pl.ds(2 * dim, dim)], 3),
            local(wo_hbm, wo, 4),
            local(dy_hbm, dy_all.at[c, own_rows, :], 5),
        ]
        for load in loads:
            load.start()
        barrier = pltpu.get_barrier_semaphore()
        for dev in (*nbr, mate):
            pl.semaphore_signal(barrier, inc=1, device_id={"model": dev}, device_id_type=MESH)
        pl.semaphore_wait(barrier, 3)
        start_own(RX)
        dwqt[...] = jnp.zeros_like(dwqt)
        dwo_acc[...] = jnp.zeros_like(dwo_acc)

        def clear(j, _):
            for kind in (0, 1):
                for hi in (0, 1):
                    dkv[kind, hi, j] = jnp.zeros(dkv.shape[3:], F32)
            return 0

        lax.fori_loop(0, quarter, clear, 0)
        for load in loads:
            load.wait()
        wot[...] = wo[...].T

        def project(ch):
            qkv = dot(x_all[ch], wqkv[...]).astype(BF16)
            q_all[ch] = qkv[:, :dim]
            kv_all[0, ch] = qkv[:, dim : 2 * dim]
            kv_all[1, ch] = qkv[:, 2 * dim :]
            kt_all[ch] = qkv[:, dim : 2 * dim].T
            vt_all[ch] = qkv[:, 2 * dim :].T

        def gathered(u, _):
            @pl.when(u == 1)
            def _():
                service(RX, 0)

            @pl.when((u >= 1) & (u <= last))
            def _():
                service(RX, u)

            @pl.when(u == last - 2)
            def _():
                start_own(RW)

            @pl.when(u == last)
            def _():
                start_own(RY)

            wait_pair(RX, u)
            project(chip_at(u))
            return 0

        lax.fori_loop(0, chips, gathered, 0)

        pair = 2 * rows
        factor = scale * math.log2(math.e)
        halves = [pl.ds(i * rows, rows) for i in (0, 1)]

        def causal(i):
            key = lax.broadcasted_iota(jnp.int32, (rows, pair), 0) + i * rows
            return key <= lax.broadcasted_iota(jnp.int32, (rows, pair), 1)

        def forward(ch):
            qt_s[...] = q_all[ch].T

            def scores(j, top):
                for at in halves:
                    s = dot(kv_all[0, j, at, :], qt_s[...])
                    st[j, at, :] = s
                    top = jnp.maximum(top, rowfold(s, "max"))
                return top

            top = lax.fori_loop(0, ch, scores, jnp.full((8, pair), -jnp.inf, F32))
            for i in (0, 1):
                s = dot(kv_all[0, ch, halves[i], :], qt_s[...])
                s = jnp.where(causal(i), s, -jnp.inf)
                st[ch, halves[i], :] = s
                top = jnp.maximum(top, rowfold(s, "max"))
            top = jnp.max(top, axis=0, keepdims=True)

            def weights(j, total):
                for at in halves:
                    p = jnp.exp2((st[j, at, :] - top) * factor)
                    st[j, at, :] = p
                    total += rowfold(p, "sum")
                return total

            total = lax.fori_loop(0, ch + 1, weights, jnp.zeros((8, pair), F32))
            total = jnp.sum(total, axis=0, keepdims=True)
            lse[ch] = jnp.broadcast_to(top * factor + jnp.log2(total), (8, pair))
            inv = 1.0 / total
            ot[...] = jnp.zeros_like(ot)

            def outputs(j, _):
                ot[...] += dot(vt_all[j], (st[j] * inv).astype(BF16))
                return 0

            lax.fori_loop(0, ch + 1, outputs, 0)
            o_all[ch] = ot[...].astype(BF16)

        def forwarded(u, _):
            @pl.when(u == hops)
            def _():
                service(RW, 1)

            forward(chip_at(u))
            return 0

        service(RW, 0)
        lax.fori_loop(0, chips, forwarded, 0)

        def attend(ch):
            dot_s[...] = dot(dy_all[ch], wot[...]).astype(BF16).T
            qt_s[...] = q_all[ch].T
            row = jnp.sum(dot_s[...].astype(F32) * o_all[ch].astype(F32), axis=0, keepdims=True)
            shift = lse[ch, 0:1, :]
            dqt[...] = jnp.zeros_like(dqt)

            def tile(j, masked):
                add_q = 0.0
                hi, lo = lax.div(j, quarter), lax.rem(j, quarter)
                for i in (0, 1):
                    at = halves[i]
                    s = dot(kv_all[0, j, at, :], qt_s[...])
                    p = jnp.exp2(s * factor - shift)
                    if masked:
                        p = jnp.where(causal(i), p, 0.0)
                    dp = dot(kv_all[1, j, at, :], dot_s[...])
                    g = (p * (dp - row) * scale).astype(BF16)
                    dkv[1, hi, lo, :, at] += dot_nt(dot_s[...], p.astype(BF16))
                    dkv[0, hi, lo, :, at] += dot_nt(qt_s[...], g)
                    add_q += dot(kt_all[j, :, at], g)
                dqt[...] += add_q

            def grads(j, _):
                tile(j, False)
                return 0

            lax.fori_loop(0, ch, grads, 0)
            tile(ch, True)
            dq = dqt[...].astype(BF16)
            q_all[ch] = dq.T
            for t in range(width // pair):
                at = pl.ds(t * pair, pair)
                dwqt[:, at] += dot(dq, x_all[ch, :, at])
                dwo_acc[:, at] += dot(o_all[ch], dy_all[ch, :, at])

        def send_dq(u, i):
            ch = chip_at(u)
            blk = 2 * ch + i

            @pl.when(blk != m)
            def _():
                remote(q_all.at[ch, halves[i], :], dq_in.at[m], dq_s.at[blk], dq_r.at[m], blk).start()

        late = chips - 1

        def attended(u, _):
            @pl.when(u == 1)
            def _():
                for a in range(2, last - 1 - 2):
                    service(RW, a)
                service(RY, 0)

            @pl.when((u >= 1) & (u < last))
            def _():
                service(RY, u)

            @pl.when(u == last - 2)
            def _():
                service(RW, last - 2 - 1)
                service(RW, last - 2 - 0)

            @pl.when(u == chips - 1)
            def _():
                service(RY, last)

            wait_pair(RY, u)
            attend(chip_at(u))

            @pl.when(u < late)
            def _():
                send_dq(u, 0)
                send_dq(u, 1)

            return 0

        lax.fori_loop(0, chips, attended, 0)

        order = [hops]
        for step in range(hops - 1, 0, -1):
            order += [step, -step]
        order.append(0)

        def chip_off(off):
            return lax.rem(c + off + chips, chips)

        def slice_of(dev):
            row = pl.multiple_of(lax.rem(dev, chips) * slim, slim)
            return dkv.at[lax.div(dev, chips), :, :, pl.ds(row, slim), :]

        def px(i):
            chip = chip_off(order[i])
            return remote(slice_of(2 * chip + 1 - k), part.at[chip], px_s.at[i], px_r.at[i], mate)

        for i in range(chips):
            px(i).start()
        dwo_out = local(dwo_acc, dwo_hbm, 0)
        dwo_out.start()
        spare = width // pair
        dwq_out = []
        for t in range(spare):
            at = pl.ds(t * pair, pair)
            staged = st.at[spare + t, :, pl.ds(0, dim)]
            staged[...] = dwqt[:, at].T
            out = local(staged, dwq_hbm.at[at, :], 6 + t)
            out.start()
            dwq_out.append(out)
            st[t, pl.ds(0, rows), :] = jnp.zeros((rows, pair), F32)

        def add_dx(dq, w_ref):
            for t in range(spare):
                st[t, pl.ds(0, rows), :] += dot_nt(dq, w_ref[pl.ds(t * pair, pair), :])

        def head_at(v):
            return 2 * chip_at(lax.div(v, 2)) + lax.rem(k + lax.rem(v, 2), 2)

        def fetch(v):
            slot = lax.rem(v, 2)
            return local(wq_all.at[head_at(v)], wq_st.at[slot], 2 + slot)

        def dx_head(v):
            h = head_at(v)
            fetch(v).wait()
            remote(dq_in.at[h], dq_in.at[h], dq_s.at[h], dq_r.at[h], mate).wait_recv()
            add_dx(dq_in[h], wq_st.at[lax.rem(v, 2)])

        def dx_heads(lo, hi):
            def body(v, _):
                @pl.when(lax.rem(v, 2) == 1)
                def _():
                    wait_pair(RW, lax.div(v, 2))

                fetch(v).start()

                @pl.when(v > 1)
                def _():
                    dx_head(v - 1)

                return 0

            lax.fori_loop(lo, hi, body, 0)

        def gather(i):
            px(i).wait_recv()
            chip = chip_off(order[i])
            part[chip] += slice_of(2 * chip + k)[...]

        def rs(d, t, h, src):
            return remote(src, sums.at[d, t - 1, h], rs_s.at[d, t - 1, h], rs_r.at[d, t - 1, h], nbr[d])

        sent = []

        def hop(t):
            for first in (True, False):
                for d in (0, 1):
                    h = d if first else 1 - d
                    chip = chip_off((hops + 1 - t) * (1 - 2 * d))
                    if t == 1 and not first:
                        continue
                    if t == 1 or (t == 2 and not first):
                        copy = rs(d, t, h, part.at[chip, h])
                    else:
                        held = sums.at[d, t - 2, h]
                        rs(d, t - 1, h, held).wait_recv()
                        held[...] += part[chip, h]
                        copy = rs(d, t, h, held)
                    copy.start()
                    sent.append(copy)

        gather(0)
        hop(1)
        service(RW, last - 1)
        add_dx(q_all[c, own_rows, :], wqkv.at[:, pl.ds(0, dim)])
        dx_heads(1, late + 3)
        service(RW, last)
        for i in range(1, chips):
            gather(i)
        hop(2)
        for t in range(3, hops):
            hop(t)
        dx_heads(late + 3, n - 2)
        hop(hops)

        for h in (0, 1):
            total = part[c, h]
            for d in (0, 1):
                held = sums.at[d, hops - 1, h]
                rs(d, hops, h, held).wait_recv()
                total += held[...]
            thin[h] = total.astype(BF16)

        def tokens_of(dev):
            chip = lax.div(dev, 2)
            at = pl.ds(pl.multiple_of(lax.rem(dev, 2) * rows, rows), rows)
            return thin.at[lax.div(chip, quarter), lax.rem(chip, quarter), :, at]

        def kv_copy(i):
            dev = lax.rem(m + i, n)
            return remote(tokens_of(dev), kv_rows.at[m], kv_s.at[i], kv_r.at[i], dev)

        far = sorted(range(1, n), key=lambda i: -min(i, n - i))
        for i in far:
            kv_copy(i).start()
        send_dq(chips - 1, 0)
        send_dq(chips - 1, 1)
        kv_rows[m] = tokens_of(m)[...]

        def dw_copy(dev):
            return remote(dw_out.at[dev], dw_in.at[m], dw_s.at[dev], dw_r.at[m], dev)

        per = pair // cols

        def key_grads(t, _):
            at = pl.ds(pl.multiple_of(t * pair, pair), pair)
            add = dot(thin[0, 0], x_all[0, :, at])
            for j in range(1, chips):
                add += dot(thin[j // quarter, j % quarter], x_all[j, :, at])
            for i in range(per):
                dw_out[t * per + i] = add[:, i * cols : (i + 1) * cols]
            for i in range(per):
                dev = t * per + i

                @pl.when(dev != m)
                def _():
                    dw_copy(dev).start()

            return 0

        lax.fori_loop(0, width // pair, key_grads, 0)
        dx_heads(n - 2, n)
        dx_head(n - 1)
        for i in far:
            kv_copy(i).wait_recv()
        own_kv = kv_rows[...].reshape(2 * dim, rows).T
        wait_sends(RY)
        for t in range(spare):
            at = pl.ds(t * pair, pair)
            add = dot_nt(own_kv, wqkv[at, pl.ds(dim, 2 * dim)])
            dy_all[0, pl.ds(0, rows), at] = (st[t, pl.ds(0, rows), :] + add).astype(BF16)
        dx_out = local(dy_all.at[0, pl.ds(0, rows), :], dx_hbm, 4)
        dx_out.start()
        dw_in[m] = dw_out[m]

        def arrived(dev, _):
            @pl.when(dev != m)
            def _():
                dw_copy(dev).wait_send()
                remote(dw_in.at[dev], dw_in.at[dev], dw_s.at[dev], dw_r.at[dev], mate).wait_recv()

            return 0

        lax.fori_loop(0, n, arrived, 0)
        turned = dw_in[...].reshape(2 * dim, cols)
        dw_t[0] = turned[:dim].T
        dw_t[1] = turned[dim:].T
        outs = [local(dw_t.at[0], dwk_hbm, 2), local(dw_t.at[1], dwv_hbm, 3)]
        for out in outs:
            out.start()
        for out in (dwo_out, *dwq_out, dx_out, *outs):
            out.wait()

        for r in (RX, RW):
            wait_sends(r)
        for i in far:
            kv_copy(i).wait_send()
        for i in range(chips):
            px(i).wait_send()
        for copy in sent:
            copy.wait_send()

        def sent_dq(h, _):
            @pl.when(h != m)
            def _():
                remote(dq_in.at[h], dq_in.at[h], dq_s.at[h], dq_r.at[h], h).wait_send()

            return 0

        lax.fori_loop(0, n, sent_dq, 0)

    return kernel


def hand_on(*refs):
    count = (len(refs) - 2) // 3
    srcs, dsts, bufs = refs[:count], refs[count : 2 * count], refs[2 * count : 3 * count]
    sems_in, sems_out = refs[3 * count :]
    pieces = []
    for src, dst, buf in zip(srcs, dsts, bufs):
        parts = max(1, src.shape[0] * src.shape[1] // (1 << 16))
        size = src.shape[0] // parts
        for i in range(parts):
            at = pl.ds(i * size, size)
            pieces.append((src.at[at, :], buf.at[at, :], dst.at[at, :]))
    ins = [pltpu.make_async_copy(a, b, sems_in.at[i]) for i, (a, b, _) in enumerate(pieces)]
    outs = [pltpu.make_async_copy(b, c, sems_out.at[i]) for i, (_, b, c) in enumerate(pieces)]
    for copy in ins:
        copy.start()
    for got, put in zip(ins, outs):
        got.wait()
        put.start()
    for put in outs:
        put.wait()


def solution(mesh):
    n = mesh.shape["model"]
    chips = n // 2
    hops = chips // 2
    tok_spec = P(("data", "model"), None)

    def local_step(x_loc, dy_loc, wq_loc, w_key, w_value, wo_loc):
        rows, width = x_loc.shape
        dim = w_key.shape[1]
        cols = width // n
        sds = jax.ShapeDtypeStruct
        vmem = pltpu.VMEM
        dma = pltpu.SemaphoreType.DMA
        arrivals = 2 * hops - 1
        slim = 2 * dim // n
        outs = pl.pallas_call(
            make_kernel(n),
            name="mqa_backward",
            out_shape=(
                sds((rows, width), BF16),
                sds((width, dim), F32),
                sds((cols, dim), F32),
                sds((cols, dim), F32),
                sds((dim, width), F32),
                sds((n, width, dim), BF16),
            ),
            in_specs=[pl.BlockSpec(memory_space=pl.ANY)] * 6,
            out_specs=[pl.BlockSpec(memory_space=pl.ANY)] * 6,
            scratch_shapes=[
                vmem((chips, 2 * rows, width), BF16),
                vmem((chips, 2 * rows, width), BF16),
                vmem((chips, 2 * rows, dim), BF16),
                vmem((2, chips, 2 * rows, dim), BF16),
                vmem((chips, dim, 2 * rows), BF16),
                vmem((chips, dim, 2 * rows), BF16),
                vmem((chips, dim, 2 * rows), BF16),
                vmem((chips, 8, 2 * rows), F32),
                vmem((width, 3 * dim), BF16),
                vmem((dim, width), BF16),
                vmem((width, dim), BF16),
                vmem((2, 2, hops, dim, 2 * rows), F32),
                vmem((chips, 2, hops, slim, 2 * rows), F32),
                vmem((2, hops, 2, hops, slim, 2 * rows), F32),
                vmem((n, rows, dim), BF16),
                vmem((dim, width), F32),
                vmem((dim, width), F32),
                vmem((chips, 2 * rows, 2 * rows), F32),
                vmem((2, width, dim), BF16),
                vmem((dim, 2 * rows), F32),
                vmem((dim, 2 * rows), F32),
                vmem((dim, 2 * rows), BF16),
                vmem((dim, 2 * rows), BF16),
                vmem((2, hops, slim, 2 * rows), BF16),
                vmem((n, slim, rows), BF16),
                vmem((n, slim, cols), F32),
                vmem((n, slim, cols), F32),
                vmem((2, cols, dim), F32),
                dma((3, 2, arrivals)),
                dma((3, 2, arrivals)),
                dma((3, 2 + 2 * arrivals)),
                dma((3, 2 + 2 * arrivals)),
                dma((n,)),
                dma((n,)),
                dma((chips,)),
                dma((chips,)),
                dma((2, hops, 2)),
                dma((2, hops, 2)),
                dma((n,)),
                dma((n,)),
                dma((n,)),
                dma((n,)),
                dma((6 + width // (2 * rows),)),
            ],
            compiler_params=pltpu.CompilerParams(
                collective_id=0, has_side_effects=True, vmem_limit_bytes=67043328
            ),
        )(
            x_loc,
            dy_loc,
            wq_loc.reshape(width, dim),
            w_key,
            w_value,
            wo_loc.reshape(dim, width),
        )
        results = outs[:5]
        any_spec = [pl.BlockSpec(memory_space=pl.ANY)] * 5
        dx, dwq, dwk, dwv, dwo = pl.pallas_call(
            hand_on,
            name="hand_on",
            out_shape=tuple(sds(o.shape, o.dtype) for o in results),
            in_specs=any_spec,
            out_specs=any_spec,
            scratch_shapes=[vmem(o.shape, o.dtype) for o in results] + [dma((64,)), dma((64,))],
        )(*results)
        return dx, dwq.reshape(width, 1, dim), dwk, dwv, dwo.reshape(1, dim, width)

    return jax.shard_map(
        local_step,
        mesh=mesh,
        in_specs=(tok_spec, tok_spec, P(None, "model", None), P(None, None), P(None, None), P("model", None, None)),
        out_specs=(tok_spec, P("data", "model", None), tok_spec, tok_spec, P(("data", "model"), None, None)),
        check_vma=False,
    )
```

```python
import math

import jax
import jax.numpy as jnp
from jax import lax
from jax.experimental import pallas as pl
from jax.experimental.pallas import tpu as pltpu
from jax.sharding import PartitionSpec as P

BF16 = jnp.bfloat16
F32 = jnp.float32
MESH = pl.DeviceIdType.MESH
RX, RY, RW = range(3)


def dot(a, b):
    return jnp.dot(a, b, preferred_element_type=F32)


def dot_nt(a, b):
    return lax.dot_general(a, b, (((1,), (1,)), ((), ())), preferred_element_type=F32)


def dot_tn(a, b):
    return lax.dot_general(a, b, (((0,), (0,)), ((), ())), preferred_element_type=F32)


def rowfold(x, op):
    y = x.reshape(x.shape[0] // 8, 8, x.shape[1])
    return jnp.max(y, axis=0) if op == "max" else jnp.sum(y, axis=0)


def make_kernel(n, groups):
    chips = n // 2
    hops = chips // 2
    last = 2 * (hops - 1)
    arrivals = last + 1

    def kernel(
        x_hbm, dy_hbm, wq_hbm, wk_hbm, wv_hbm, wo_hbm,
        dx_hbm, dwq_hbm, dwk_hbm, dwv_hbm, dwo_hbm, wq_all,
        x_all, dy_all, q_all, kv_all, kt_all, vo_all, lse, wqkv, wot,
        dkv, part, sums, dq_in, dwqt, dwo_acc, st, wq_st,
        dqt, dot_s, qt_s, thin, kv_rows, dw_out, dw_in, dw_t,
        ring_r, ring_s, pair_r, pair_s, dq_r, dq_s, px_r, px_s, rs_r, rs_s,
        kv_r, kv_s, dw_r, dw_s, peer_r, peer_s, loc,
    ):
        rows, width = x_hbm.shape
        dim = wk_hbm.shape[1]
        cols = width // n
        slim = 2 * dim // n
        quarter = chips // 2
        scale = 1.0 / math.sqrt(dim)
        m = lax.axis_index("model")
        g = lax.axis_index("data")
        share = width // groups
        c = lax.div(m, 2)
        k = lax.rem(m, 2)
        mate = m + 1 - 2 * k
        nbr = (lax.rem(m + 2, n), lax.rem(m + n - 2, n))

        def remote(src, dst, ssem, rsem, dev):
            return pltpu.make_async_remote_copy(
                src_ref=src, dst_ref=dst, send_sem=ssem, recv_sem=rsem,
                device_id={"model": dev}, device_id_type=MESH,
            )

        bufs = (x_all, dy_all)
        owns = (x_hbm, dy_hbm, wq_hbm)

        def half(ref, h, size, base=0):
            return ref.at[pl.ds(pl.multiple_of(base + h * size, size), size), :]

        def chunk_at(r, blk, h):
            chip = lax.div(blk, 2)
            base = lax.rem(blk, 2) * rows
            if r == RW:
                return half(wq_all.at[blk], h, share // 2, g * share)
            return half(bufs[r].at[chip], h, rows // 2, base)

        def own_at(r, h):
            if r == RW:
                return half(wq_hbm, h, share // 2, g * share)
            return half(owns[r], h, owns[r].shape[0] // 2)

        def start_own(r):
            for p in (0, 1):
                for d in (0, 1):
                    h = p if d == 0 else 1 - p
                    remote(own_at(r, h), chunk_at(r, m, h), ring_s.at[r, d, p], ring_r.at[r, d, p], nbr[d]).start()
            for h in (0, 1):
                remote(own_at(r, h), chunk_at(r, m, h), pair_s.at[r, h], pair_r.at[r, h], mate).start()

        def service(r, a):
            step = lax.div(a, 2) + 1
            p = lax.rem(a, 2)
            for d in (0, 1):
                blk = lax.rem(m + (n - 2 * step if d == 0 else 2 * step), n)
                chunk = chunk_at(r, blk, p if d == 0 else 1 - p)
                remote(chunk, chunk, ring_s.at[r, d, 0], ring_r.at[r, d, a], nbr[d]).wait_recv()

                @pl.when(a <= last - 2)
                def _():
                    remote(chunk, chunk, ring_s.at[r, d, 2 + a], ring_r.at[r, d, a + 2], nbr[d]).start()

                i = 2 + d * arrivals + a
                remote(chunk, chunk, pair_s.at[r, i], pair_r.at[r, i], mate).start()

        def chip_at(u):
            step = lax.div(u + 1, 2)
            odd = lax.rem(u, 2)
            return lax.rem(c + odd * (chips - step) + (1 - odd) * step, chips)

        def wait_pair(r, u):
            blk = 2 * chip_at(u) + 1 - k

            def wait(h, i):
                chunk = chunk_at(r, blk, h)
                remote(chunk, chunk, pair_s.at[r, 0], pair_r.at[r, i], mate).wait_recv()

            @pl.when(u == 0)
            def _():
                wait(0, 0)
                wait(1, 1)

            @pl.when(u > 0)
            def _():
                d = 1 - lax.rem(u, 2)
                i = 2 + d * arrivals + 2 * (lax.div(u + 1, 2) - 1)
                wait(d, i)
                wait(1 - d, i + 1 + lax.div(u, chips - 1) * last)

        def wait_sends(r):
            chunk = own_at(r, 0)
            for d in (0, 1):
                for i in range(last + 1):
                    remote(chunk, chunk, ring_s.at[r, d, i], ring_r.at[r, d, 0], nbr[d]).wait_send()
            for i in range(2 + 2 * arrivals):
                remote(chunk, chunk, pair_s.at[r, i], pair_r.at[r, 0], mate).wait_send()

        def local(src, dst, i):
            return pltpu.make_async_copy(src, dst, loc.at[i])

        own_rows = pl.ds(pl.multiple_of(k * rows, rows), rows)
        loads = [
            local(x_hbm, x_all.at[c, own_rows, :], 0),
            local(wq_hbm, wqkv.at[:, pl.ds(0, dim)], 1),
            local(wk_hbm, wqkv.at[:, pl.ds(dim, dim)], 2),
            local(wv_hbm, wqkv.at[:, pl.ds(2 * dim, dim)], 3),
            local(dy_hbm, dy_all.at[c, own_rows, :], 5),
        ]
        pair = 2 * rows
        for t in range(width // pair):
            loads.append(local(wo_hbm.at[:, pl.ds(t * pair, pair)], vo_all.at[t], 6 + t))
        for load in loads:
            load.start()
        barrier = pltpu.get_barrier_semaphore()
        for dev in (*nbr, mate):
            pl.semaphore_signal(barrier, inc=1, device_id={"model": dev}, device_id_type=MESH)
        for i in range(1, groups):
            pl.semaphore_signal(barrier, inc=1, device_id={"data": lax.rem(g + i, groups), "model": m}, device_id_type=MESH)
        pl.semaphore_wait(barrier, 2 + groups)
        start_own(RW)
        start_own(RX)
        dwqt[...] = jnp.zeros_like(dwqt)
        dwo_acc[...] = jnp.zeros_like(dwo_acc)

        def clear(j, _):
            for kind in (0, 1):
                for hi in (0, 1):
                    dkv[kind, hi, j] = jnp.zeros(dkv.shape[3:], F32)
            return 0

        lax.fori_loop(0, quarter, clear, 0)
        for load in loads:
            load.wait()
        for t in range(width // pair):
            wot[pl.ds(t * pair, pair), :] = vo_all[t].T

        def rows_at(group):
            return wq_all.at[:, pl.ds(pl.multiple_of(group * share, share), share), :]

        def peer(i):
            there = rows_at(g)
            return pltpu.make_async_remote_copy(
                src_ref=there, dst_ref=there, send_sem=peer_s.at[i], recv_sem=peer_r.at[i],
                device_id={"data": lax.rem(g + i, groups), "model": m}, device_id_type=MESH,
            )

        mine = pl.ds(pl.multiple_of(g * share, share), share)
        own_rows_out = local(wqkv.at[mine, pl.ds(0, dim)], wq_all.at[m, mine, :], 1)
        own_rows_out.start()

        def spread():
            def waited(u, _):
                wait_pair(RW, u)
                return 0

            lax.fori_loop(0, chips, waited, 0)
            own_rows_out.wait()
            for i in range(1, groups):
                peer(i).start()

        def gathered_weights():
            for i in range(1, groups):
                there = rows_at(lax.rem(g + groups - i, groups))
                pltpu.make_async_remote_copy(
                    src_ref=there, dst_ref=there, send_sem=peer_s.at[i], recv_sem=peer_r.at[i],
                    device_id={"data": lax.rem(g + i, groups), "model": m}, device_id_type=MESH,
                ).wait_recv()

        def project(ch):
            qkv = dot(x_all[ch], wqkv[...]).astype(BF16)
            q_all[ch] = qkv[:, :dim]
            kv_all[0, ch] = qkv[:, dim : 2 * dim]
            kv_all[1, ch] = qkv[:, 2 * dim :]
            kt_all[ch] = qkv[:, dim : 2 * dim].T
            vo_all[ch] = qkv[:, 2 * dim :].T

        def gathered(u, _):
            @pl.when(u == 1)
            def _():
                service(RX, 0)

            @pl.when((u >= 1) & (u < hops))
            def _():
                service(RW, 2 * u - 2)
                service(RW, 2 * u - 1)

            @pl.when(u == hops)
            def _():
                service(RW, last)

            @pl.when((u >= 1) & (u <= last))
            def _():
                service(RX, u)

            @pl.when(u == last - 2)
            def _():
                start_own(RY)

            @pl.when(u == hops + 1)
            def _():
                spread()

            wait_pair(RX, u)
            project(chip_at(u))
            return 0

        lax.fori_loop(0, chips, gathered, 0)

        factor = scale * math.log2(math.e)
        halves = [pl.ds(i * rows, rows) for i in (0, 1)]

        def causal(i):
            key = lax.broadcasted_iota(jnp.int32, (rows, pair), 0) + i * rows
            return key <= lax.broadcasted_iota(jnp.int32, (rows, pair), 1)

        def forward(ch):
            qt_s[...] = q_all[ch].T

            def scores(j, top):
                for at in halves:
                    s = dot(kv_all[0, j, at, :], qt_s[...])
                    st[j, at, :] = s
                    top = jnp.maximum(top, rowfold(s, "max"))
                return top

            top = lax.fori_loop(0, ch, scores, jnp.full((8, pair), -jnp.inf, F32))
            for i in (0, 1):
                s = dot(kv_all[0, ch, halves[i], :], qt_s[...])
                s = jnp.where(causal(i), s, -jnp.inf)
                st[ch, halves[i], :] = s
                top = jnp.maximum(top, rowfold(s, "max"))
            top = jnp.max(top, axis=0, keepdims=True)

            def weights(j, total):
                for at in halves:
                    p = jnp.exp2((st[j, at, :] - top) * factor)
                    st[j, at, :] = p
                    total += rowfold(p, "sum")
                return total

            total = lax.fori_loop(0, ch + 1, weights, jnp.zeros((8, pair), F32))
            total = jnp.sum(total, axis=0, keepdims=True)
            lse[ch] = jnp.broadcast_to(top * factor + jnp.log2(total), (8, pair))
            inv = 1.0 / total
            dqt[...] = jnp.zeros_like(dqt)

            def outputs(j, _):
                dqt[...] += dot(vo_all[j], (st[j] * inv).astype(BF16))
                return 0

            lax.fori_loop(0, ch + 1, outputs, 0)
            vo_all[ch] = dqt[...].astype(BF16)

        def forwarded(u, _):
            @pl.when(u == hops)
            def _():
                service(RY, 0)

            forward(chips - 1 - u)
            return 0

        lax.fori_loop(0, chips, forwarded, 0)

        def attend(ch):
            dot_s[...] = dot(dy_all[ch], wot[...]).astype(BF16).T
            qt_s[...] = q_all[ch].T
            row = jnp.sum(dot_s[...].astype(F32) * vo_all[ch].astype(F32), axis=0, keepdims=True)
            shift = lse[ch, 0:1, :]
            dqt[...] = jnp.zeros_like(dqt)

            def tile(j, masked):
                add_q = 0.0
                hi, lo = lax.div(j, quarter), lax.rem(j, quarter)
                for i in (0, 1):
                    at = halves[i]
                    s = dot(kv_all[0, j, at, :], qt_s[...])
                    p = jnp.exp2(s * factor - shift)
                    if masked:
                        p = jnp.where(causal(i), p, 0.0)
                    dp = dot(kv_all[1, j, at, :], dot_s[...])
                    g = (p * (dp - row) * scale).astype(BF16)
                    dkv[1, hi, lo, :, at] += dot_nt(dot_s[...], p.astype(BF16))
                    dkv[0, hi, lo, :, at] += dot_nt(qt_s[...], g)
                    add_q += dot(kt_all[j, :, at], g)
                dqt[...] += add_q

            def grads(j, _):
                tile(j, False)
                return 0

            lax.fori_loop(0, ch, grads, 0)
            tile(ch, True)
            q_all[ch] = dqt[...].astype(BF16).T

        def weight_grads(ch):
            dq = dqt[...].astype(BF16)
            for t in range(width // pair):
                at = pl.ds(t * pair, pair)
                dwqt[:, at] += dot(dq, x_all[ch, :, at])
                dwo_acc[:, at] += dot(vo_all[ch], dy_all[ch, :, at])

        def send_dq(u, i):
            ch = chip_at(u)
            blk = 2 * ch + i

            @pl.when(blk != m)
            def _():
                remote(q_all.at[ch, halves[i], :], dq_in.at[m], dq_s.at[blk], dq_r.at[m], blk).start()

        def attended(u, _):
            @pl.when((u >= 1) & (u < last))
            def _():
                service(RY, u)

            @pl.when(u == chips - 1)
            def _():
                service(RY, last)

            wait_pair(RY, u)
            attend(chip_at(u))

            send_dq(u, 0)
            send_dq(u, 1)

            @pl.when(u < chips - 1)
            def _():
                weight_grads(chip_at(u))

            return 0

        lax.fori_loop(0, chips, attended, 0)

        order = [hops]
        for step in range(hops - 1, 0, -1):
            order += [step, -step]
        order.append(0)

        def chip_off(off):
            return lax.rem(c + off + chips, chips)

        def slice_of(dev):
            row = pl.multiple_of(lax.rem(dev, chips) * slim, slim)
            return dkv.at[lax.div(dev, chips), :, :, pl.ds(row, slim), :]

        def px(i):
            chip = chip_off(order[i])
            return remote(slice_of(2 * chip + 1 - k), part.at[chip], px_s.at[i], px_r.at[i], mate)

        for i in range(chips):
            px(i).start()
        spare = width // pair

        def add_dx(dq, w_ref):
            for t in range(spare):
                st[t, pl.ds(0, rows), :] += dot_nt(dq, w_ref[pl.ds(t * pair, pair), :])

        def head_at(v):
            return 2 * chip_at(lax.div(v, 2)) + lax.rem(k + lax.rem(v, 2), 2)

        def fetch(v):
            slot = lax.rem(v, 2)
            return local(wq_all.at[head_at(v)], wq_st.at[slot], 2 + slot)

        def dx_head(v):
            h = head_at(v)
            fetch(v).wait()
            remote(dq_in.at[h], dq_in.at[h], dq_s.at[h], dq_r.at[h], mate).wait_recv()
            add_dx(dq_in[h], wq_st.at[lax.rem(v, 2)])

        def dx_heads(lo, hi):
            def body(v, _):
                fetch(v).start()

                @pl.when(v > 1)
                def _():
                    dx_head(v - 1)

                return 0

            lax.fori_loop(lo, hi, body, 0)

        def gather(i):
            px(i).wait_recv()
            chip = chip_off(order[i])
            part[chip] += slice_of(2 * chip + k)[...]

        def rs(d, t, h, src):
            return remote(src, sums.at[d, t - 1, h], rs_s.at[d, t - 1, h], rs_r.at[d, t - 1, h], nbr[d])

        sent = []

        def hop(t):
            for first in (True, False):
                for d in (0, 1):
                    h = d if first else 1 - d
                    chip = chip_off((hops + 1 - t) * (1 - 2 * d))
                    if t == 1 and not first:
                        continue
                    if t == 1 or (t == 2 and not first):
                        copy = rs(d, t, h, part.at[chip, h])
                    else:
                        held = sums.at[d, t - 2, h]
                        rs(d, t - 1, h, held).wait_recv()
                        held[...] += part[chip, h]
                        copy = rs(d, t, h, held)
                    copy.start()
                    sent.append(copy)

        gather(0)
        hop(1)
        weight_grads(chip_at(chips - 1))
        for i in range(1, chips):
            gather(i)
        hop(2)
        dwo_out = local(dwo_acc, dwo_hbm, 0)
        dwo_out.start()
        dwq_out = []
        for t in range(spare):
            at = pl.ds(t * pair, pair)
            staged = st.at[spare + t, :, pl.ds(0, dim)]
            staged[...] = dwqt[:, at].T
            out = local(staged, dwq_hbm.at[at, :], 6 + t)
            out.start()
            dwq_out.append(out)
            st[t, pl.ds(0, rows), :] = jnp.zeros((rows, pair), F32)

        add_dx(q_all[c, own_rows, :], wqkv.at[:, pl.ds(0, dim)])
        gathered_weights()
        dx_heads(1, 4)
        done = 4
        for t in range(3, hops + 1):
            hop(t)
            dx_heads(done, done + 4)
            done += 4

        def tokens_of(dev):
            chip = lax.div(dev, 2)
            at = pl.ds(pl.multiple_of(lax.rem(dev, 2) * rows, rows), rows)
            return thin.at[lax.div(chip, quarter), lax.rem(chip, quarter), :, at]

        def kv_copy(dev):
            return remote(tokens_of(dev), kv_rows.at[m], kv_s.at[dev], kv_r.at[m], dev)

        def dw_copy(dev):
            return remote(dw_out.at[dev], dw_in.at[m], dw_s.at[dev], dw_r.at[m], dev)

        per = pair // cols

        def key_grads(h):
            def body(t, _):
                at = pl.ds(pl.multiple_of(t * pair, pair), pair)
                add = dot(thin[h, 0], x_all[h * quarter, :, at])
                for j in range(1, quarter):
                    add += dot(thin[h, j], x_all[h * quarter + j, :, at])
                for i in range(per):
                    dev = t * per + i
                    piece = add[:, i * cols : (i + 1) * cols]
                    dw_out[dev] = piece if h == 0 else dw_out[dev] + piece
                if h == 1:
                    for i in range(per):
                        dev = t * per + i

                        @pl.when(dev != m)
                        def _():
                            dw_copy(dev).start()

                return 0

            lax.fori_loop(0, width // pair, body, 0)

        for h in (0, 1):
            total = part[c, h]
            for d in (0, 1):
                held = sums.at[d, hops - 1, h]
                rs(d, hops, h, held).wait_recv()
                total += held[...]
            thin[h] = total.astype(BF16)

            def send_rows(dev, _):
                @pl.when(dev != m)
                def _():
                    kv_copy(dev).start()

                return 0

            lax.fori_loop(h * n // 2, (h + 1) * n // 2, send_rows, 0)
            key_grads(h)
        kv_rows[m] = tokens_of(m)[...]
        dx_heads(done, n)
        dx_head(n - 1)

        def rows_arrived(dev, _):
            @pl.when(dev != m)
            def _():
                kv_copy(dev).wait_send()
                remote(kv_rows.at[dev], kv_rows.at[dev], kv_s.at[dev], kv_r.at[dev], mate).wait_recv()

            return 0

        lax.fori_loop(0, n, rows_arrived, 0)
        own_kv = kv_rows[...].reshape(2 * dim, rows).T
        wait_sends(RY)
        for t in range(spare):
            at = pl.ds(t * pair, pair)
            add = dot_nt(own_kv, wqkv[at, pl.ds(dim, 2 * dim)])
            dy_all[0, pl.ds(0, rows), at] = (st[t, pl.ds(0, rows), :] + add).astype(BF16)
        dx_out = local(dy_all.at[0, pl.ds(0, rows), :], dx_hbm, 4)
        dx_out.start()
        dw_in[m] = dw_out[m]

        def arrived(dev, _):
            @pl.when(dev != m)
            def _():
                dw_copy(dev).wait_send()
                remote(dw_in.at[dev], dw_in.at[dev], dw_s.at[dev], dw_r.at[dev], mate).wait_recv()

            return 0

        lax.fori_loop(0, n, arrived, 0)
        turned = dw_in[...].reshape(2 * dim, cols)
        dw_t[0] = turned[:dim].T
        dw_t[1] = turned[dim:].T
        outs = [local(dw_t.at[0], dwk_hbm, 2), local(dw_t.at[1], dwv_hbm, 3)]
        for out in outs:
            out.start()
        for out in (dwo_out, *dwq_out, dx_out, *outs):
            out.wait()

        for r in (RX, RW):
            wait_sends(r)
        for i in range(1, groups):
            peer(i).wait_send()
        for i in range(chips):
            px(i).wait_send()
        for copy in sent:
            copy.wait_send()

        def sent_dq(h, _):
            @pl.when(h != m)
            def _():
                remote(dq_in.at[h], dq_in.at[h], dq_s.at[h], dq_r.at[h], h).wait_send()

            return 0

        lax.fori_loop(0, n, sent_dq, 0)

    return kernel


def hand_on(*refs):
    count = (len(refs) - 2) // 3
    srcs, dsts, bufs = refs[:count], refs[count : 2 * count], refs[2 * count : 3 * count]
    sems_in, sems_out = refs[3 * count :]
    pieces = []
    for src, dst, buf in zip(srcs, dsts, bufs):
        parts = max(1, src.shape[0] * src.shape[1] // (1 << 16))
        size = src.shape[0] // parts
        for i in range(parts):
            at = pl.ds(i * size, size)
            pieces.append((src.at[at, :], buf.at[at, :], dst.at[at, :]))
    ins = [pltpu.make_async_copy(a, b, sems_in.at[i]) for i, (a, b, _) in enumerate(pieces)]
    outs = [pltpu.make_async_copy(b, c, sems_out.at[i]) for i, (_, b, c) in enumerate(pieces)]
    for copy in ins:
        copy.start()
    for got, put in zip(ins, outs):
        got.wait()
        put.start()
    for put in outs:
        put.wait()


def solution(mesh):
    n = mesh.shape["model"]
    groups = mesh.shape["data"]
    chips = n // 2
    hops = chips // 2
    tok_spec = P(("data", "model"), None)

    def local_step(x_loc, dy_loc, wq_loc, w_key, w_value, wo_loc):
        rows, width = x_loc.shape
        dim = w_key.shape[1]
        cols = width // n
        sds = jax.ShapeDtypeStruct
        vmem = pltpu.VMEM
        dma = pltpu.SemaphoreType.DMA
        arrivals = 2 * hops - 1
        slim = 2 * dim // n
        outs = pl.pallas_call(
            make_kernel(n, groups),
            name="mqa_backward",
            out_shape=(
                sds((rows, width), BF16),
                sds((width, dim), F32),
                sds((cols, dim), F32),
                sds((cols, dim), F32),
                sds((dim, width), F32),
                sds((n, width, dim), BF16),
            ),
            in_specs=[pl.BlockSpec(memory_space=pl.ANY)] * 6,
            out_specs=[pl.BlockSpec(memory_space=pl.ANY)] * 6,
            scratch_shapes=[
                vmem((chips, 2 * rows, width), BF16),
                vmem((chips, 2 * rows, width), BF16),
                vmem((chips, 2 * rows, dim), BF16),
                vmem((2, chips, 2 * rows, dim), BF16),
                vmem((chips, dim, 2 * rows), BF16),
                vmem((chips, dim, 2 * rows), BF16),
                vmem((chips, 8, 2 * rows), F32),
                vmem((width, 3 * dim), BF16),
                vmem((width, dim), BF16),
                vmem((2, 2, hops, dim, 2 * rows), F32),
                vmem((chips, 2, hops, slim, 2 * rows), F32),
                vmem((2, hops, 2, hops, slim, 2 * rows), F32),
                vmem((n, rows, dim), BF16),
                vmem((dim, width), F32),
                vmem((dim, width), F32),
                vmem((chips, 2 * rows, 2 * rows), F32),
                vmem((2, width, dim), BF16),
                vmem((dim, 2 * rows), F32),
                vmem((dim, 2 * rows), BF16),
                vmem((dim, 2 * rows), BF16),
                vmem((2, hops, slim, 2 * rows), BF16),
                vmem((n, slim, rows), BF16),
                vmem((n, slim, cols), F32),
                vmem((n, slim, cols), F32),
                vmem((2, cols, dim), F32),
                dma((3, 2, arrivals)),
                dma((3, 2, arrivals)),
                dma((3, 2 + 2 * arrivals)),
                dma((3, 2 + 2 * arrivals)),
                dma((n,)),
                dma((n,)),
                dma((chips,)),
                dma((chips,)),
                dma((2, hops, 2)),
                dma((2, hops, 2)),
                dma((n,)),
                dma((n,)),
                dma((n,)),
                dma((n,)),
                dma((groups,)),
                dma((groups,)),
                dma((6 + width // (2 * rows),)),
            ],
            compiler_params=pltpu.CompilerParams(
                collective_id=0, has_side_effects=True, vmem_limit_bytes=67043328
            ),
        )(
            x_loc,
            dy_loc,
            wq_loc.reshape(width, dim),
            w_key,
            w_value,
            wo_loc.reshape(dim, width),
        )
        results = outs[:5]
        any_spec = [pl.BlockSpec(memory_space=pl.ANY)] * 5
        dx, dwq, dwk, dwv, dwo = pl.pallas_call(
            hand_on,
            name="hand_on",
            out_shape=tuple(sds(o.shape, o.dtype) for o in results),
            in_specs=any_spec,
            out_specs=any_spec,
            scratch_shapes=[vmem(o.shape, o.dtype) for o in results] + [dma((64,)), dma((64,))],
        )(*results)
        return dx, dwq.reshape(width, 1, dim), dwk, dwv, dwo.reshape(1, dim, width)

    return jax.shard_map(
        local_step,
        mesh=mesh,
        in_specs=(tok_spec, tok_spec, P(None, "model", None), P(None, None), P(None, None), P("model", None, None)),
        out_specs=(tok_spec, P("data", "model", None), tok_spec, tok_spec, P(("data", "model"), None, None)),
        check_vma=False,
    )
```

```python
import math

import jax
import jax.numpy as jnp
from jax import lax
from jax.experimental import pallas as pl
from jax.experimental.pallas import tpu as pltpu
from jax.sharding import PartitionSpec as P

BF16 = jnp.bfloat16
F32 = jnp.float32
MESH = pl.DeviceIdType.MESH
RX, RY, RW = range(3)


def dot(a, b):
    return jnp.dot(a, b, preferred_element_type=F32)


def dot_nt(a, b):
    return lax.dot_general(a, b, (((1,), (1,)), ((), ())), preferred_element_type=F32)


def dot_tn(a, b):
    return lax.dot_general(a, b, (((0,), (0,)), ((), ())), preferred_element_type=F32)


def rowfold(x, op):
    y = x.reshape(x.shape[0] // 8, 8, x.shape[1])
    return jnp.max(y, axis=0) if op == "max" else jnp.sum(y, axis=0)


def make_kernel(n, groups):
    chips = n // 2
    hops = chips // 2
    last = 2 * (hops - 1)
    arrivals = last + 1

    def kernel(
        x_hbm, dy_hbm, wq_hbm, wk_hbm, wv_hbm, wo_hbm,
        dx_hbm, dwq_hbm, dwk_hbm, dwv_hbm, dwo_hbm, wq_all,
        x_all, dy_all, q_all, kv_all, kt_all, vo_all, lse, wqkv, wot,
        dkv, part, sums, dq_in, dwqt, dwo_acc, st, wq_st,
        dqt, dot_s, qt_s, thin, kv_rows, dw_out, dw_in, dw_t,
        ring_r, ring_s, pair_r, pair_s, dq_r, dq_s, px_r, px_s, rs_r, rs_s,
        kv_r, kv_s, dw_r, dw_s, peer_r, peer_s, loc,
    ):
        rows, width = x_hbm.shape
        dim = wk_hbm.shape[1]
        cols = width // n
        slim = 2 * dim // n
        quarter = chips // 2
        scale = 1.0 / math.sqrt(dim)
        m = lax.axis_index("model")
        g = lax.axis_index("data")
        share = width // groups
        c = lax.div(m, 2)
        k = lax.rem(m, 2)
        mate = m + 1 - 2 * k
        nbr = (lax.rem(m + 2, n), lax.rem(m + n - 2, n))

        def remote(src, dst, ssem, rsem, dev):
            return pltpu.make_async_remote_copy(
                src_ref=src, dst_ref=dst, send_sem=ssem, recv_sem=rsem,
                device_id={"model": dev}, device_id_type=MESH,
            )

        bufs = (x_all, dy_all)
        owns = (x_hbm, dy_hbm, wq_hbm)

        def half(ref, h, size, base=0):
            return ref.at[pl.ds(pl.multiple_of(base + h * size, size), size), :]

        def chunk_at(r, blk, h):
            chip = lax.div(blk, 2)
            base = lax.rem(blk, 2) * rows
            if r == RW:
                return half(wq_all.at[blk], h, share // 2, g * share)
            return half(bufs[r].at[chip], h, rows // 2, base)

        def own_at(r, h):
            if r == RW:
                return half(wq_hbm, h, share // 2, g * share)
            return half(owns[r], h, owns[r].shape[0] // 2)

        def start_own(r):
            for p in (0, 1):
                for d in (0, 1):
                    h = p if d == 0 else 1 - p
                    remote(own_at(r, h), chunk_at(r, m, h), ring_s.at[r, d, p], ring_r.at[r, d, p], nbr[d]).start()
            for h in (0, 1):
                remote(own_at(r, h), chunk_at(r, m, h), pair_s.at[r, h], pair_r.at[r, h], mate).start()

        def service(r, a):
            step = lax.div(a, 2) + 1
            p = lax.rem(a, 2)
            for d in (0, 1):
                blk = lax.rem(m + (n - 2 * step if d == 0 else 2 * step), n)
                chunk = chunk_at(r, blk, p if d == 0 else 1 - p)
                remote(chunk, chunk, ring_s.at[r, d, 0], ring_r.at[r, d, a], nbr[d]).wait_recv()

                @pl.when(a <= last - 2)
                def _():
                    remote(chunk, chunk, ring_s.at[r, d, 2 + a], ring_r.at[r, d, a + 2], nbr[d]).start()

                i = 2 + d * arrivals + a
                remote(chunk, chunk, pair_s.at[r, i], pair_r.at[r, i], mate).start()

        def chip_at(u):
            step = lax.div(u + 1, 2)
            odd = lax.rem(u, 2)
            return lax.rem(c + odd * (chips - step) + (1 - odd) * step, chips)

        def wait_pair(r, u):
            blk = 2 * chip_at(u) + 1 - k

            def wait(h, i):
                chunk = chunk_at(r, blk, h)
                remote(chunk, chunk, pair_s.at[r, 0], pair_r.at[r, i], mate).wait_recv()

            @pl.when(u == 0)
            def _():
                wait(0, 0)
                wait(1, 1)

            @pl.when(u > 0)
            def _():
                d = 1 - lax.rem(u, 2)
                i = 2 + d * arrivals + 2 * (lax.div(u + 1, 2) - 1)
                wait(d, i)
                wait(1 - d, i + 1 + lax.div(u, chips - 1) * last)

        def wait_sends(r):
            chunk = own_at(r, 0)
            for d in (0, 1):
                for i in range(last + 1):
                    remote(chunk, chunk, ring_s.at[r, d, i], ring_r.at[r, d, 0], nbr[d]).wait_send()
            for i in range(2 + 2 * arrivals):
                remote(chunk, chunk, pair_s.at[r, i], pair_r.at[r, 0], mate).wait_send()

        def local(src, dst, i):
            return pltpu.make_async_copy(src, dst, loc.at[i])

        own_rows = pl.ds(pl.multiple_of(k * rows, rows), rows)
        loads = [
            local(x_hbm, x_all.at[c, own_rows, :], 0),
            local(wq_hbm, wqkv.at[:, pl.ds(0, dim)], 1),
            local(wk_hbm, wqkv.at[:, pl.ds(dim, dim)], 2),
            local(wv_hbm, wqkv.at[:, pl.ds(2 * dim, dim)], 3),
            local(dy_hbm, dy_all.at[c, own_rows, :], 5),
        ]
        pair = 2 * rows
        for t in range(width // pair):
            loads.append(local(wo_hbm.at[:, pl.ds(t * pair, pair)], vo_all.at[t], 6 + t))
        for load in loads:
            load.start()
        barrier = pltpu.get_barrier_semaphore()
        for dev in (*nbr, mate):
            pl.semaphore_signal(barrier, inc=1, device_id={"model": dev}, device_id_type=MESH)
        for i in range(1, groups):
            pl.semaphore_signal(barrier, inc=1, device_id={"data": lax.rem(g + i, groups), "model": m}, device_id_type=MESH)
        pl.semaphore_wait(barrier, 2 + groups)
        start_own(RW)
        start_own(RX)
        dwqt[...] = jnp.zeros_like(dwqt)
        dwo_acc[...] = jnp.zeros_like(dwo_acc)

        def clear(j, _):
            for kind in (0, 1):
                for hi in (0, 1):
                    dkv[kind, hi, j] = jnp.zeros(dkv.shape[3:], F32)
            return 0

        lax.fori_loop(0, quarter, clear, 0)
        for load in loads:
            load.wait()
        for t in range(width // pair):
            wot[pl.ds(t * pair, pair), :] = vo_all[t].T

        def rows_at(group):
            return wq_all.at[:, pl.ds(pl.multiple_of(group * share, share), share), :]

        def peer(i):
            there = rows_at(g)
            return pltpu.make_async_remote_copy(
                src_ref=there, dst_ref=there, send_sem=peer_s.at[i], recv_sem=peer_r.at[i],
                device_id={"data": lax.rem(g + i, groups), "model": m}, device_id_type=MESH,
            )

        mine = pl.ds(pl.multiple_of(g * share, share), share)
        own_rows_out = local(wqkv.at[mine, pl.ds(0, dim)], wq_all.at[m, mine, :], 1)
        own_rows_out.start()

        def spread():
            def waited(u, _):
                wait_pair(RW, u)
                return 0

            lax.fori_loop(0, chips, waited, 0)
            own_rows_out.wait()
            for i in range(1, groups):
                peer(i).start()

        def gathered_weights():
            for i in range(1, groups):
                there = rows_at(lax.rem(g + groups - i, groups))
                pltpu.make_async_remote_copy(
                    src_ref=there, dst_ref=there, send_sem=peer_s.at[i], recv_sem=peer_r.at[i],
                    device_id={"data": lax.rem(g + i, groups), "model": m}, device_id_type=MESH,
                ).wait_recv()

        def project(ch):
            qkv = dot(x_all[ch], wqkv[...]).astype(BF16)
            q_all[ch] = qkv[:, :dim]
            kv_all[0, ch] = qkv[:, dim : 2 * dim]
            kv_all[1, ch] = qkv[:, 2 * dim :]
            kt_all[ch] = qkv[:, dim : 2 * dim].T
            vo_all[ch] = qkv[:, 2 * dim :].T

        def gathered(u, _):
            @pl.when(u == 1)
            def _():
                service(RX, 0)

            @pl.when((u >= 1) & (u < hops))
            def _():
                service(RW, 2 * u - 2)
                service(RW, 2 * u - 1)

            @pl.when(u == hops)
            def _():
                service(RW, last)
                spread()

            @pl.when((u >= 1) & (u <= last))
            def _():
                service(RX, u)

            @pl.when(u == last - 2)
            def _():
                start_own(RY)

            wait_pair(RX, u)
            project(chip_at(u))
            return 0

        lax.fori_loop(0, chips, gathered, 0)

        factor = scale * math.log2(math.e)
        halves = [pl.ds(i * rows, rows) for i in (0, 1)]

        def causal(i):
            key = lax.broadcasted_iota(jnp.int32, (rows, pair), 0) + i * rows
            return key <= lax.broadcasted_iota(jnp.int32, (rows, pair), 1)

        def forward(ch):
            qt_s[...] = q_all[ch].T

            def scores(j, top):
                for at in halves:
                    s = dot(kv_all[0, j, at, :], qt_s[...])
                    st[j, at, :] = s
                    top = jnp.maximum(top, rowfold(s, "max"))
                return top

            top = lax.fori_loop(0, ch, scores, jnp.full((8, pair), -jnp.inf, F32))
            for i in (0, 1):
                s = dot(kv_all[0, ch, halves[i], :], qt_s[...])
                s = jnp.where(causal(i), s, -jnp.inf)
                st[ch, halves[i], :] = s
                top = jnp.maximum(top, rowfold(s, "max"))
            top = jnp.max(top, axis=0, keepdims=True)

            def weights(j, total):
                for at in halves:
                    p = jnp.exp2((st[j, at, :] - top) * factor)
                    st[j, at, :] = p
                    total += rowfold(p, "sum")
                return total

            total = lax.fori_loop(0, ch + 1, weights, jnp.zeros((8, pair), F32))
            total = jnp.sum(total, axis=0, keepdims=True)
            lse[ch] = jnp.broadcast_to(top * factor + jnp.log2(total), (8, pair))
            inv = 1.0 / total
            dqt[...] = jnp.zeros_like(dqt)

            def outputs(j, _):
                dqt[...] += dot(vo_all[j], (st[j] * inv).astype(BF16))
                return 0

            lax.fori_loop(0, ch + 1, outputs, 0)
            vo_all[ch] = dqt[...].astype(BF16)

        def forwarded(u, _):
            @pl.when(u == 2)
            def _():
                service(RY, 0)

            @pl.when(u == chips - 2)
            def _():
                service(RY, 1)

            forward(chips - 1 - u)
            return 0

        lax.fori_loop(0, chips, forwarded, 0)

        def attend(ch):
            dot_s[...] = dot(dy_all[ch], wot[...]).astype(BF16).T
            qt_s[...] = q_all[ch].T
            row = jnp.sum(dot_s[...].astype(F32) * vo_all[ch].astype(F32), axis=0, keepdims=True)
            shift = lse[ch, 0:1, :]
            dqt[...] = jnp.zeros_like(dqt)

            def tile(j, masked):
                add_q = 0.0
                hi, lo = lax.div(j, quarter), lax.rem(j, quarter)
                for i in (0, 1):
                    at = halves[i]
                    s = dot(kv_all[0, j, at, :], qt_s[...])
                    p = jnp.exp2(s * factor - shift)
                    if masked:
                        p = jnp.where(causal(i), p, 0.0)
                    dp = dot(kv_all[1, j, at, :], dot_s[...])
                    g = (p * (dp - row) * scale).astype(BF16)
                    dkv[1, hi, lo, :, at] += dot_nt(dot_s[...], p.astype(BF16))
                    dkv[0, hi, lo, :, at] += dot_nt(qt_s[...], g)
                    add_q += dot(kt_all[j, :, at], g)
                dqt[...] += add_q

            def grads(j, _):
                tile(j, False)
                return 0

            lax.fori_loop(0, ch, grads, 0)
            tile(ch, True)
            q_all[ch] = dqt[...].astype(BF16).T

        def weight_grads(ch):
            dq = dqt[...].astype(BF16)
            for t in range(width // pair):
                at = pl.ds(t * pair, pair)
                dwqt[:, at] += dot(dq, x_all[ch, :, at])
                dwo_acc[:, at] += dot(vo_all[ch], dy_all[ch, :, at])

        def send_dq(u, i):
            ch = chip_at(u)
            blk = 2 * ch + i

            @pl.when(blk != m)
            def _():
                remote(q_all.at[ch, halves[i], :], dq_in.at[m], dq_s.at[blk], dq_r.at[m], blk).start()

            @pl.when(blk == m)
            def _():
                dq_in[m] = q_all[ch, halves[i], :]

        spare = width // pair

        def fetch(u, i):
            slot = lax.rem(u, 2)
            dst = wq_st.at[slot, :, pl.ds(i * dim, dim)]
            return local(wq_all.at[2 * chip_at(u) + i], dst, 2 + 2 * slot + i)

        def dx_start(u):
            fetch(u, 0).start()
            fetch(u, 1).start()

        def dx_pair(u):
            dq = []
            for i in (0, 1):
                h = 2 * chip_at(u) + i
                fetch(u, i).wait()

                @pl.when(h != m)
                def _():
                    remote(dq_in.at[h], dq_in.at[h], dq_s.at[h], dq_r.at[h], mate).wait_recv()

                dq.append(dq_in[h])
            dq = jnp.concatenate(dq, axis=1)
            for t in range(spare):
                at = pl.ds(t * pair, pair)
                st[t, pl.ds(0, rows), :] += dot_nt(dq, wq_st[lax.rem(u, 2), at, :])

        def dx_pairs(lo, hi):
            def body(u, _):
                @pl.when(u + 1 < chips)
                def _():
                    dx_start(u + 1)

                dx_pair(u)
                return 0

            lax.fori_loop(lo, hi, body, 0)

        def attended(u, _):
            @pl.when((u >= 2) & (u < last))
            def _():
                service(RY, u)

            @pl.when(u == chips - 1)
            def _():
                service(RY, last)

            wait_pair(RY, u)
            attend(chip_at(u))

            @pl.when(u == chips - 2)
            def _():
                send_dq(chips - 3, 0)
                send_dq(chips - 3, 1)

            @pl.when(u != chips - 3)
            def _():
                send_dq(u, 0)
                send_dq(u, 1)

            @pl.when(u < chips - 1)
            def _():
                weight_grads(chip_at(u))

            return 0

        lax.fori_loop(0, chips, attended, 0)

        order = [hops]
        for step in range(hops - 1, 0, -1):
            order += [step, -step]
        order.append(0)

        def chip_off(off):
            return lax.rem(c + off + chips, chips)

        def slice_of(dev):
            row = pl.multiple_of(lax.rem(dev, chips) * slim, slim)
            return dkv.at[lax.div(dev, chips), :, :, pl.ds(row, slim), :]

        def px(i):
            chip = chip_off(order[i])
            return remote(slice_of(2 * chip + 1 - k), part.at[chip], px_s.at[i], px_r.at[i], mate)

        for i in range(chips):
            px(i).start()

        def gather(i):
            px(i).wait_recv()
            chip = chip_off(order[i])
            part[chip] += slice_of(2 * chip + k)[...]

        def rs(d, t, h, src):
            return remote(src, sums.at[d, t - 1, h], rs_s.at[d, t - 1, h], rs_r.at[d, t - 1, h], nbr[d])

        sent = []

        def hop(t):
            for first in (True, False):
                for d in (0, 1):
                    h = d if first else 1 - d
                    chip = chip_off((hops + 1 - t) * (1 - 2 * d))
                    if t == 1 and not first:
                        continue
                    if t == 1 or (t == 2 and not first):
                        copy = rs(d, t, h, part.at[chip, h])
                    else:
                        held = sums.at[d, t - 2, h]
                        rs(d, t - 1, h, held).wait_recv()
                        held[...] += part[chip, h]
                        copy = rs(d, t, h, held)
                    copy.start()
                    sent.append(copy)

        gather(0)
        hop(1)
        weight_grads(chip_at(chips - 1))
        gathered_weights()
        for t in range(spare):
            st[t, pl.ds(0, rows), :] = jnp.zeros((rows, pair), F32)
        dx_start(0)
        dx_pairs(0, 5)
        for i in range(1, chips):
            gather(i)
        hop(2)
        dwo_out = local(dwo_acc, dwo_hbm, 0)
        dwo_out.start()
        dwq_out = []
        for t in range(spare):
            at = pl.ds(t * pair, pair)
            staged = st.at[spare + t, :, pl.ds(0, dim)]
            staged[...] = dwqt[:, at].T
            out = local(staged, dwq_hbm.at[at, :], 6 + t)
            out.start()
            dwq_out.append(out)

        dx_pairs(5, 6)
        hop(hops - 1)
        dx_pairs(6, 7)
        hop(hops)
        dx_pairs(7, 7)

        def tokens_of(dev):
            chip = lax.div(dev, 2)
            at = pl.ds(pl.multiple_of(lax.rem(dev, 2) * rows, rows), rows)
            return thin.at[lax.div(chip, quarter), lax.rem(chip, quarter), :, at]

        def kv_copy(dev):
            return remote(tokens_of(dev), kv_rows.at[m], kv_s.at[dev], kv_r.at[m], dev)

        def dw_copy(dev):
            return remote(dw_out.at[dev], dw_in.at[m], dw_s.at[dev], dw_r.at[m], dev)

        per = pair // cols

        def key_grads(h):
            def body(t, _):
                at = pl.ds(pl.multiple_of(t * pair, pair), pair)
                add = dot(thin[h, 0], x_all[h * quarter, :, at])
                for j in range(1, quarter):
                    add += dot(thin[h, j], x_all[h * quarter + j, :, at])
                for i in range(per):
                    dev = t * per + i
                    piece = add[:, i * cols : (i + 1) * cols]
                    dw_out[dev] = piece if h == 0 else dw_out[dev] + piece
                if h == 1:
                    for i in range(per):
                        dev = t * per + i

                        @pl.when(dev != m)
                        def _():
                            dw_copy(dev).start()

                return 0

            lax.fori_loop(0, width // pair, body, 0)

        for h in (0, 1):
            total = part[c, h]
            for d in (0, 1):
                held = sums.at[d, hops - 1, h]
                rs(d, hops, h, held).wait_recv()
                total += held[...]
            thin[h] = total.astype(BF16)

            def send_rows(dev, _):
                @pl.when(dev != m)
                def _():
                    kv_copy(dev).start()

                return 0

            lax.fori_loop(h * n // 2, (h + 1) * n // 2, send_rows, 0)
            key_grads(h)
        kv_rows[m] = tokens_of(m)[...]
        dx_pairs(7, chips)

        def rows_arrived(dev, _):
            @pl.when(dev != m)
            def _():
                kv_copy(dev).wait_send()
                remote(kv_rows.at[dev], kv_rows.at[dev], kv_s.at[dev], kv_r.at[dev], mate).wait_recv()

            return 0

        lax.fori_loop(0, n, rows_arrived, 0)
        own_kv = kv_rows[...].reshape(2 * dim, rows).T
        wait_sends(RY)
        for t in range(spare):
            at = pl.ds(t * pair, pair)
            add = dot_nt(own_kv, wqkv[at, pl.ds(dim, 2 * dim)])
            dy_all[0, pl.ds(0, rows), at] = (st[t, pl.ds(0, rows), :] + add).astype(BF16)
        dx_out = local(dy_all.at[0, pl.ds(0, rows), :], dx_hbm, 4)
        dx_out.start()
        dw_in[m] = dw_out[m]

        def arrived(dev, _):
            @pl.when(dev != m)
            def _():
                dw_copy(dev).wait_send()
                remote(dw_in.at[dev], dw_in.at[dev], dw_s.at[dev], dw_r.at[dev], mate).wait_recv()

            return 0

        lax.fori_loop(0, n, arrived, 0)
        turned = dw_in[...].reshape(2 * dim, cols)
        dw_t[0] = turned[:dim].T
        dw_t[1] = turned[dim:].T
        outs = [local(dw_t.at[0], dwk_hbm, 2), local(dw_t.at[1], dwv_hbm, 3)]
        for out in outs:
            out.start()
        for out in (dwo_out, *dwq_out, dx_out, *outs):
            out.wait()

        for r in (RX, RW):
            wait_sends(r)
        for i in range(1, groups):
            peer(i).wait_send()
        for i in range(chips):
            px(i).wait_send()
        for copy in sent:
            copy.wait_send()

        def sent_dq(h, _):
            @pl.when(h != m)
            def _():
                remote(dq_in.at[h], dq_in.at[h], dq_s.at[h], dq_r.at[h], h).wait_send()

            return 0

        lax.fori_loop(0, n, sent_dq, 0)

    return kernel


def hand_on(*refs):
    count = (len(refs) - 2) // 3
    srcs, dsts, bufs = refs[:count], refs[count : 2 * count], refs[2 * count : 3 * count]
    sems_in, sems_out = refs[3 * count :]
    pieces = []
    for src, dst, buf in zip(srcs, dsts, bufs):
        parts = max(1, src.shape[0] * src.shape[1] // (1 << 16))
        size = src.shape[0] // parts
        for i in range(parts):
            at = pl.ds(i * size, size)
            pieces.append((src.at[at, :], buf.at[at, :], dst.at[at, :]))
    ins = [pltpu.make_async_copy(a, b, sems_in.at[i]) for i, (a, b, _) in enumerate(pieces)]
    outs = [pltpu.make_async_copy(b, c, sems_out.at[i]) for i, (_, b, c) in enumerate(pieces)]
    for copy in ins:
        copy.start()
    for got, put in zip(ins, outs):
        got.wait()
        put.start()
    for put in outs:
        put.wait()


def solution(mesh):
    n = mesh.shape["model"]
    groups = mesh.shape["data"]
    chips = n // 2
    hops = chips // 2
    tok_spec = P(("data", "model"), None)

    def local_step(x_loc, dy_loc, wq_loc, w_key, w_value, wo_loc):
        rows, width = x_loc.shape
        dim = w_key.shape[1]
        cols = width // n
        sds = jax.ShapeDtypeStruct
        vmem = pltpu.VMEM
        dma = pltpu.SemaphoreType.DMA
        arrivals = 2 * hops - 1
        slim = 2 * dim // n
        outs = pl.pallas_call(
            make_kernel(n, groups),
            name="mqa_backward",
            out_shape=(
                sds((rows, width), BF16),
                sds((width, dim), F32),
                sds((cols, dim), F32),
                sds((cols, dim), F32),
                sds((dim, width), F32),
                sds((n, width, dim), BF16),
            ),
            in_specs=[pl.BlockSpec(memory_space=pl.ANY)] * 6,
            out_specs=[pl.BlockSpec(memory_space=pl.ANY)] * 6,
            scratch_shapes=[
                vmem((chips, 2 * rows, width), BF16),
                vmem((chips, 2 * rows, width), BF16),
                vmem((chips, 2 * rows, dim), BF16),
                vmem((2, chips, 2 * rows, dim), BF16),
                vmem((chips, dim, 2 * rows), BF16),
                vmem((chips, dim, 2 * rows), BF16),
                vmem((chips, 8, 2 * rows), F32),
                vmem((width, 3 * dim), BF16),
                vmem((width, dim), BF16),
                vmem((2, 2, hops, dim, 2 * rows), F32),
                vmem((chips, 2, hops, slim, 2 * rows), F32),
                vmem((2, hops, 2, hops, slim, 2 * rows), F32),
                vmem((n, rows, dim), BF16),
                vmem((dim, width), F32),
                vmem((dim, width), F32),
                vmem((chips, 2 * rows, 2 * rows), F32),
                vmem((2, width, 2 * dim), BF16),
                vmem((dim, 2 * rows), F32),
                vmem((dim, 2 * rows), BF16),
                vmem((dim, 2 * rows), BF16),
                vmem((2, hops, slim, 2 * rows), BF16),
                vmem((n, slim, rows), BF16),
                vmem((n, slim, cols), F32),
                vmem((n, slim, cols), F32),
                vmem((2, cols, dim), F32),
                dma((3, 2, arrivals)),
                dma((3, 2, arrivals)),
                dma((3, 2 + 2 * arrivals)),
                dma((3, 2 + 2 * arrivals)),
                dma((n,)),
                dma((n,)),
                dma((chips,)),
                dma((chips,)),
                dma((2, hops, 2)),
                dma((2, hops, 2)),
                dma((n,)),
                dma((n,)),
                dma((n,)),
                dma((n,)),
                dma((groups,)),
                dma((groups,)),
                dma((6 + width // (2 * rows),)),
            ],
            compiler_params=pltpu.CompilerParams(
                collective_id=0, has_side_effects=True, vmem_limit_bytes=67043328
            ),
        )(
            x_loc,
            dy_loc,
            wq_loc.reshape(width, dim),
            w_key,
            w_value,
            wo_loc.reshape(dim, width),
        )
        results = outs[:5]
        any_spec = [pl.BlockSpec(memory_space=pl.ANY)] * 5
        dx, dwq, dwk, dwv, dwo = pl.pallas_call(
            hand_on,
            name="hand_on",
            out_shape=tuple(sds(o.shape, o.dtype) for o in results),
            in_specs=any_spec,
            out_specs=any_spec,
            scratch_shapes=[vmem(o.shape, o.dtype) for o in results] + [dma((64,)), dma((64,))],
        )(*results)
        return dx, dwq.reshape(width, 1, dim), dwk, dwv, dwo.reshape(1, dim, width)

    return jax.shard_map(
        local_step,
        mesh=mesh,
        in_specs=(tok_spec, tok_spec, P(None, "model", None), P(None, None), P(None, None), P("model", None, None)),
        out_specs=(tok_spec, P("data", "model", None), tok_spec, tok_spec, P(("data", "model"), None, None)),
        check_vma=False,
    )
```

```python
import math

import jax
import jax.numpy as jnp
from jax import lax
from jax.experimental import pallas as pl
from jax.experimental.pallas import tpu as pltpu
from jax.sharding import PartitionSpec as P

BF16 = jnp.bfloat16
F32 = jnp.float32
MESH = pl.DeviceIdType.MESH
RX, RY, RW = range(3)


def dot(a, b):
    return jnp.dot(a, b, preferred_element_type=F32)


def dot_nt(a, b):
    return lax.dot_general(a, b, (((1,), (1,)), ((), ())), preferred_element_type=F32)


def dot_tn(a, b):
    return lax.dot_general(a, b, (((0,), (0,)), ((), ())), preferred_element_type=F32)


def rowfold(x, op):
    y = x.reshape(x.shape[0] // 8, 8, x.shape[1])
    return jnp.max(y, axis=0) if op == "max" else jnp.sum(y, axis=0)


def make_kernel(n, groups):
    chips = n // 2
    hops = chips // 2
    last = 2 * (hops - 1)
    arrivals = last + 1

    def kernel(
        x_hbm, dy_hbm, wq_hbm, wk_hbm, wv_hbm, wo_hbm,
        dx_hbm, dwq_hbm, dwk_hbm, dwv_hbm, dwo_hbm, wq_all,
        x_all, dy_all, q_all, kv_all, kt_all, vo_all, lse, wqkv, wot,
        dkv, part, sums, dq_in, dwqt, dwo_acc, st, wq_st,
        dqt, dot_s, qt_s, thin, kv_rows, dw_out, dw_in, dw_t,
        ring_r, ring_s, pair_r, pair_s, dq_r, dq_s, px_r, px_s, rs_r, rs_s,
        kv_r, kv_s, dw_r, dw_s, peer_r, peer_s, loc,
    ):
        rows, width = x_hbm.shape
        dim = wk_hbm.shape[1]
        cols = width // n
        slim = 2 * dim // n
        quarter = chips // 2
        scale = 1.0 / math.sqrt(dim)
        m = lax.axis_index("model")
        g = lax.axis_index("data")
        share = width // groups
        c = lax.div(m, 2)
        k = lax.rem(m, 2)
        mate = m + 1 - 2 * k
        nbr = (lax.rem(m + 2, n), lax.rem(m + n - 2, n))

        def remote(src, dst, ssem, rsem, dev):
            return pltpu.make_async_remote_copy(
                src_ref=src, dst_ref=dst, send_sem=ssem, recv_sem=rsem,
                device_id={"model": dev}, device_id_type=MESH,
            )

        bufs = (x_all, dy_all)
        owns = (x_hbm, dy_hbm, wq_hbm)

        def half(ref, h, size, base=0):
            return ref.at[pl.ds(pl.multiple_of(base + h * size, size), size), :]

        def chunk_at(r, blk, h):
            chip = lax.div(blk, 2)
            base = lax.rem(blk, 2) * rows
            if r == RW:
                return half(wq_all.at[blk], h, share // 2, g * share)
            return half(bufs[r].at[chip], h, rows // 2, base)

        def own_at(r, h):
            if r == RW:
                return half(wq_hbm, h, share // 2, g * share)
            return half(owns[r], h, owns[r].shape[0] // 2)

        def start_own(r):
            for p in (0, 1):
                for d in (0, 1):
                    h = p if d == 0 else 1 - p
                    remote(own_at(r, h), chunk_at(r, m, h), ring_s.at[r, d, p], ring_r.at[r, d, p], nbr[d]).start()
            for h in (0, 1):
                remote(own_at(r, h), chunk_at(r, m, h), pair_s.at[r, h], pair_r.at[r, h], mate).start()

        def service(r, a):
            step = lax.div(a, 2) + 1
            p = lax.rem(a, 2)
            for d in (0, 1):
                blk = lax.rem(m + (n - 2 * step if d == 0 else 2 * step), n)
                chunk = chunk_at(r, blk, p if d == 0 else 1 - p)
                remote(chunk, chunk, ring_s.at[r, d, 0], ring_r.at[r, d, a], nbr[d]).wait_recv()

                @pl.when(a <= last - 2)
                def _():
                    remote(chunk, chunk, ring_s.at[r, d, 2 + a], ring_r.at[r, d, a + 2], nbr[d]).start()

                i = 2 + d * arrivals + a
                remote(chunk, chunk, pair_s.at[r, i], pair_r.at[r, i], mate).start()

        def chip_at(u):
            step = lax.div(u + 1, 2)
            odd = lax.rem(u, 2)
            return lax.rem(c + odd * (chips - step) + (1 - odd) * step, chips)

        def wait_pair(r, u):
            blk = 2 * chip_at(u) + 1 - k

            def wait(h, i):
                chunk = chunk_at(r, blk, h)
                remote(chunk, chunk, pair_s.at[r, 0], pair_r.at[r, i], mate).wait_recv()

            @pl.when(u == 0)
            def _():
                wait(0, 0)
                wait(1, 1)

            @pl.when(u > 0)
            def _():
                d = 1 - lax.rem(u, 2)
                i = 2 + d * arrivals + 2 * (lax.div(u + 1, 2) - 1)
                wait(d, i)
                wait(1 - d, i + 1 + lax.div(u, chips - 1) * last)

        def wait_sends(r):
            chunk = own_at(r, 0)
            for d in (0, 1):
                for i in range(last + 1):
                    remote(chunk, chunk, ring_s.at[r, d, i], ring_r.at[r, d, 0], nbr[d]).wait_send()
            for i in range(2 + 2 * arrivals):
                remote(chunk, chunk, pair_s.at[r, i], pair_r.at[r, 0], mate).wait_send()

        def local(src, dst, i):
            return pltpu.make_async_copy(src, dst, loc.at[i])

        own_rows = pl.ds(pl.multiple_of(k * rows, rows), rows)
        loads = [
            local(x_hbm, x_all.at[c, own_rows, :], 0),
            local(wq_hbm, wqkv.at[:, pl.ds(0, dim)], 1),
            local(wk_hbm, wqkv.at[:, pl.ds(dim, dim)], 2),
            local(wv_hbm, wqkv.at[:, pl.ds(2 * dim, dim)], 3),
            local(dy_hbm, dy_all.at[c, own_rows, :], 5),
        ]
        pair = 2 * rows
        for t in range(width // pair):
            loads.append(local(wo_hbm.at[:, pl.ds(t * pair, pair)], vo_all.at[t], 6 + t))
        for load in loads:
            load.start()
        barrier = pltpu.get_barrier_semaphore()
        for dev in (*nbr, mate):
            pl.semaphore_signal(barrier, inc=1, device_id={"model": dev}, device_id_type=MESH)
        for i in range(1, groups):
            pl.semaphore_signal(barrier, inc=1, device_id={"data": lax.rem(g + i, groups), "model": m}, device_id_type=MESH)
        pl.semaphore_wait(barrier, 2 + groups)
        start_own(RW)
        start_own(RX)
        dwqt[...] = jnp.zeros_like(dwqt)
        dwo_acc[...] = jnp.zeros_like(dwo_acc)

        def clear(j, _):
            for kind in (0, 1):
                for hi in (0, 1):
                    dkv[kind, hi, j] = jnp.zeros(dkv.shape[3:], F32)
            return 0

        lax.fori_loop(0, quarter, clear, 0)
        for load in loads:
            load.wait()
        for t in range(width // pair):
            wot[pl.ds(t * pair, pair), :] = vo_all[t].T

        def rows_at(group):
            return wq_all.at[:, pl.ds(pl.multiple_of(group * share, share), share), :]

        def peer(i):
            there = rows_at(g)
            return pltpu.make_async_remote_copy(
                src_ref=there, dst_ref=there, send_sem=peer_s.at[i], recv_sem=peer_r.at[i],
                device_id={"data": lax.rem(g + i, groups), "model": m}, device_id_type=MESH,
            )

        mine = pl.ds(pl.multiple_of(g * share, share), share)
        own_rows_out = local(wqkv.at[mine, pl.ds(0, dim)], wq_all.at[m, mine, :], 1)
        own_rows_out.start()

        def spread():
            def waited(u, _):
                wait_pair(RW, u)
                return 0

            lax.fori_loop(0, chips, waited, 0)
            own_rows_out.wait()
            for i in range(1, groups):
                peer(i).start()

        def gathered_weights():
            for i in range(1, groups):
                there = rows_at(lax.rem(g + groups - i, groups))
                pltpu.make_async_remote_copy(
                    src_ref=there, dst_ref=there, send_sem=peer_s.at[i], recv_sem=peer_r.at[i],
                    device_id={"data": lax.rem(g + i, groups), "model": m}, device_id_type=MESH,
                ).wait_recv()

        def project(ch):
            qkv = dot(x_all[ch], wqkv[...]).astype(BF16)
            q_all[ch] = qkv[:, :dim]
            kv_all[0, ch] = qkv[:, dim : 2 * dim]
            kv_all[1, ch] = qkv[:, 2 * dim :]
            kt_all[ch] = qkv[:, dim : 2 * dim].T
            vo_all[ch] = qkv[:, 2 * dim :].T

        def gathered(u, _):
            @pl.when(u == 1)
            def _():
                service(RX, 0)

            @pl.when((u >= 1) & (u < hops))
            def _():
                service(RW, 2 * u - 2)
                service(RW, 2 * u - 1)

            @pl.when(u == hops)
            def _():
                service(RW, last)
                spread()

            @pl.when((u >= 1) & (u <= last))
            def _():
                service(RX, u)

            @pl.when(u == last - 2)
            def _():
                start_own(RY)

            wait_pair(RX, u)
            project(chip_at(u))
            return 0

        lax.fori_loop(0, chips, gathered, 0)

        factor = scale * math.log2(math.e)
        halves = [pl.ds(i * rows, rows) for i in (0, 1)]

        def causal(i):
            key = lax.broadcasted_iota(jnp.int32, (rows, pair), 0) + i * rows
            return key <= lax.broadcasted_iota(jnp.int32, (rows, pair), 1)

        def forward(ch):
            qt_s[...] = q_all[ch].T

            def scores(j, top):
                for at in halves:
                    s = dot(kv_all[0, j, at, :], qt_s[...])
                    st[j, at, :] = s
                    top = jnp.maximum(top, rowfold(s, "max"))
                return top

            top = lax.fori_loop(0, ch, scores, jnp.full((8, pair), -jnp.inf, F32))
            for i in (0, 1):
                s = dot(kv_all[0, ch, halves[i], :], qt_s[...])
                s = jnp.where(causal(i), s, -jnp.inf)
                st[ch, halves[i], :] = s
                top = jnp.maximum(top, rowfold(s, "max"))
            top = jnp.max(top, axis=0, keepdims=True)

            def weights(j, total):
                for at in halves:
                    p = jnp.exp2((st[j, at, :] - top) * factor)
                    st[j, at, :] = p
                    total += rowfold(p, "sum")
                return total

            total = lax.fori_loop(0, ch + 1, weights, jnp.zeros((8, pair), F32))
            total = jnp.sum(total, axis=0, keepdims=True)
            lse[ch] = jnp.broadcast_to(top * factor + jnp.log2(total), (8, pair))
            inv = 1.0 / total
            dqt[...] = jnp.zeros_like(dqt)

            def outputs(j, _):
                dqt[...] += dot(vo_all[j], (st[j] * inv).astype(BF16))
                return 0

            lax.fori_loop(0, ch + 1, outputs, 0)
            vo_all[ch] = dqt[...].astype(BF16)

        def forwarded(u, _):
            @pl.when(u == 2)
            def _():
                service(RY, 0)

            @pl.when(u == chips - 2)
            def _():
                service(RY, 1)

            forward(chips - 1 - u)
            return 0

        lax.fori_loop(0, chips, forwarded, 0)

        def attend(ch):
            dot_s[...] = dot(dy_all[ch], wot[...]).astype(BF16).T
            qt_s[...] = q_all[ch].T
            row = jnp.sum(dot_s[...].astype(F32) * vo_all[ch].astype(F32), axis=0, keepdims=True)
            shift = lse[ch, 0:1, :]
            dqt[...] = jnp.zeros_like(dqt)

            def tile(j, masked):
                add_q = 0.0
                hi, lo = lax.div(j, quarter), lax.rem(j, quarter)
                step = rows // 2
                for i in (0, 1):
                    ps, gs = [], []
                    for b in (0, 1):
                        at = pl.ds(i * rows + b * step, step)
                        s = dot(kv_all[0, j, at, :], qt_s[...])
                        dp = dot(kv_all[1, j, at, :], dot_s[...])
                        p = jnp.exp2(s * factor - shift)
                        if masked:
                            p = jnp.where(causal(i)[b * step : (b + 1) * step], p, 0.0)
                        ps.append(p.astype(BF16))
                        gs.append((p * (dp - row) * scale).astype(BF16))
                    at = halves[i]
                    g = jnp.concatenate(gs, axis=0)
                    dkv[1, hi, lo, :, at] += dot_nt(dot_s[...], jnp.concatenate(ps, axis=0))
                    dkv[0, hi, lo, :, at] += dot_nt(qt_s[...], g)
                    add_q += dot(kt_all[j, :, at], g)
                dqt[...] += add_q

            def grads(j, _):
                tile(j, False)
                return 0

            lax.fori_loop(0, ch, grads, 0)
            tile(ch, True)
            q_all[ch] = dqt[...].astype(BF16).T

        def weight_grads(ch):
            dq = dqt[...].astype(BF16)
            for t in range(width // pair):
                at = pl.ds(t * pair, pair)
                dwqt[:, at] += dot(dq, x_all[ch, :, at])
                dwo_acc[:, at] += dot(vo_all[ch], dy_all[ch, :, at])

        def send_dq(u, i):
            ch = chip_at(u)
            blk = 2 * ch + i

            @pl.when(blk != m)
            def _():
                remote(q_all.at[ch, halves[i], :], dq_in.at[m], dq_s.at[blk], dq_r.at[m], blk).start()

            @pl.when(blk == m)
            def _():
                dq_in[m] = q_all[ch, halves[i], :]

        spare = width // pair

        def fetch(u, i):
            slot = lax.rem(u, 2)
            dst = wq_st.at[slot, :, pl.ds(i * dim, dim)]
            return local(wq_all.at[2 * chip_at(u) + i], dst, 2 + 2 * slot + i)

        def dx_start(u):
            fetch(u, 0).start()
            fetch(u, 1).start()

        def dx_pair(u):
            dq = []
            for i in (0, 1):
                h = 2 * chip_at(u) + i
                fetch(u, i).wait()

                @pl.when(h != m)
                def _():
                    remote(dq_in.at[h], dq_in.at[h], dq_s.at[h], dq_r.at[h], mate).wait_recv()

                dq.append(dq_in[h])
            dq = jnp.concatenate(dq, axis=1)
            for t in range(spare):
                at = pl.ds(t * pair, pair)
                st[t, pl.ds(0, rows), :] += dot_nt(dq, wq_st[lax.rem(u, 2), at, :])

        def dx_pairs(lo, hi):
            def body(u, _):
                @pl.when(u + 1 < chips)
                def _():
                    dx_start(u + 1)

                dx_pair(u)
                return 0

            lax.fori_loop(lo, hi, body, 0)

        def attended(u, _):
            @pl.when((u >= 2) & (u < last))
            def _():
                service(RY, u)

            @pl.when(u == chips - 1)
            def _():
                service(RY, last)

            wait_pair(RY, u)
            attend(chip_at(u))

            @pl.when(u == chips - 2)
            def _():
                send_dq(chips - 3, 0)
                send_dq(chips - 3, 1)

            @pl.when(u != chips - 3)
            def _():
                send_dq(u, 0)
                send_dq(u, 1)

            @pl.when(u < chips - 1)
            def _():
                weight_grads(chip_at(u))

            return 0

        lax.fori_loop(0, chips, attended, 0)

        order = [hops]
        for step in range(hops - 1, 0, -1):
            order += [step, -step]
        order.append(0)

        def chip_off(off):
            return lax.rem(c + off + chips, chips)

        def slice_of(dev):
            row = pl.multiple_of(lax.rem(dev, chips) * slim, slim)
            return dkv.at[lax.div(dev, chips), :, :, pl.ds(row, slim), :]

        def px(i):
            chip = chip_off(order[i])
            return remote(slice_of(2 * chip + 1 - k), part.at[chip], px_s.at[i], px_r.at[i], mate)

        for i in range(chips):
            px(i).start()

        def gather(i):
            px(i).wait_recv()
            chip = chip_off(order[i])
            part[chip] += slice_of(2 * chip + k)[...]

        few = quarter // 2

        def piece(ref, q):
            return ref.at[q // 2, pl.ds(q % 2 * few, few)]

        def rs(d, t, q, src):
            return remote(src, piece(sums.at[d, t - 1], q), rs_s.at[d, t - 1, q], rs_r.at[d, t - 1, q], nbr[d])

        sent = []

        def hop(t):
            for q in range(4):
                for d in (0, 1):
                    chip = chip_off((hops + 1 - t) * (1 - 2 * d))
                    if t == 1 and q // 2 != d:
                        continue
                    if t == 1 or (t == 2 and q // 2 != d):
                        copy = rs(d, t, q, piece(part.at[chip], q))
                    else:
                        held = piece(sums.at[d, t - 2], q)
                        rs(d, t - 1, q, held).wait_recv()
                        held[...] += piece(part.at[chip], q)[...]
                        copy = rs(d, t, q, held)
                    copy.start()
                    sent.append(copy)

        gather(0)
        hop(1)
        weight_grads(chip_at(chips - 1))
        gathered_weights()
        for t in range(spare):
            st[t, pl.ds(0, rows), :] = jnp.zeros((rows, pair), F32)
        dx_start(0)
        dx_pairs(0, 5)
        for i in range(1, chips):
            gather(i)
        hop(2)
        dwo_out = local(dwo_acc, dwo_hbm, 0)
        dwo_out.start()
        dwq_out = []
        for t in range(spare):
            at = pl.ds(t * pair, pair)
            staged = st.at[spare + t, :, pl.ds(0, dim)]
            staged[...] = dwqt[:, at].T
            out = local(staged, dwq_hbm.at[at, :], 6 + t)
            out.start()
            dwq_out.append(out)

        dx_pairs(5, 6)
        hop(hops - 1)
        dx_pairs(6, 7)
        hop(hops)
        dx_pairs(7, 7)

        def tokens_of(dev):
            chip = lax.div(dev, 2)
            at = pl.ds(pl.multiple_of(lax.rem(dev, 2) * rows, rows), rows)
            return thin.at[lax.div(chip, quarter), lax.rem(chip, quarter), :, at]

        def kv_copy(dev):
            return remote(tokens_of(dev), kv_rows.at[m], kv_s.at[dev], kv_r.at[m], dev)

        def dw_copy(dev):
            return remote(dw_out.at[dev], dw_in.at[m], dw_s.at[dev], dw_r.at[m], dev)

        per = pair // cols

        def key_grads(h):
            def body(t, _):
                at = pl.ds(pl.multiple_of(t * pair, pair), pair)
                add = dot(thin[h, 0], x_all[h * quarter, :, at])
                for j in range(1, quarter):
                    add += dot(thin[h, j], x_all[h * quarter + j, :, at])
                for i in range(per):
                    dev = t * per + i
                    piece = add[:, i * cols : (i + 1) * cols]
                    dw_out[dev] = piece if h == 0 else dw_out[dev] + piece
                if h == 1:
                    for i in range(per):
                        dev = t * per + i

                        @pl.when(dev != m)
                        def _():
                            dw_copy(dev).start()

                return 0

            lax.fori_loop(0, width // pair, body, 0)

        for h in (0, 1):
            total = part[c, h]
            for d in (0, 1):
                for q in (2 * h, 2 * h + 1):
                    rs(d, hops, q, piece(sums.at[d, hops - 1], q)).wait_recv()
                total += sums[d, hops - 1, h]
            thin[h] = total.astype(BF16)

            def send_rows(dev, _):
                @pl.when(dev != m)
                def _():
                    kv_copy(dev).start()

                return 0

            lax.fori_loop(h * n // 2, (h + 1) * n // 2, send_rows, 0)
            key_grads(h)
        kv_rows[m] = tokens_of(m)[...]
        dx_pairs(7, chips)

        def rows_arrived(dev, _):
            @pl.when(dev != m)
            def _():
                kv_copy(dev).wait_send()
                remote(kv_rows.at[dev], kv_rows.at[dev], kv_s.at[dev], kv_r.at[dev], mate).wait_recv()

            return 0

        lax.fori_loop(0, n, rows_arrived, 0)
        own_kv = kv_rows[...].reshape(2 * dim, rows).T
        wait_sends(RY)
        for t in range(spare):
            at = pl.ds(t * pair, pair)
            add = dot_nt(own_kv, wqkv[at, pl.ds(dim, 2 * dim)])
            dy_all[0, pl.ds(0, rows), at] = (st[t, pl.ds(0, rows), :] + add).astype(BF16)
        dx_out = local(dy_all.at[0, pl.ds(0, rows), :], dx_hbm, 4)
        dx_out.start()
        dw_in[m] = dw_out[m]

        def arrived(dev, _):
            @pl.when(dev != m)
            def _():
                dw_copy(dev).wait_send()
                remote(dw_in.at[dev], dw_in.at[dev], dw_s.at[dev], dw_r.at[dev], mate).wait_recv()

            return 0

        lax.fori_loop(0, n, arrived, 0)
        turned = dw_in[...].reshape(2 * dim, cols)
        dw_t[0] = turned[:dim].T
        dw_t[1] = turned[dim:].T
        outs = [local(dw_t.at[0], dwk_hbm, 2), local(dw_t.at[1], dwv_hbm, 3)]
        for out in outs:
            out.start()
        for out in (dwo_out, *dwq_out, dx_out, *outs):
            out.wait()

        for r in (RX, RW):
            wait_sends(r)
        for i in range(1, groups):
            peer(i).wait_send()
        for i in range(chips):
            px(i).wait_send()
        for copy in sent:
            copy.wait_send()

        def sent_dq(h, _):
            @pl.when(h != m)
            def _():
                remote(dq_in.at[h], dq_in.at[h], dq_s.at[h], dq_r.at[h], h).wait_send()

            return 0

        lax.fori_loop(0, n, sent_dq, 0)

    return kernel


def hand_on(*refs):
    count = (len(refs) - 2) // 3
    srcs, dsts, bufs = refs[:count], refs[count : 2 * count], refs[2 * count : 3 * count]
    sems_in, sems_out = refs[3 * count :]
    pieces = []
    for src, dst, buf in zip(srcs, dsts, bufs):
        parts = max(1, src.shape[0] * src.shape[1] // (1 << 17))
        size = src.shape[0] // parts
        for i in range(parts):
            at = pl.ds(i * size, size)
            pieces.append((src.at[at, :], buf.at[at, :], dst.at[at, :]))
    ins = [pltpu.make_async_copy(a, b, sems_in.at[i]) for i, (a, b, _) in enumerate(pieces)]
    outs = [pltpu.make_async_copy(b, c, sems_out.at[i]) for i, (_, b, c) in enumerate(pieces)]
    for copy in ins:
        copy.start()
    for got, put in zip(ins, outs):
        got.wait()
        put.start()
    for put in outs:
        put.wait()


def solution(mesh):
    n = mesh.shape["model"]
    groups = mesh.shape["data"]
    chips = n // 2
    hops = chips // 2
    tok_spec = P(("data", "model"), None)

    def local_step(x_loc, dy_loc, wq_loc, w_key, w_value, wo_loc):
        rows, width = x_loc.shape
        dim = w_key.shape[1]
        cols = width // n
        sds = jax.ShapeDtypeStruct
        vmem = pltpu.VMEM
        dma = pltpu.SemaphoreType.DMA
        arrivals = 2 * hops - 1
        slim = 2 * dim // n
        outs = pl.pallas_call(
            make_kernel(n, groups),
            name="mqa_backward",
            out_shape=(
                sds((rows, width), BF16),
                sds((width, dim), F32),
                sds((cols, dim), F32),
                sds((cols, dim), F32),
                sds((dim, width), F32),
                sds((n, width, dim), BF16),
            ),
            in_specs=[pl.BlockSpec(memory_space=pl.ANY)] * 6,
            out_specs=[pl.BlockSpec(memory_space=pl.ANY)] * 6,
            scratch_shapes=[
                vmem((chips, 2 * rows, width), BF16),
                vmem((chips, 2 * rows, width), BF16),
                vmem((chips, 2 * rows, dim), BF16),
                vmem((2, chips, 2 * rows, dim), BF16),
                vmem((chips, dim, 2 * rows), BF16),
                vmem((chips, dim, 2 * rows), BF16),
                vmem((chips, 8, 2 * rows), F32),
                vmem((width, 3 * dim), BF16),
                vmem((width, dim), BF16),
                vmem((2, 2, hops, dim, 2 * rows), F32),
                vmem((chips, 2, hops, slim, 2 * rows), F32),
                vmem((2, hops, 2, hops, slim, 2 * rows), F32),
                vmem((n, rows, dim), BF16),
                vmem((dim, width), F32),
                vmem((dim, width), F32),
                vmem((chips, 2 * rows, 2 * rows), F32),
                vmem((2, width, 2 * dim), BF16),
                vmem((dim, 2 * rows), F32),
                vmem((dim, 2 * rows), BF16),
                vmem((dim, 2 * rows), BF16),
                vmem((2, hops, slim, 2 * rows), BF16),
                vmem((n, slim, rows), BF16),
                vmem((n, slim, cols), F32),
                vmem((n, slim, cols), F32),
                vmem((2, cols, dim), F32),
                dma((3, 2, arrivals)),
                dma((3, 2, arrivals)),
                dma((3, 2 + 2 * arrivals)),
                dma((3, 2 + 2 * arrivals)),
                dma((n,)),
                dma((n,)),
                dma((chips,)),
                dma((chips,)),
                dma((2, hops, 4)),
                dma((2, hops, 4)),
                dma((n,)),
                dma((n,)),
                dma((n,)),
                dma((n,)),
                dma((groups,)),
                dma((groups,)),
                dma((6 + width // (2 * rows),)),
            ],
            compiler_params=pltpu.CompilerParams(
                collective_id=0, has_side_effects=True, vmem_limit_bytes=67043328
            ),
        )(
            x_loc,
            dy_loc,
            wq_loc.reshape(width, dim),
            w_key,
            w_value,
            wo_loc.reshape(dim, width),
        )
        results = outs[:5]
        any_spec = [pl.BlockSpec(memory_space=pl.ANY)] * 5
        dx, dwq, dwk, dwv, dwo = pl.pallas_call(
            hand_on,
            name="hand_on",
            out_shape=tuple(sds(o.shape, o.dtype) for o in results),
            in_specs=any_spec,
            out_specs=any_spec,
            scratch_shapes=[vmem(o.shape, o.dtype) for o in results] + [dma((64,)), dma((64,))],
        )(*results)
        return dx, dwq.reshape(width, 1, dim), dwk, dwv, dwo.reshape(1, dim, width)

    return jax.shard_map(
        local_step,
        mesh=mesh,
        in_specs=(tok_spec, tok_spec, P(None, "model", None), P(None, None), P(None, None), P("model", None, None)),
        out_specs=(tok_spec, P("data", "model", None), tok_spec, tok_spec, P(("data", "model"), None, None)),
        check_vma=False,
    )
```

```python
import math

import jax
import jax.numpy as jnp
from jax import lax
from jax.experimental import pallas as pl
from jax.experimental.pallas import tpu as pltpu
from jax.sharding import PartitionSpec as P

BF16 = jnp.bfloat16
F32 = jnp.float32
MESH = pl.DeviceIdType.MESH
RX, RY, RW = range(3)


def dot(a, b):
    return jnp.dot(a, b, preferred_element_type=F32)


def dot_nt(a, b):
    return lax.dot_general(a, b, (((1,), (1,)), ((), ())), preferred_element_type=F32)


def dot_tn(a, b):
    return lax.dot_general(a, b, (((0,), (0,)), ((), ())), preferred_element_type=F32)


def rowfold(x, op):
    y = x.reshape(x.shape[0] // 8, 8, x.shape[1])
    return jnp.max(y, axis=0) if op == "max" else jnp.sum(y, axis=0)


def make_kernel(n, groups):
    chips = n // 2
    hops = chips // 2
    last = 2 * (hops - 1)
    arrivals = last + 1

    def kernel(
        x_hbm, dy_hbm, wq_hbm, wk_hbm, wv_hbm, wo_hbm,
        dx_hbm, dwq_hbm, dwk_hbm, dwv_hbm, dwo_hbm, wq_all,
        x_all, dy_all, q_all, kv_all, kt_all, vo_all, soft, wqkv, wot,
        dkv, part, sums, dq_in, dwqt, dwo_acc, st, wq_st,
        dqt, dot_s, qt_s, thin, kv_rows, dw_out, dw_in, dw_t,
        ring_r, ring_s, pair_r, pair_s, dq_r, dq_s, px_r, px_s, rs_r, rs_s,
        kv_r, kv_s, dw_r, dw_s, peer_r, peer_s, loc,
    ):
        rows, width = x_hbm.shape
        dim = wk_hbm.shape[1]
        cols = width // n
        slim = 2 * dim // n
        quarter = chips // 2
        scale = 1.0 / math.sqrt(dim)
        m = lax.axis_index("model")
        g = lax.axis_index("data")
        share = width // groups
        c = lax.div(m, 2)
        k = lax.rem(m, 2)
        mate = m + 1 - 2 * k
        nbr = (lax.rem(m + 2, n), lax.rem(m + n - 2, n))

        def remote(src, dst, ssem, rsem, dev):
            return pltpu.make_async_remote_copy(
                src_ref=src, dst_ref=dst, send_sem=ssem, recv_sem=rsem,
                device_id={"model": dev}, device_id_type=MESH,
            )

        bufs = (x_all, dy_all)
        owns = (x_hbm, dy_hbm, wq_hbm)

        def half(ref, h, size, base=0):
            return ref.at[pl.ds(pl.multiple_of(base + h * size, size), size), :]

        def chunk_at(r, blk, h):
            chip = lax.div(blk, 2)
            base = lax.rem(blk, 2) * rows
            if r == RW:
                return half(wq_all.at[blk], h, share // 2, g * share)
            return half(bufs[r].at[chip], h, rows // 2, base)

        def own_at(r, h):
            if r == RW:
                return half(wq_hbm, h, share // 2, g * share)
            return half(owns[r], h, owns[r].shape[0] // 2)

        def start_own(r):
            for p in (0, 1):
                for d in (0, 1):
                    h = p if d == 0 else 1 - p
                    remote(own_at(r, h), chunk_at(r, m, h), ring_s.at[r, d, p], ring_r.at[r, d, p], nbr[d]).start()
            for h in (0, 1):
                remote(own_at(r, h), chunk_at(r, m, h), pair_s.at[r, h], pair_r.at[r, h], mate).start()

        def service(r, a):
            step = lax.div(a, 2) + 1
            p = lax.rem(a, 2)
            for d in (0, 1):
                blk = lax.rem(m + (n - 2 * step if d == 0 else 2 * step), n)
                chunk = chunk_at(r, blk, p if d == 0 else 1 - p)
                remote(chunk, chunk, ring_s.at[r, d, 0], ring_r.at[r, d, a], nbr[d]).wait_recv()

                @pl.when(a <= last - 2)
                def _():
                    remote(chunk, chunk, ring_s.at[r, d, 2 + a], ring_r.at[r, d, a + 2], nbr[d]).start()

                i = 2 + d * arrivals + a
                remote(chunk, chunk, pair_s.at[r, i], pair_r.at[r, i], mate).start()

        def chip_at(u):
            step = lax.div(u + 1, 2)
            odd = lax.rem(u, 2)
            return lax.rem(c + odd * (chips - step) + (1 - odd) * step, chips)

        def wait_pair(r, u):
            blk = 2 * chip_at(u) + 1 - k

            def wait(h, i):
                chunk = chunk_at(r, blk, h)
                remote(chunk, chunk, pair_s.at[r, 0], pair_r.at[r, i], mate).wait_recv()

            @pl.when(u == 0)
            def _():
                wait(0, 0)
                wait(1, 1)

            @pl.when(u > 0)
            def _():
                d = 1 - lax.rem(u, 2)
                i = 2 + d * arrivals + 2 * (lax.div(u + 1, 2) - 1)
                wait(d, i)
                wait(1 - d, i + 1 + lax.div(u, chips - 1) * last)

        def wait_sends(r):
            chunk = own_at(r, 0)
            for d in (0, 1):
                for i in range(last + 1):
                    remote(chunk, chunk, ring_s.at[r, d, i], ring_r.at[r, d, 0], nbr[d]).wait_send()
            for i in range(2 + 2 * arrivals):
                remote(chunk, chunk, pair_s.at[r, i], pair_r.at[r, 0], mate).wait_send()

        def local(src, dst, i):
            return pltpu.make_async_copy(src, dst, loc.at[i])

        own_rows = pl.ds(pl.multiple_of(k * rows, rows), rows)
        loads = [
            local(x_hbm, x_all.at[c, own_rows, :], 0),
            local(wq_hbm, wqkv.at[:, pl.ds(0, dim)], 1),
            local(wk_hbm, wqkv.at[:, pl.ds(dim, dim)], 2),
            local(wv_hbm, wqkv.at[:, pl.ds(2 * dim, dim)], 3),
            local(dy_hbm, dy_all.at[c, own_rows, :], 5),
        ]
        pair = 2 * rows
        for t in range(width // pair):
            loads.append(local(wo_hbm.at[:, pl.ds(t * pair, pair)], vo_all.at[t], 6 + t))
        for load in loads:
            load.start()
        barrier = pltpu.get_barrier_semaphore()
        for dev in (*nbr, mate):
            pl.semaphore_signal(barrier, inc=1, device_id={"model": dev}, device_id_type=MESH)
        for i in range(1, groups):
            pl.semaphore_signal(barrier, inc=1, device_id={"data": lax.rem(g + i, groups), "model": m}, device_id_type=MESH)
        pl.semaphore_wait(barrier, 2 + groups)
        start_own(RW)
        start_own(RX)
        dwqt[...] = jnp.zeros_like(dwqt)
        dwo_acc[...] = jnp.zeros_like(dwo_acc)

        def clear(j, _):
            for kind in (0, 1):
                for hi in (0, 1):
                    dkv[kind, hi, j] = jnp.zeros(dkv.shape[3:], F32)
            return 0

        lax.fori_loop(0, quarter, clear, 0)
        for load in loads:
            load.wait()
        for t in range(width // pair):
            wot[pl.ds(t * pair, pair), :] = vo_all[t].T

        def rows_at(group):
            return wq_all.at[:, pl.ds(pl.multiple_of(group * share, share), share), :]

        def peer(i):
            there = rows_at(g)
            return pltpu.make_async_remote_copy(
                src_ref=there, dst_ref=there, send_sem=peer_s.at[i], recv_sem=peer_r.at[i],
                device_id={"data": lax.rem(g + i, groups), "model": m}, device_id_type=MESH,
            )

        mine = pl.ds(pl.multiple_of(g * share, share), share)
        own_rows_out = local(wqkv.at[mine, pl.ds(0, dim)], wq_all.at[m, mine, :], 1)
        own_rows_out.start()

        def spread():
            def waited(u, _):
                wait_pair(RW, u)
                return 0

            lax.fori_loop(0, chips, waited, 0)
            own_rows_out.wait()
            for i in range(1, groups):
                peer(i).start()

        def gathered_weights():
            for i in range(1, groups):
                there = rows_at(lax.rem(g + groups - i, groups))
                pltpu.make_async_remote_copy(
                    src_ref=there, dst_ref=there, send_sem=peer_s.at[i], recv_sem=peer_r.at[i],
                    device_id={"data": lax.rem(g + i, groups), "model": m}, device_id_type=MESH,
                ).wait_recv()

        def project(ch):
            qkv = dot(x_all[ch], wqkv[...]).astype(BF16)
            q_all[ch] = qkv[:, :dim]
            kv_all[0, ch] = qkv[:, dim : 2 * dim]
            kv_all[1, ch] = qkv[:, 2 * dim :]
            kt_all[ch] = qkv[:, dim : 2 * dim].T
            vo_all[ch] = qkv[:, 2 * dim :].T

        def gathered(u, _):
            @pl.when(u == 1)
            def _():
                service(RX, 0)

            @pl.when((u >= 1) & (u < hops))
            def _():
                service(RW, 2 * u - 2)
                service(RW, 2 * u - 1)

            @pl.when(u == hops)
            def _():
                service(RW, last)
                spread()

            @pl.when((u >= 1) & (u <= last))
            def _():
                service(RX, u)

            @pl.when(u == last - 2)
            def _():
                start_own(RY)

            wait_pair(RX, u)
            project(chip_at(u))
            return 0

        lax.fori_loop(0, chips, gathered, 0)

        factor = scale * math.log2(math.e)
        halves = [pl.ds(i * rows, rows) for i in (0, 1)]

        def causal(i):
            key = lax.broadcasted_iota(jnp.int32, (rows, pair), 0) + i * rows
            return key <= lax.broadcasted_iota(jnp.int32, (rows, pair), 1)

        def forward(ch):
            qt_s[...] = q_all[ch].T

            def scores(j, top):
                for at in halves:
                    s = dot(kv_all[0, j, at, :], qt_s[...])
                    st[j, at, :] = s
                    top = jnp.maximum(top, rowfold(s, "max"))
                return top

            top = lax.fori_loop(0, ch, scores, jnp.full((8, pair), -jnp.inf, F32))
            for i in (0, 1):
                s = dot(kv_all[0, ch, halves[i], :], qt_s[...])
                s = jnp.where(causal(i), s, -jnp.inf)
                st[ch, halves[i], :] = s
                top = jnp.maximum(top, rowfold(s, "max"))
            top = jnp.max(top, axis=0, keepdims=True)

            def weights(j, total):
                for at in halves:
                    p = jnp.exp2((st[j, at, :] - top) * factor)
                    st[j, at, :] = p
                    total += rowfold(p, "sum")
                return total

            total = lax.fori_loop(0, ch + 1, weights, jnp.zeros((8, pair), F32))
            total = jnp.sum(total, axis=0, keepdims=True)
            inv = 1.0 / total
            soft[ch, 0] = jnp.broadcast_to(top, (8, pair))
            soft[ch, 1] = jnp.broadcast_to(inv, (8, pair))
            dqt[...] = jnp.zeros_like(dqt)

            def outputs(j, _):
                dqt[...] += dot(vo_all[j], (st[j] * inv).astype(BF16))
                return 0

            lax.fori_loop(0, ch + 1, outputs, 0)
            vo_all[ch] = dqt[...].astype(BF16)

        def forwarded(u, _):
            @pl.when(u == 2)
            def _():
                service(RY, 0)

            @pl.when(u == chips - 2)
            def _():
                service(RY, 1)

            forward(chips - 1 - u)
            return 0

        lax.fori_loop(0, chips, forwarded, 0)

        def attend(ch):
            dot_s[...] = dot(dy_all[ch], wot[...]).astype(BF16).T
            qt_s[...] = q_all[ch].T
            row = jnp.sum(dot_s[...].astype(F32) * vo_all[ch].astype(F32), axis=0, keepdims=True)
            top, inv = soft[ch, 0, 0:1, :], soft[ch, 1, 0:1, :]
            dqt[...] = jnp.zeros_like(dqt)

            def tile(j, masked):
                add_q = 0.0
                hi, lo = lax.div(j, quarter), lax.rem(j, quarter)
                step = rows // 2
                for i in (0, 1):
                    ps, gs = [], []
                    for b in (0, 1):
                        at = pl.ds(i * rows + b * step, step)
                        s = dot(kv_all[0, j, at, :], qt_s[...])
                        dp = dot(kv_all[1, j, at, :], dot_s[...])
                        p = jnp.exp2((s - top) * factor) * inv
                        if masked:
                            p = jnp.where(causal(i)[b * step : (b + 1) * step], p, 0.0)
                        ps.append(p.astype(BF16))
                        gs.append((p * (dp - row) * scale).astype(BF16))
                    at = halves[i]
                    g = jnp.concatenate(gs, axis=0)
                    dkv[1, hi, lo, :, at] += dot_nt(dot_s[...], jnp.concatenate(ps, axis=0))
                    dkv[0, hi, lo, :, at] += dot_nt(qt_s[...], g)
                    add_q += dot(kt_all[j, :, at], g)
                dqt[...] += add_q

            def grads(j, _):
                tile(j, False)
                return 0

            lax.fori_loop(0, ch, grads, 0)
            tile(ch, True)
            q_all[ch] = dqt[...].astype(BF16).T

        def weight_grads(ch):
            dq = dqt[...].astype(BF16)
            for t in range(width // pair):
                at = pl.ds(t * pair, pair)
                dwqt[:, at] += dot(dq, x_all[ch, :, at])
                dwo_acc[:, at] += dot(vo_all[ch], dy_all[ch, :, at])

        def send_dq(u, i):
            ch = chip_at(u)
            blk = 2 * ch + i

            @pl.when(blk != m)
            def _():
                remote(q_all.at[ch, halves[i], :], dq_in.at[m], dq_s.at[blk], dq_r.at[m], blk).start()

            @pl.when(blk == m)
            def _():
                dq_in[m] = q_all[ch, halves[i], :]

        spare = width // pair

        def fetch(u, i):
            slot = lax.rem(u, 2)
            dst = wq_st.at[slot, :, pl.ds(i * dim, dim)]
            return local(wq_all.at[2 * chip_at(u) + i], dst, 2 + 2 * slot + i)

        def dx_start(u):
            fetch(u, 0).start()
            fetch(u, 1).start()

        def dx_pair(u):
            dq = []
            for i in (0, 1):
                h = 2 * chip_at(u) + i
                fetch(u, i).wait()

                @pl.when(h != m)
                def _():
                    remote(dq_in.at[h], dq_in.at[h], dq_s.at[h], dq_r.at[h], mate).wait_recv()

                dq.append(dq_in[h])
            dq = jnp.concatenate(dq, axis=1)
            for t in range(spare):
                at = pl.ds(t * pair, pair)
                st[t, pl.ds(0, rows), :] += dot_nt(dq, wq_st[lax.rem(u, 2), at, :])

        def dx_pairs(lo, hi):
            def body(u, _):
                @pl.when(u + 1 < chips)
                def _():
                    dx_start(u + 1)

                dx_pair(u)
                return 0

            lax.fori_loop(lo, hi, body, 0)

        def attended(u, _):
            @pl.when((u >= 2) & (u < last))
            def _():
                service(RY, u)

            @pl.when(u == chips - 1)
            def _():
                service(RY, last)
                send_dq(chips - 3, 0)
                send_dq(chips - 3, 1)

            wait_pair(RY, u)
            attend(chip_at(u))

            @pl.when(u != chips - 3)
            def _():
                send_dq(u, 0)
                send_dq(u, 1)

            @pl.when(u < chips - 1)
            def _():
                weight_grads(chip_at(u))

            return 0

        lax.fori_loop(0, chips, attended, 0)

        order = [hops]
        for step in range(hops - 1, 0, -1):
            order += [step, -step]
        order.append(0)

        def chip_off(off):
            return lax.rem(c + off + chips, chips)

        def slice_of(dev):
            row = pl.multiple_of(lax.rem(dev, chips) * slim, slim)
            return dkv.at[lax.div(dev, chips), :, :, pl.ds(row, slim), :]

        def px(i):
            chip = chip_off(order[i])
            return remote(slice_of(2 * chip + 1 - k), part.at[chip], px_s.at[i], px_r.at[i], mate)

        for i in range(chips):
            px(i).start()

        def gather(i):
            px(i).wait_recv()
            chip = chip_off(order[i])
            part[chip] += slice_of(2 * chip + k)[...]

        few = quarter // 2

        def piece(ref, q):
            return ref.at[q // 2, pl.ds(q % 2 * few, few)]

        def rs(d, t, q, src):
            return remote(src, piece(sums.at[d, t - 1], q), rs_s.at[d, t - 1, q], rs_r.at[d, t - 1, q], nbr[d])

        sent = []

        def hop(t):
            for q in range(4):
                for d in (0, 1):
                    chip = chip_off((hops + 1 - t) * (1 - 2 * d))
                    if t == 1 and q // 2 != d:
                        continue
                    if t == 1 or (t == 2 and q // 2 != d):
                        copy = rs(d, t, q, piece(part.at[chip], q))
                    else:
                        held = piece(sums.at[d, t - 2], q)
                        rs(d, t - 1, q, held).wait_recv()
                        held[...] += piece(part.at[chip], q)[...]
                        copy = rs(d, t, q, held)
                    copy.start()
                    sent.append(copy)

        gather(0)
        hop(1)
        weight_grads(chip_at(chips - 1))
        gathered_weights()
        for t in range(spare):
            st[t, pl.ds(0, rows), :] = jnp.zeros((rows, pair), F32)
        dx_start(0)
        dx_pairs(0, 5)
        for i in range(1, chips):
            gather(i)
        hop(2)
        dwo_out = local(dwo_acc, dwo_hbm, 0)
        dwo_out.start()
        dwq_out = []
        for t in range(spare):
            at = pl.ds(t * pair, pair)
            staged = st.at[spare + t, :, pl.ds(0, dim)]
            staged[...] = dwqt[:, at].T
            out = local(staged, dwq_hbm.at[at, :], 6 + t)
            out.start()
            dwq_out.append(out)

        dx_pairs(5, 6)
        hop(hops - 1)
        dx_pairs(6, 7)
        hop(hops)
        dx_pairs(7, 7)

        def tokens_of(dev):
            chip = lax.div(dev, 2)
            at = pl.ds(pl.multiple_of(lax.rem(dev, 2) * rows, rows), rows)
            return thin.at[lax.div(chip, quarter), lax.rem(chip, quarter), :, at]

        def kv_copy(dev):
            return remote(tokens_of(dev), kv_rows.at[m], kv_s.at[dev], kv_r.at[m], dev)

        def dw_copy(dev):
            return remote(dw_out.at[dev], dw_in.at[m], dw_s.at[dev], dw_r.at[m], dev)

        per = pair // cols

        def key_grads(h):
            def body(t, _):
                at = pl.ds(pl.multiple_of(t * pair, pair), pair)
                add = dot(thin[h, 0], x_all[h * quarter, :, at])
                for j in range(1, quarter):
                    add += dot(thin[h, j], x_all[h * quarter + j, :, at])
                for i in range(per):
                    dev = t * per + i
                    piece = add[:, i * cols : (i + 1) * cols]
                    dw_out[dev] = piece if h == 0 else dw_out[dev] + piece
                if h == 1:
                    for i in range(per):
                        dev = t * per + i

                        @pl.when(dev != m)
                        def _():
                            dw_copy(dev).start()

                return 0

            lax.fori_loop(0, width // pair, body, 0)

        for h in (0, 1):
            total = part[c, h]
            for d in (0, 1):
                for q in (2 * h, 2 * h + 1):
                    rs(d, hops, q, piece(sums.at[d, hops - 1], q)).wait_recv()
                total += sums[d, hops - 1, h]
            thin[h] = total.astype(BF16)

            def send_rows(dev, _):
                @pl.when(dev != m)
                def _():
                    kv_copy(dev).start()

                return 0

            lax.fori_loop(h * n // 2, (h + 1) * n // 2, send_rows, 0)
            key_grads(h)
        kv_rows[m] = tokens_of(m)[...]
        dx_pairs(7, chips)

        def rows_arrived(dev, _):
            @pl.when(dev != m)
            def _():
                kv_copy(dev).wait_send()
                remote(kv_rows.at[dev], kv_rows.at[dev], kv_s.at[dev], kv_r.at[dev], mate).wait_recv()

            return 0

        lax.fori_loop(0, n, rows_arrived, 0)
        own_kv = kv_rows[...].reshape(2 * dim, rows).T
        wait_sends(RY)
        for t in range(spare):
            at = pl.ds(t * pair, pair)
            add = dot_nt(own_kv, wqkv[at, pl.ds(dim, 2 * dim)])
            dy_all[0, pl.ds(0, rows), at] = (st[t, pl.ds(0, rows), :] + add).astype(BF16)
        dx_out = local(dy_all.at[0, pl.ds(0, rows), :], dx_hbm, 4)
        dx_out.start()
        dw_in[m] = dw_out[m]

        def arrived(dev, _):
            @pl.when(dev != m)
            def _():
                dw_copy(dev).wait_send()
                remote(dw_in.at[dev], dw_in.at[dev], dw_s.at[dev], dw_r.at[dev], mate).wait_recv()

            return 0

        lax.fori_loop(0, n, arrived, 0)
        turned = dw_in[...].reshape(2 * dim, cols)
        dw_t[0] = turned[:dim].T
        dw_t[1] = turned[dim:].T
        outs = [local(dw_t.at[0], dwk_hbm, 2), local(dw_t.at[1], dwv_hbm, 3)]
        for out in outs:
            out.start()
        for out in (dwo_out, *dwq_out, dx_out, *outs):
            out.wait()

        for r in (RX, RW):
            wait_sends(r)
        for i in range(1, groups):
            peer(i).wait_send()
        for i in range(chips):
            px(i).wait_send()
        for copy in sent:
            copy.wait_send()

        def sent_dq(h, _):
            @pl.when(h != m)
            def _():
                remote(dq_in.at[h], dq_in.at[h], dq_s.at[h], dq_r.at[h], h).wait_send()

            return 0

        lax.fori_loop(0, n, sent_dq, 0)

    return kernel


def hand_on(*refs):
    count = (len(refs) - 2) // 3
    srcs, dsts, bufs = refs[:count], refs[count : 2 * count], refs[2 * count : 3 * count]
    sems_in, sems_out = refs[3 * count :]
    pieces = []
    for src, dst, buf in zip(srcs, dsts, bufs):
        parts = max(1, src.shape[0] * src.shape[1] // (1 << 17))
        size = src.shape[0] // parts
        for i in range(parts):
            at = pl.ds(i * size, size)
            pieces.append((src.at[at, :], buf.at[at, :], dst.at[at, :]))
    ins = [pltpu.make_async_copy(a, b, sems_in.at[i]) for i, (a, b, _) in enumerate(pieces)]
    outs = [pltpu.make_async_copy(b, c, sems_out.at[i]) for i, (_, b, c) in enumerate(pieces)]
    for copy in ins:
        copy.start()
    for got, put in zip(ins, outs):
        got.wait()
        put.start()
    for put in outs:
        put.wait()


def solution(mesh):
    n = mesh.shape["model"]
    groups = mesh.shape["data"]
    chips = n // 2
    hops = chips // 2
    tok_spec = P(("data", "model"), None)

    def local_step(x_loc, dy_loc, wq_loc, w_key, w_value, wo_loc):
        rows, width = x_loc.shape
        dim = w_key.shape[1]
        cols = width // n
        sds = jax.ShapeDtypeStruct
        vmem = pltpu.VMEM
        dma = pltpu.SemaphoreType.DMA
        arrivals = 2 * hops - 1
        slim = 2 * dim // n
        outs = pl.pallas_call(
            make_kernel(n, groups),
            name="mqa_backward",
            out_shape=(
                sds((rows, width), BF16),
                sds((width, dim), F32),
                sds((cols, dim), F32),
                sds((cols, dim), F32),
                sds((dim, width), F32),
                sds((n, width, dim), BF16),
            ),
            in_specs=[pl.BlockSpec(memory_space=pl.ANY)] * 6,
            out_specs=[pl.BlockSpec(memory_space=pl.ANY)] * 6,
            scratch_shapes=[
                vmem((chips, 2 * rows, width), BF16),
                vmem((chips, 2 * rows, width), BF16),
                vmem((chips, 2 * rows, dim), BF16),
                vmem((2, chips, 2 * rows, dim), BF16),
                vmem((chips, dim, 2 * rows), BF16),
                vmem((chips, dim, 2 * rows), BF16),
                vmem((chips, 2, 8, 2 * rows), F32),
                vmem((width, 3 * dim), BF16),
                vmem((width, dim), BF16),
                vmem((2, 2, hops, dim, 2 * rows), F32),
                vmem((chips, 2, hops, slim, 2 * rows), F32),
                vmem((2, hops, 2, hops, slim, 2 * rows), F32),
                vmem((n, rows, dim), BF16),
                vmem((dim, width), F32),
                vmem((dim, width), F32),
                vmem((chips, 2 * rows, 2 * rows), F32),
                vmem((2, width, 2 * dim), BF16),
                vmem((dim, 2 * rows), F32),
                vmem((dim, 2 * rows), BF16),
                vmem((dim, 2 * rows), BF16),
                vmem((2, hops, slim, 2 * rows), BF16),
                vmem((n, slim, rows), BF16),
                vmem((n, slim, cols), F32),
                vmem((n, slim, cols), F32),
                vmem((2, cols, dim), F32),
                dma((3, 2, arrivals)),
                dma((3, 2, arrivals)),
                dma((3, 2 + 2 * arrivals)),
                dma((3, 2 + 2 * arrivals)),
                dma((n,)),
                dma((n,)),
                dma((chips,)),
                dma((chips,)),
                dma((2, hops, 4)),
                dma((2, hops, 4)),
                dma((n,)),
                dma((n,)),
                dma((n,)),
                dma((n,)),
                dma((groups,)),
                dma((groups,)),
                dma((6 + width // (2 * rows),)),
            ],
            compiler_params=pltpu.CompilerParams(
                collective_id=0, has_side_effects=True, vmem_limit_bytes=67043328
            ),
        )(
            x_loc,
            dy_loc,
            wq_loc.reshape(width, dim),
            w_key,
            w_value,
            wo_loc.reshape(dim, width),
        )
        results = outs[:5]
        any_spec = [pl.BlockSpec(memory_space=pl.ANY)] * 5
        dx, dwq, dwk, dwv, dwo = pl.pallas_call(
            hand_on,
            name="hand_on",
            out_shape=tuple(sds(o.shape, o.dtype) for o in results),
            in_specs=any_spec,
            out_specs=any_spec,
            scratch_shapes=[vmem(o.shape, o.dtype) for o in results] + [dma((64,)), dma((64,))],
        )(*results)
        return dx, dwq.reshape(width, 1, dim), dwk, dwv, dwo.reshape(1, dim, width)

    return jax.shard_map(
        local_step,
        mesh=mesh,
        in_specs=(tok_spec, tok_spec, P(None, "model", None), P(None, None), P(None, None), P("model", None, None)),
        out_specs=(tok_spec, P("data", "model", None), tok_spec, tok_spec, P(("data", "model"), None, None)),
        check_vma=False,
    )
```

```python
import math

import jax
import jax.numpy as jnp
from jax import lax
from jax.experimental import pallas as pl
from jax.experimental.pallas import tpu as pltpu
from jax.sharding import PartitionSpec as P

BF16 = jnp.bfloat16
F32 = jnp.float32
MESH = pl.DeviceIdType.MESH
RX, RY, RW = range(3)


def dot(a, b):
    return jnp.dot(a, b, preferred_element_type=F32)


def dot_nt(a, b):
    return lax.dot_general(a, b, (((1,), (1,)), ((), ())), preferred_element_type=F32)


def dot_tn(a, b):
    return lax.dot_general(a, b, (((0,), (0,)), ((), ())), preferred_element_type=F32)


def rowfold(x, op):
    y = x.reshape(x.shape[0] // 8, 8, x.shape[1])
    return jnp.max(y, axis=0) if op == "max" else jnp.sum(y, axis=0)


def make_kernel(n, groups):
    chips = n // 2
    hops = chips // 2
    last = 2 * (hops - 1)
    arrivals = last + 1

    def kernel(
        x_hbm, dy_hbm, wq_hbm, wk_hbm, wv_hbm, wo_hbm,
        dx_hbm, dwq_hbm, dwk_hbm, dwv_hbm, dwo_hbm, wq_all,
        x_all, dy_all, q_all, kv_all, kt_all, vo_all, soft, wqkv, wot,
        dkv, part, sums, dq_in, dwqt, dwo_acc, st, wq_st,
        dqt, dot_s, qt_s, thin, kv_rows, dw_out, dw_in, dw_t,
        ring_r, ring_s, pair_r, pair_s, dq_r, dq_s, px_r, px_s, rs_r, rs_s,
        kv_r, kv_s, dw_r, dw_s, peer_r, peer_s, loc,
    ):
        rows, width = x_hbm.shape
        dim = wk_hbm.shape[1]
        cols = width // n
        slim = 2 * dim // n
        quarter = chips // 2
        scale = 1.0 / math.sqrt(dim)
        m = lax.axis_index("model")
        g = lax.axis_index("data")
        share = width // groups
        c = lax.div(m, 2)
        k = lax.rem(m, 2)
        mate = m + 1 - 2 * k
        nbr = (lax.rem(m + 2, n), lax.rem(m + n - 2, n))

        def remote(src, dst, ssem, rsem, dev):
            return pltpu.make_async_remote_copy(
                src_ref=src, dst_ref=dst, send_sem=ssem, recv_sem=rsem,
                device_id={"model": dev}, device_id_type=MESH,
            )

        bufs = (x_all, dy_all)
        owns = (x_hbm, dy_hbm, wq_hbm)

        def half(ref, h, size, base=0):
            return ref.at[pl.ds(pl.multiple_of(base + h * size, size), size), :]

        def chunk_at(r, blk, h):
            chip = lax.div(blk, 2)
            base = lax.rem(blk, 2) * rows
            if r == RW:
                return half(wq_all.at[blk], h, share // 2, g * share)
            return half(bufs[r].at[chip], h, rows // 2, base)

        def own_at(r, h):
            if r == RW:
                return half(wq_hbm, h, share // 2, g * share)
            return half(owns[r], h, owns[r].shape[0] // 2)

        def start_own(r):
            for p in (0, 1):
                for d in (0, 1):
                    h = p if d == 0 else 1 - p
                    remote(own_at(r, h), chunk_at(r, m, h), ring_s.at[r, d, p], ring_r.at[r, d, p], nbr[d]).start()
            for h in (0, 1):
                remote(own_at(r, h), chunk_at(r, m, h), pair_s.at[r, h], pair_r.at[r, h], mate).start()

        def service(r, a):
            step = lax.div(a, 2) + 1
            p = lax.rem(a, 2)
            for d in (0, 1):
                blk = lax.rem(m + (n - 2 * step if d == 0 else 2 * step), n)
                chunk = chunk_at(r, blk, p if d == 0 else 1 - p)
                remote(chunk, chunk, ring_s.at[r, d, 0], ring_r.at[r, d, a], nbr[d]).wait_recv()

                @pl.when(a <= last - 2)
                def _():
                    remote(chunk, chunk, ring_s.at[r, d, 2 + a], ring_r.at[r, d, a + 2], nbr[d]).start()

                i = 2 + d * arrivals + a
                remote(chunk, chunk, pair_s.at[r, i], pair_r.at[r, i], mate).start()

        def chip_at(u):
            step = lax.div(u + 1, 2)
            odd = lax.rem(u, 2)
            return lax.rem(c + odd * (chips - step) + (1 - odd) * step, chips)

        def wait_pair(r, u):
            blk = 2 * chip_at(u) + 1 - k

            def wait(h, i):
                chunk = chunk_at(r, blk, h)
                remote(chunk, chunk, pair_s.at[r, 0], pair_r.at[r, i], mate).wait_recv()

            @pl.when(u == 0)
            def _():
                wait(0, 0)
                wait(1, 1)

            @pl.when(u > 0)
            def _():
                d = 1 - lax.rem(u, 2)
                i = 2 + d * arrivals + 2 * (lax.div(u + 1, 2) - 1)
                wait(d, i)
                wait(1 - d, i + 1 + lax.div(u, chips - 1) * last)

        def wait_sends(r):
            chunk = own_at(r, 0)
            for d in (0, 1):
                for i in range(last + 1):
                    remote(chunk, chunk, ring_s.at[r, d, i], ring_r.at[r, d, 0], nbr[d]).wait_send()
            for i in range(2 + 2 * arrivals):
                remote(chunk, chunk, pair_s.at[r, i], pair_r.at[r, 0], mate).wait_send()

        def local(src, dst, i):
            return pltpu.make_async_copy(src, dst, loc.at[i])

        own_rows = pl.ds(pl.multiple_of(k * rows, rows), rows)
        loads = [
            local(x_hbm, x_all.at[c, own_rows, :], 0),
            local(wq_hbm, wqkv.at[:, pl.ds(0, dim)], 1),
            local(wk_hbm, wqkv.at[:, pl.ds(dim, dim)], 2),
            local(wv_hbm, wqkv.at[:, pl.ds(2 * dim, dim)], 3),
            local(dy_hbm, dy_all.at[c, own_rows, :], 5),
        ]
        pair = 2 * rows
        for t in range(width // pair):
            loads.append(local(wo_hbm.at[:, pl.ds(t * pair, pair)], vo_all.at[t], 6 + t))
        for load in loads:
            load.start()
        barrier = pltpu.get_barrier_semaphore()
        for dev in (*nbr, mate):
            pl.semaphore_signal(barrier, inc=1, device_id={"model": dev}, device_id_type=MESH)
        for i in range(1, groups):
            pl.semaphore_signal(barrier, inc=1, device_id={"data": lax.rem(g + i, groups), "model": m}, device_id_type=MESH)
        pl.semaphore_wait(barrier, 2 + groups)
        start_own(RW)
        start_own(RX)
        dwqt[...] = jnp.zeros_like(dwqt)
        dwo_acc[...] = jnp.zeros_like(dwo_acc)

        def clear(j, _):
            for kind in (0, 1):
                for hi in (0, 1):
                    dkv[kind, hi, j] = jnp.zeros(dkv.shape[3:], F32)
            return 0

        lax.fori_loop(0, quarter, clear, 0)
        for load in loads:
            load.wait()
        for t in range(width // pair):
            wot[pl.ds(t * pair, pair), :] = vo_all[t].T

        def rows_at(group):
            return wq_all.at[:, pl.ds(pl.multiple_of(group * share, share), share), :]

        def peer(i):
            there = rows_at(g)
            return pltpu.make_async_remote_copy(
                src_ref=there, dst_ref=there, send_sem=peer_s.at[i], recv_sem=peer_r.at[i],
                device_id={"data": lax.rem(g + i, groups), "model": m}, device_id_type=MESH,
            )

        mine = pl.ds(pl.multiple_of(g * share, share), share)
        own_rows_out = local(wqkv.at[mine, pl.ds(0, dim)], wq_all.at[m, mine, :], 1)
        own_rows_out.start()

        def spread():
            def waited(u, _):
                wait_pair(RW, u)
                return 0

            lax.fori_loop(0, chips, waited, 0)
            own_rows_out.wait()
            for i in range(1, groups):
                peer(i).start()

        def gathered_weights():
            for i in range(1, groups):
                there = rows_at(lax.rem(g + groups - i, groups))
                pltpu.make_async_remote_copy(
                    src_ref=there, dst_ref=there, send_sem=peer_s.at[i], recv_sem=peer_r.at[i],
                    device_id={"data": lax.rem(g + i, groups), "model": m}, device_id_type=MESH,
                ).wait_recv()

        def project(ch):
            qkv = dot(x_all[ch], wqkv[...]).astype(BF16)
            q_all[ch] = qkv[:, :dim]
            kv_all[0, ch] = qkv[:, dim : 2 * dim]
            kv_all[1, ch] = qkv[:, 2 * dim :]
            kt_all[ch] = qkv[:, dim : 2 * dim].T
            vo_all[ch] = qkv[:, 2 * dim :].T

        def gathered(u, _):
            @pl.when(u == 1)
            def _():
                service(RX, 0)

            @pl.when((u >= 1) & (u < hops))
            def _():
                service(RW, 2 * u - 2)
                service(RW, 2 * u - 1)

            @pl.when(u == hops)
            def _():
                service(RW, last)
                spread()

            @pl.when((u >= 1) & (u <= last))
            def _():
                service(RX, u)

            @pl.when(u == last - 2)
            def _():
                start_own(RY)

            wait_pair(RX, u)
            project(chip_at(u))
            return 0

        lax.fori_loop(0, chips, gathered, 0)

        factor = scale * math.log2(math.e)
        halves = [pl.ds(i * rows, rows) for i in (0, 1)]

        def causal(i):
            key = lax.broadcasted_iota(jnp.int32, (rows, pair), 0) + i * rows
            return key <= lax.broadcasted_iota(jnp.int32, (rows, pair), 1)

        def forward(ch):
            qt_s[...] = q_all[ch].T

            def scores(j, top):
                for at in halves:
                    s = dot(kv_all[0, j, at, :], qt_s[...])
                    st[j, at, :] = s
                    top = jnp.maximum(top, rowfold(s, "max"))
                return top

            top = lax.fori_loop(0, ch, scores, jnp.full((8, pair), -jnp.inf, F32))
            for i in (0, 1):
                s = dot(kv_all[0, ch, halves[i], :], qt_s[...])
                s = jnp.where(causal(i), s, -jnp.inf)
                st[ch, halves[i], :] = s
                top = jnp.maximum(top, rowfold(s, "max"))
            top = jnp.max(top, axis=0, keepdims=True)

            def weights(j, total):
                for at in halves:
                    p = jnp.exp2((st[j, at, :] - top) * factor)
                    st[j, at, :] = p
                    total += rowfold(p, "sum")
                return total

            total = lax.fori_loop(0, ch + 1, weights, jnp.zeros((8, pair), F32))
            total = jnp.sum(total, axis=0, keepdims=True)
            inv = 1.0 / total
            soft[ch, 0] = jnp.broadcast_to(top, (8, pair))
            soft[ch, 1] = jnp.broadcast_to(inv, (8, pair))
            dqt[...] = jnp.zeros_like(dqt)

            def outputs(j, _):
                dqt[...] += dot(vo_all[j], (st[j] * inv).astype(BF16))
                return 0

            lax.fori_loop(0, ch + 1, outputs, 0)
            vo_all[ch] = dqt[...].astype(BF16)

        def forwarded(u, _):
            @pl.when(u == 2)
            def _():
                service(RY, 0)

            @pl.when(u == chips - 2)
            def _():
                service(RY, 1)

            forward(chips - 1 - u)
            return 0

        lax.fori_loop(0, chips, forwarded, 0)

        def attend(ch):
            dot_s[...] = dot(dy_all[ch], wot[...]).astype(BF16).T
            qt_s[...] = q_all[ch].T
            row = jnp.sum(dot_s[...].astype(F32) * vo_all[ch].astype(F32), axis=0, keepdims=True)
            top, inv = soft[ch, 0, 0:1, :], soft[ch, 1, 0:1, :]
            dqt[...] = jnp.zeros_like(dqt)

            def tile(j, masked):
                add_q = []
                hi, lo = lax.div(j, quarter), lax.rem(j, quarter)
                step = rows // 2
                for i in (0, 1):
                    first = i * rows if masked else 0
                    ask = pl.ds(first, pair - first)
                    ps, gs = [], []
                    for b in (0, 1):
                        at = pl.ds(i * rows + b * step, step)
                        s = dot(kv_all[0, j, at, :], qt_s[:, ask])
                        dp = dot(kv_all[1, j, at, :], dot_s[:, ask])
                        p = jnp.exp2((s - top[:, first:]) * factor) * inv[:, first:]
                        if masked:
                            p = jnp.where(causal(0)[b * step : (b + 1) * step, : pair - first], p, 0.0)
                        ps.append(p.astype(BF16))
                        gs.append((p * (dp - row[:, first:]) * scale).astype(BF16))
                    at = halves[i]
                    g = jnp.concatenate(gs, axis=0)
                    dkv[1, hi, lo, :, at] += dot_nt(dot_s[:, ask], jnp.concatenate(ps, axis=0))
                    dkv[0, hi, lo, :, at] += dot_nt(qt_s[:, ask], g)
                    add_q.append(dot(kt_all[j, :, at], g))
                if masked:
                    dqt[...] += add_q[0]
                    dqt[:, halves[1]] += add_q[1]
                else:
                    dqt[...] += add_q[0] + add_q[1]

            def grads(j, _):
                tile(j, False)
                return 0

            lax.fori_loop(0, ch, grads, 0)
            tile(ch, True)
            q_all[ch] = dqt[...].astype(BF16).T

        def weight_grads(ch):
            dq = dqt[...].astype(BF16)
            for t in range(width // pair):
                at = pl.ds(t * pair, pair)
                dwqt[:, at] += dot(dq, x_all[ch, :, at])
                dwo_acc[:, at] += dot(vo_all[ch], dy_all[ch, :, at])

        def send_dq(u, i):
            ch = chip_at(u)
            blk = 2 * ch + i

            @pl.when(blk != m)
            def _():
                remote(q_all.at[ch, halves[i], :], dq_in.at[m], dq_s.at[blk], dq_r.at[m], blk).start()

            @pl.when(blk == m)
            def _():
                dq_in[m] = q_all[ch, halves[i], :]

        spare = width // pair

        def fetch(u, i):
            slot = lax.rem(u, 2)
            dst = wq_st.at[slot, :, pl.ds(i * dim, dim)]
            return local(wq_all.at[2 * chip_at(u) + i], dst, 2 + 2 * slot + i)

        def dx_start(u):
            fetch(u, 0).start()
            fetch(u, 1).start()

        def dx_pair(u):
            dq = []
            for i in (0, 1):
                h = 2 * chip_at(u) + i
                fetch(u, i).wait()

                @pl.when(h != m)
                def _():
                    remote(dq_in.at[h], dq_in.at[h], dq_s.at[h], dq_r.at[h], mate).wait_recv()

                dq.append(dq_in[h])
            dq = jnp.concatenate(dq, axis=1)
            for t in range(spare):
                at = pl.ds(t * pair, pair)
                st[t, pl.ds(0, rows), :] += dot_nt(dq, wq_st[lax.rem(u, 2), at, :])

        def dx_pairs(lo, hi):
            def body(u, _):
                @pl.when(u + 1 < chips)
                def _():
                    dx_start(u + 1)

                dx_pair(u)
                return 0

            lax.fori_loop(lo, hi, body, 0)

        def attended(u, _):
            @pl.when((u >= 2) & (u < last))
            def _():
                service(RY, u)

            @pl.when(u == chips - 1)
            def _():
                service(RY, last)
                send_dq(chips - 3, 0)
                send_dq(chips - 3, 1)

            wait_pair(RY, u)
            attend(chip_at(u))

            @pl.when(u != chips - 3)
            def _():
                send_dq(u, 0)
                send_dq(u, 1)

            @pl.when(u < chips - 1)
            def _():
                weight_grads(chip_at(u))

            return 0

        lax.fori_loop(0, chips, attended, 0)

        order = [hops]
        for step in range(hops - 1, 0, -1):
            order += [step, -step]
        order.append(0)

        def chip_off(off):
            return lax.rem(c + off + chips, chips)

        def slice_of(dev):
            row = pl.multiple_of(lax.rem(dev, chips) * slim, slim)
            return dkv.at[lax.div(dev, chips), :, :, pl.ds(row, slim), :]

        def px(i):
            chip = chip_off(order[i])
            return remote(slice_of(2 * chip + 1 - k), part.at[chip], px_s.at[i], px_r.at[i], mate)

        for i in range(chips):
            px(i).start()

        def gather(i):
            px(i).wait_recv()
            chip = chip_off(order[i])
            part[chip] += slice_of(2 * chip + k)[...]

        few = quarter // 2

        def piece(ref, q):
            return ref.at[q // 2, pl.ds(q % 2 * few, few)]

        def rs(d, t, q, src):
            return remote(src, piece(sums.at[d, t - 1], q), rs_s.at[d, t - 1, q], rs_r.at[d, t - 1, q], nbr[d])

        sent = []

        def hop(t):
            for q in range(4):
                for d in (0, 1):
                    chip = chip_off((hops + 1 - t) * (1 - 2 * d))
                    if t == 1 and q // 2 != d:
                        continue
                    if t == 1 or (t == 2 and q // 2 != d):
                        copy = rs(d, t, q, piece(part.at[chip], q))
                    else:
                        held = piece(sums.at[d, t - 2], q)
                        rs(d, t - 1, q, held).wait_recv()
                        held[...] += piece(part.at[chip], q)[...]
                        copy = rs(d, t, q, held)
                    copy.start()
                    sent.append(copy)

        gather(0)
        hop(1)
        weight_grads(chip_at(chips - 1))
        gathered_weights()
        for t in range(spare):
            st[t, pl.ds(0, rows), :] = jnp.zeros((rows, pair), F32)
        dx_start(0)
        dx_pairs(0, 5)
        for i in range(1, chips):
            gather(i)
        hop(2)
        dwo_out = local(dwo_acc, dwo_hbm, 0)
        dwo_out.start()
        dwq_out = []
        for t in range(spare):
            at = pl.ds(t * pair, pair)
            staged = st.at[spare + t, :, pl.ds(0, dim)]
            staged[...] = dwqt[:, at].T
            out = local(staged, dwq_hbm.at[at, :], 6 + t)
            out.start()
            dwq_out.append(out)

        dx_pairs(5, 6)
        hop(hops - 1)
        dx_pairs(6, 7)
        hop(hops)
        dx_pairs(7, 7)

        def tokens_of(dev):
            chip = lax.div(dev, 2)
            at = pl.ds(pl.multiple_of(lax.rem(dev, 2) * rows, rows), rows)
            return thin.at[lax.div(chip, quarter), lax.rem(chip, quarter), :, at]

        def kv_copy(dev):
            return remote(tokens_of(dev), kv_rows.at[m], kv_s.at[dev], kv_r.at[m], dev)

        def dw_copy(dev):
            return remote(dw_out.at[dev], dw_in.at[m], dw_s.at[dev], dw_r.at[m], dev)

        per = pair // cols

        def key_grads(h):
            def body(t, _):
                at = pl.ds(pl.multiple_of(t * pair, pair), pair)
                add = dot(thin[h, 0], x_all[h * quarter, :, at])
                for j in range(1, quarter):
                    add += dot(thin[h, j], x_all[h * quarter + j, :, at])
                for i in range(per):
                    dev = t * per + i
                    piece = add[:, i * cols : (i + 1) * cols]
                    dw_out[dev] = piece if h == 0 else dw_out[dev] + piece
                if h == 1:
                    for i in range(per):
                        dev = t * per + i

                        @pl.when(dev != m)
                        def _():
                            dw_copy(dev).start()

                return 0

            lax.fori_loop(0, width // pair, body, 0)

        for h in (0, 1):
            total = part[c, h]
            for d in (0, 1):
                for q in (2 * h, 2 * h + 1):
                    rs(d, hops, q, piece(sums.at[d, hops - 1], q)).wait_recv()
                total += sums[d, hops - 1, h]
            thin[h] = total.astype(BF16)

            def send_rows(dev, _):
                @pl.when(dev != m)
                def _():
                    kv_copy(dev).start()

                return 0

            lax.fori_loop(h * n // 2, (h + 1) * n // 2, send_rows, 0)
            key_grads(h)
        kv_rows[m] = tokens_of(m)[...]
        dx_pairs(7, chips)

        def rows_arrived(dev, _):
            @pl.when(dev != m)
            def _():
                kv_copy(dev).wait_send()
                remote(kv_rows.at[dev], kv_rows.at[dev], kv_s.at[dev], kv_r.at[dev], mate).wait_recv()

            return 0

        lax.fori_loop(0, n, rows_arrived, 0)
        own_kv = kv_rows[...].reshape(2 * dim, rows).T
        wait_sends(RY)
        for t in range(spare):
            at = pl.ds(t * pair, pair)
            add = dot_nt(own_kv, wqkv[at, pl.ds(dim, 2 * dim)])
            dy_all[0, pl.ds(0, rows), at] = (st[t, pl.ds(0, rows), :] + add).astype(BF16)
        dx_out = local(dy_all.at[0, pl.ds(0, rows), :], dx_hbm, 4)
        dx_out.start()
        dw_in[m] = dw_out[m]

        def arrived(dev, _):
            @pl.when(dev != m)
            def _():
                dw_copy(dev).wait_send()
                remote(dw_in.at[dev], dw_in.at[dev], dw_s.at[dev], dw_r.at[dev], mate).wait_recv()

            return 0

        lax.fori_loop(0, n, arrived, 0)
        turned = dw_in[...].reshape(2 * dim, cols)
        dw_t[0] = turned[:dim].T
        dw_t[1] = turned[dim:].T
        outs = [local(dw_t.at[0], dwk_hbm, 2), local(dw_t.at[1], dwv_hbm, 3)]
        for out in outs:
            out.start()
        for out in (dwo_out, *dwq_out, dx_out, *outs):
            out.wait()

        for r in (RX, RW):
            wait_sends(r)
        for i in range(1, groups):
            peer(i).wait_send()
        for i in range(chips):
            px(i).wait_send()
        for copy in sent:
            copy.wait_send()

        def sent_dq(h, _):
            @pl.when(h != m)
            def _():
                remote(dq_in.at[h], dq_in.at[h], dq_s.at[h], dq_r.at[h], h).wait_send()

            return 0

        lax.fori_loop(0, n, sent_dq, 0)

    return kernel


def hand_on(*refs):
    count = (len(refs) - 2) // 3
    srcs, dsts, bufs = refs[:count], refs[count : 2 * count], refs[2 * count : 3 * count]
    sems_in, sems_out = refs[3 * count :]
    pieces = []
    for src, dst, buf in zip(srcs, dsts, bufs):
        parts = max(1, src.shape[0] * src.shape[1] // (1 << 17))
        size = src.shape[0] // parts
        for i in range(parts):
            at = pl.ds(i * size, size)
            pieces.append((src.at[at, :], buf.at[at, :], dst.at[at, :]))
    ins = [pltpu.make_async_copy(a, b, sems_in.at[i]) for i, (a, b, _) in enumerate(pieces)]
    outs = [pltpu.make_async_copy(b, c, sems_out.at[i]) for i, (_, b, c) in enumerate(pieces)]
    for copy in ins:
        copy.start()
    for got, put in zip(ins, outs):
        got.wait()
        put.start()
    for put in outs:
        put.wait()


def solution(mesh):
    n = mesh.shape["model"]
    groups = mesh.shape["data"]
    chips = n // 2
    hops = chips // 2
    tok_spec = P(("data", "model"), None)

    def local_step(x_loc, dy_loc, wq_loc, w_key, w_value, wo_loc):
        rows, width = x_loc.shape
        dim = w_key.shape[1]
        cols = width // n
        sds = jax.ShapeDtypeStruct
        vmem = pltpu.VMEM
        dma = pltpu.SemaphoreType.DMA
        arrivals = 2 * hops - 1
        slim = 2 * dim // n
        outs = pl.pallas_call(
            make_kernel(n, groups),
            name="mqa_backward",
            out_shape=(
                sds((rows, width), BF16),
                sds((width, dim), F32),
                sds((cols, dim), F32),
                sds((cols, dim), F32),
                sds((dim, width), F32),
                sds((n, width, dim), BF16),
            ),
            in_specs=[pl.BlockSpec(memory_space=pl.ANY)] * 6,
            out_specs=[pl.BlockSpec(memory_space=pl.ANY)] * 6,
            scratch_shapes=[
                vmem((chips, 2 * rows, width), BF16),
                vmem((chips, 2 * rows, width), BF16),
                vmem((chips, 2 * rows, dim), BF16),
                vmem((2, chips, 2 * rows, dim), BF16),
                vmem((chips, dim, 2 * rows), BF16),
                vmem((chips, dim, 2 * rows), BF16),
                vmem((chips, 2, 8, 2 * rows), F32),
                vmem((width, 3 * dim), BF16),
                vmem((width, dim), BF16),
                vmem((2, 2, hops, dim, 2 * rows), F32),
                vmem((chips, 2, hops, slim, 2 * rows), F32),
                vmem((2, hops, 2, hops, slim, 2 * rows), F32),
                vmem((n, rows, dim), BF16),
                vmem((dim, width), F32),
                vmem((dim, width), F32),
                vmem((chips, 2 * rows, 2 * rows), F32),
                vmem((2, width, 2 * dim), BF16),
                vmem((dim, 2 * rows), F32),
                vmem((dim, 2 * rows), BF16),
                vmem((dim, 2 * rows), BF16),
                vmem((2, hops, slim, 2 * rows), BF16),
                vmem((n, slim, rows), BF16),
                vmem((n, slim, cols), F32),
                vmem((n, slim, cols), F32),
                vmem((2, cols, dim), F32),
                dma((3, 2, arrivals)),
                dma((3, 2, arrivals)),
                dma((3, 2 + 2 * arrivals)),
                dma((3, 2 + 2 * arrivals)),
                dma((n,)),
                dma((n,)),
                dma((chips,)),
                dma((chips,)),
                dma((2, hops, 4)),
                dma((2, hops, 4)),
                dma((n,)),
                dma((n,)),
                dma((n,)),
                dma((n,)),
                dma((groups,)),
                dma((groups,)),
                dma((6 + width // (2 * rows),)),
            ],
            compiler_params=pltpu.CompilerParams(
                collective_id=0, has_side_effects=True, vmem_limit_bytes=67043328
            ),
        )(
            x_loc,
            dy_loc,
            wq_loc.reshape(width, dim),
            w_key,
            w_value,
            wo_loc.reshape(dim, width),
        )
        results = outs[:5]
        any_spec = [pl.BlockSpec(memory_space=pl.ANY)] * 5
        dx, dwq, dwk, dwv, dwo = pl.pallas_call(
            hand_on,
            name="hand_on",
            out_shape=tuple(sds(o.shape, o.dtype) for o in results),
            in_specs=any_spec,
            out_specs=any_spec,
            scratch_shapes=[vmem(o.shape, o.dtype) for o in results] + [dma((64,)), dma((64,))],
        )(*results)
        return dx, dwq.reshape(width, 1, dim), dwk, dwv, dwo.reshape(1, dim, width)

    return jax.shard_map(
        local_step,
        mesh=mesh,
        in_specs=(tok_spec, tok_spec, P(None, "model", None), P(None, None), P(None, None), P("model", None, None)),
        out_specs=(tok_spec, P("data", "model", None), tok_spec, tok_spec, P(("data", "model"), None, None)),
        check_vma=False,
    )
```

```python
import math

import jax
import jax.numpy as jnp
from jax import lax
from jax.experimental import pallas as pl
from jax.experimental.pallas import tpu as pltpu
from jax.sharding import PartitionSpec as P

BF16 = jnp.bfloat16
F32 = jnp.float32
MESH = pl.DeviceIdType.MESH
RX, RY, RW = range(3)


def dot(a, b):
    return jnp.dot(a, b, preferred_element_type=F32)


def dot_nt(a, b):
    return lax.dot_general(a, b, (((1,), (1,)), ((), ())), preferred_element_type=F32)


def dot_tn(a, b):
    return lax.dot_general(a, b, (((0,), (0,)), ((), ())), preferred_element_type=F32)


def rowfold(x, op):
    y = x.reshape(x.shape[0] // 8, 8, x.shape[1])
    return jnp.max(y, axis=0) if op == "max" else jnp.sum(y, axis=0)


def make_kernel(n, groups):
    chips = n // 2
    hops = chips // 2
    last = 2 * (hops - 1)
    arrivals = last + 1

    def kernel(
        x_hbm, dy_hbm, wq_hbm, wk_hbm, wv_hbm, wo_hbm,
        dx_hbm, dwq_hbm, dwk_hbm, dwv_hbm, dwo_hbm, wq_all,
        x_all, dy_all, q_all, kv_all, kt_all, vo_all, soft, wqkv, wot,
        dkv, part, sums, dq_in, dwqt, dwo_acc, st, wq_st,
        dqt, dot_s, qt_s, thin, kv_rows, dw_out, dw_in, dw_t,
        ring_r, ring_s, pair_r, pair_s, dq_r, dq_s, px_r, px_s, rs_r, rs_s,
        kv_r, kv_s, dw_r, dw_s, peer_r, peer_s, loc,
    ):
        rows, width = x_hbm.shape
        dim = wk_hbm.shape[1]
        cols = width // n
        slim = 2 * dim // n
        quarter = chips // 2
        scale = 1.0 / math.sqrt(dim)
        m = lax.axis_index("model")
        g = lax.axis_index("data")
        share = width // groups
        c = lax.div(m, 2)
        k = lax.rem(m, 2)
        mate = m + 1 - 2 * k
        nbr = (lax.rem(m + 2, n), lax.rem(m + n - 2, n))

        def remote(src, dst, ssem, rsem, dev):
            return pltpu.make_async_remote_copy(
                src_ref=src, dst_ref=dst, send_sem=ssem, recv_sem=rsem,
                device_id={"model": dev}, device_id_type=MESH,
            )

        bufs = (x_all, dy_all)
        owns = (x_hbm, dy_hbm, wq_hbm)

        def half(ref, h, size, base=0):
            return ref.at[pl.ds(pl.multiple_of(base + h * size, size), size), :]

        def chunk_at(r, blk, h):
            chip = lax.div(blk, 2)
            base = lax.rem(blk, 2) * rows
            if r == RW:
                return half(wq_all.at[blk], h, share // 2, g * share)
            return half(bufs[r].at[chip], h, rows // 2, base)

        def own_at(r, h):
            if r == RW:
                return half(wq_hbm, h, share // 2, g * share)
            return half(owns[r], h, owns[r].shape[0] // 2)

        def start_own(r):
            for p in (0, 1):
                for d in (0, 1):
                    h = p if d == 0 else 1 - p
                    remote(own_at(r, h), chunk_at(r, m, h), ring_s.at[r, d, p], ring_r.at[r, d, p], nbr[d]).start()
            for h in (0, 1):
                remote(own_at(r, h), chunk_at(r, m, h), pair_s.at[r, h], pair_r.at[r, h], mate).start()

        def service(r, a):
            step = lax.div(a, 2) + 1
            p = lax.rem(a, 2)
            for d in (0, 1):
                blk = lax.rem(m + (n - 2 * step if d == 0 else 2 * step), n)
                chunk = chunk_at(r, blk, p if d == 0 else 1 - p)
                remote(chunk, chunk, ring_s.at[r, d, 0], ring_r.at[r, d, a], nbr[d]).wait_recv()

                @pl.when(a <= last - 2)
                def _():
                    remote(chunk, chunk, ring_s.at[r, d, 2 + a], ring_r.at[r, d, a + 2], nbr[d]).start()

                i = 2 + d * arrivals + a
                remote(chunk, chunk, pair_s.at[r, i], pair_r.at[r, i], mate).start()

        def chip_at(u):
            step = lax.div(u + 1, 2)
            odd = lax.rem(u, 2)
            return lax.rem(c + odd * (chips - step) + (1 - odd) * step, chips)

        def wait_pair(r, u):
            blk = 2 * chip_at(u) + 1 - k

            def wait(h, i):
                chunk = chunk_at(r, blk, h)
                remote(chunk, chunk, pair_s.at[r, 0], pair_r.at[r, i], mate).wait_recv()

            @pl.when(u == 0)
            def _():
                wait(0, 0)
                wait(1, 1)

            @pl.when(u > 0)
            def _():
                d = 1 - lax.rem(u, 2)
                i = 2 + d * arrivals + 2 * (lax.div(u + 1, 2) - 1)
                wait(d, i)
                wait(1 - d, i + 1 + lax.div(u, chips - 1) * last)

        def wait_sends(r):
            chunk = own_at(r, 0)
            for d in (0, 1):
                for i in range(last + 1):
                    remote(chunk, chunk, ring_s.at[r, d, i], ring_r.at[r, d, 0], nbr[d]).wait_send()
            for i in range(2 + 2 * arrivals):
                remote(chunk, chunk, pair_s.at[r, i], pair_r.at[r, 0], mate).wait_send()

        def local(src, dst, i):
            return pltpu.make_async_copy(src, dst, loc.at[i])

        own_rows = pl.ds(pl.multiple_of(k * rows, rows), rows)
        loads = [
            local(x_hbm, x_all.at[c, own_rows, :], 0),
            local(wq_hbm, wqkv.at[:, pl.ds(0, dim)], 1),
            local(wk_hbm, wqkv.at[:, pl.ds(dim, dim)], 2),
            local(wv_hbm, wqkv.at[:, pl.ds(2 * dim, dim)], 3),
            local(dy_hbm, dy_all.at[c, own_rows, :], 5),
        ]
        pair = 2 * rows
        for t in range(width // pair):
            loads.append(local(wo_hbm.at[:, pl.ds(t * pair, pair)], vo_all.at[t], 6 + t))
        for load in loads:
            load.start()
        barrier = pltpu.get_barrier_semaphore()
        for dev in (*nbr, mate):
            pl.semaphore_signal(barrier, inc=1, device_id={"model": dev}, device_id_type=MESH)
        for i in range(1, groups):
            pl.semaphore_signal(barrier, inc=1, device_id={"data": lax.rem(g + i, groups), "model": m}, device_id_type=MESH)
        pl.semaphore_wait(barrier, 2 + groups)
        start_own(RW)
        start_own(RX)
        dwqt[...] = jnp.zeros_like(dwqt)
        dwo_acc[...] = jnp.zeros_like(dwo_acc)

        def clear(j, _):
            for kind in (0, 1):
                for hi in (0, 1):
                    dkv[kind, hi, j] = jnp.zeros(dkv.shape[3:], F32)
            return 0

        lax.fori_loop(0, quarter, clear, 0)
        for load in loads:
            load.wait()
        for t in range(width // pair):
            wot[pl.ds(t * pair, pair), :] = vo_all[t].T

        def rows_at(group):
            return wq_all.at[:, pl.ds(pl.multiple_of(group * share, share), share), :]

        def peer(i):
            there = rows_at(g)
            return pltpu.make_async_remote_copy(
                src_ref=there, dst_ref=there, send_sem=peer_s.at[i], recv_sem=peer_r.at[i],
                device_id={"data": lax.rem(g + i, groups), "model": m}, device_id_type=MESH,
            )

        mine = pl.ds(pl.multiple_of(g * share, share), share)
        own_rows_out = local(wqkv.at[mine, pl.ds(0, dim)], wq_all.at[m, mine, :], 1)
        own_rows_out.start()

        def spread():
            def waited(u, _):
                wait_pair(RW, u)
                return 0

            lax.fori_loop(0, chips, waited, 0)
            own_rows_out.wait()
            for i in range(1, groups):
                peer(i).start()

        def gathered_weights():
            for i in range(1, groups):
                there = rows_at(lax.rem(g + groups - i, groups))
                pltpu.make_async_remote_copy(
                    src_ref=there, dst_ref=there, send_sem=peer_s.at[i], recv_sem=peer_r.at[i],
                    device_id={"data": lax.rem(g + i, groups), "model": m}, device_id_type=MESH,
                ).wait_recv()

        def project(ch):
            qkv = dot(x_all[ch], wqkv[...]).astype(BF16)
            q_all[ch] = qkv[:, :dim]
            kv_all[0, ch] = qkv[:, dim : 2 * dim]
            kv_all[1, ch] = qkv[:, 2 * dim :]
            kt_all[ch] = qkv[:, dim : 2 * dim].T
            vo_all[ch] = qkv[:, 2 * dim :].T

        def gathered(u, _):
            @pl.when(u == 1)
            def _():
                service(RX, 0)

            @pl.when((u >= 1) & (u < hops))
            def _():
                service(RW, 2 * u - 2)
                service(RW, 2 * u - 1)

            @pl.when(u == hops)
            def _():
                service(RW, last)
                spread()

            @pl.when((u >= 1) & (u <= last))
            def _():
                service(RX, u)

            @pl.when(u == last - 2)
            def _():
                start_own(RY)

            wait_pair(RX, u)
            project(chip_at(u))
            return 0

        lax.fori_loop(0, chips, gathered, 0)

        factor = scale * math.log2(math.e)
        halves = [pl.ds(i * rows, rows) for i in (0, 1)]

        def causal(i):
            key = lax.broadcasted_iota(jnp.int32, (rows, pair), 0) + i * rows
            return key <= lax.broadcasted_iota(jnp.int32, (rows, pair), 1)

        def forward(ch):
            qt_s[...] = q_all[ch].T

            def scores(j, top):
                for at in halves:
                    s = dot(kv_all[0, j, at, :], qt_s[...])
                    st[j, at, :] = s
                    top = jnp.maximum(top, rowfold(s, "max"))
                return top

            top = lax.fori_loop(0, ch, scores, jnp.full((8, pair), -jnp.inf, F32))
            for i in (0, 1):
                s = dot(kv_all[0, ch, halves[i], :], qt_s[...])
                s = jnp.where(causal(i), s, -jnp.inf)
                st[ch, halves[i], :] = s
                top = jnp.maximum(top, rowfold(s, "max"))
            top = jnp.max(top, axis=0, keepdims=True)

            def weights(j, total):
                for at in halves:
                    p = jnp.exp2((st[j, at, :] - top) * factor)
                    st[j, at, :] = p
                    total += rowfold(p, "sum")
                return total

            total = lax.fori_loop(0, ch + 1, weights, jnp.zeros((8, pair), F32))
            total = jnp.sum(total, axis=0, keepdims=True)
            inv = 1.0 / total
            soft[ch, 0] = jnp.broadcast_to(top, (8, pair))
            soft[ch, 1] = jnp.broadcast_to(inv, (8, pair))
            dqt[...] = jnp.zeros_like(dqt)

            def outputs(j, _):
                dqt[...] += dot(vo_all[j], (st[j] * inv).astype(BF16))
                return 0

            lax.fori_loop(0, ch + 1, outputs, 0)
            vo_all[ch] = dqt[...].astype(BF16)

        def forwarded(u, _):
            @pl.when(u == 2)
            def _():
                service(RY, 0)

            @pl.when(u == chips - 2)
            def _():
                service(RY, 1)

            forward(chips - 1 - u)
            return 0

        lax.fori_loop(0, chips, forwarded, 0)

        def attend(ch):
            dot_s[...] = dot(dy_all[ch], wot[...]).astype(BF16).T
            qt_s[...] = q_all[ch].T
            row = jnp.sum(dot_s[...].astype(F32) * vo_all[ch].astype(F32), axis=0, keepdims=True)
            top, inv = soft[ch, 0, 0:1, :], soft[ch, 1, 0:1, :]
            dqt[...] = jnp.zeros_like(dqt)

            def tile(j, masked):
                add_q = []
                hi, lo = lax.div(j, quarter), lax.rem(j, quarter)
                step = rows // 2
                for i in (0, 1):
                    first = i * rows if masked else 0
                    ask = pl.ds(first, pair - first)
                    ps, gs = [], []
                    for b in (0, 1):
                        at = pl.ds(i * rows + b * step, step)
                        s = dot(kv_all[0, j, at, :], qt_s[:, ask])
                        dp = dot(kv_all[1, j, at, :], dot_s[:, ask])
                        p = jnp.exp2((s - top[:, first:]) * factor) * inv[:, first:]
                        if masked:
                            p = jnp.where(causal(0)[b * step : (b + 1) * step, : pair - first], p, 0.0)
                        ps.append(p.astype(BF16))
                        gs.append((p * (dp - row[:, first:]) * scale).astype(BF16))
                    at = halves[i]
                    g = jnp.concatenate(gs, axis=0)
                    dkv[1, hi, lo, :, at] += dot_nt(dot_s[:, ask], jnp.concatenate(ps, axis=0))
                    dkv[0, hi, lo, :, at] += dot_nt(qt_s[:, ask], g)
                    add_q.append(dot(kt_all[j, :, at], g))
                if masked:
                    dqt[...] += add_q[0]
                    dqt[:, halves[1]] += add_q[1]
                else:
                    dqt[...] += add_q[0] + add_q[1]

            def grads(j, _):
                tile(j, False)
                return 0

            lax.fori_loop(0, ch, grads, 0)
            tile(ch, True)
            q_all[ch] = dqt[...].astype(BF16).T

        def weight_grads(ch):
            dq = dqt[...].astype(BF16)
            for t in range(width // pair):
                at = pl.ds(t * pair, pair)
                dwqt[:, at] += dot(dq, x_all[ch, :, at])
                dwo_acc[:, at] += dot(vo_all[ch], dy_all[ch, :, at])

        def send_dq(u, i):
            ch = chip_at(u)
            blk = 2 * ch + i

            @pl.when(blk != m)
            def _():
                remote(q_all.at[ch, halves[i], :], dq_in.at[m], dq_s.at[blk], dq_r.at[m], blk).start()

            @pl.when(blk == m)
            def _():
                dq_in[m] = q_all[ch, halves[i], :]

        spare = width // pair

        def fetch(u, i):
            slot = lax.rem(u, 2)
            dst = wq_st.at[slot, :, pl.ds(i * dim, dim)]
            return local(wq_all.at[2 * chip_at(u) + i], dst, 2 + 2 * slot + i)

        def dx_start(u):
            fetch(u, 0).start()
            fetch(u, 1).start()

        def dx_pair(u):
            dq = []
            for i in (0, 1):
                h = 2 * chip_at(u) + i
                fetch(u, i).wait()

                @pl.when(h != m)
                def _():
                    remote(dq_in.at[h], dq_in.at[h], dq_s.at[h], dq_r.at[h], mate).wait_recv()

                dq.append(dq_in[h])
            dq = jnp.concatenate(dq, axis=1)
            for t in range(spare):
                at = pl.ds(t * pair, pair)
                st[t, pl.ds(0, rows), :] += dot_nt(dq, wq_st[lax.rem(u, 2), at, :])

        def dx_pairs(lo, hi):
            def body(u, _):
                @pl.when(u + 1 < chips)
                def _():
                    dx_start(u + 1)

                dx_pair(u)
                return 0

            lax.fori_loop(lo, hi, body, 0)

        def attended(u, _):
            @pl.when((u >= 2) & (u < last))
            def _():
                service(RY, u)

            @pl.when(u == chips - 1)
            def _():
                service(RY, last)
                send_dq(chips - 3, 0)
                send_dq(chips - 3, 1)

            wait_pair(RY, u)
            attend(chip_at(u))

            @pl.when(u != chips - 3)
            def _():
                send_dq(u, 0)
                send_dq(u, 1)

            @pl.when(u < chips - 1)
            def _():
                weight_grads(chip_at(u))

            return 0

        lax.fori_loop(0, chips, attended, 0)

        order = [hops]
        for step in range(hops - 1, 0, -1):
            order += [step, -step]
        order.append(0)

        def chip_off(off):
            return lax.rem(c + off + chips, chips)

        def slice_of(dev):
            row = pl.multiple_of(lax.rem(dev, chips) * slim, slim)
            return dkv.at[lax.div(dev, chips), :, :, pl.ds(row, slim), :]

        def px(i):
            chip = chip_off(order[i])
            return remote(slice_of(2 * chip + 1 - k), part.at[chip], px_s.at[i], px_r.at[i], mate)

        for i in range(chips):
            px(i).start()

        def gather(i):
            px(i).wait_recv()
            chip = chip_off(order[i])
            part[chip] += slice_of(2 * chip + k)[...]

        few = quarter // 2

        def piece(ref, q):
            return ref.at[q // 2, pl.ds(q % 2 * few, few)]

        def rs(d, t, q, src):
            return remote(src, piece(sums.at[d, t - 1], q), rs_s.at[d, t - 1, q], rs_r.at[d, t - 1, q], nbr[d])

        sent = []

        def hop(t):
            for q in range(4):
                for d in (0, 1):
                    chip = chip_off((hops + 1 - t) * (1 - 2 * d))
                    if t == 1 and q // 2 != d:
                        continue
                    if t == 1 or (t == 2 and q // 2 != d):
                        copy = rs(d, t, q, piece(part.at[chip], q))
                    else:
                        held = piece(sums.at[d, t - 2], q)
                        rs(d, t - 1, q, held).wait_recv()
                        held[...] += piece(part.at[chip], q)[...]
                        copy = rs(d, t, q, held)
                    copy.start()
                    sent.append(copy)

        gather(0)
        hop(1)
        gathered_weights()
        for t in range(spare):
            st[t, pl.ds(0, rows), :] = jnp.zeros((rows, pair), F32)
        dx_start(0)
        dx_pairs(0, 5)
        for i in range(1, chips):
            gather(i)
        hop(2)
        weight_grads(chip_at(chips - 1))
        dwo_out = local(dwo_acc, dwo_hbm, 0)
        dwo_out.start()
        dwq_out = []
        for t in range(spare):
            at = pl.ds(t * pair, pair)
            staged = st.at[spare + t, :, pl.ds(0, dim)]
            staged[...] = dwqt[:, at].T
            out = local(staged, dwq_hbm.at[at, :], 6 + t)
            out.start()
            dwq_out.append(out)

        dx_pairs(5, 6)
        hop(hops - 1)
        dx_pairs(6, 7)
        hop(hops)
        dx_pairs(7, 7)

        def tokens_of(dev):
            chip = lax.div(dev, 2)
            at = pl.ds(pl.multiple_of(lax.rem(dev, 2) * rows, rows), rows)
            return thin.at[lax.div(chip, quarter), lax.rem(chip, quarter), :, at]

        def kv_copy(dev):
            return remote(tokens_of(dev), kv_rows.at[m], kv_s.at[dev], kv_r.at[m], dev)

        def dw_copy(dev):
            return remote(dw_out.at[dev], dw_in.at[m], dw_s.at[dev], dw_r.at[m], dev)

        per = pair // cols

        def key_grads(h):
            def body(t, _):
                at = pl.ds(pl.multiple_of(t * pair, pair), pair)
                add = dot(thin[h, 0], x_all[h * quarter, :, at])
                for j in range(1, quarter):
                    add += dot(thin[h, j], x_all[h * quarter + j, :, at])
                for i in range(per):
                    dev = t * per + i
                    piece = add[:, i * cols : (i + 1) * cols]
                    dw_out[dev] = piece if h == 0 else dw_out[dev] + piece
                if h == 1:
                    for i in range(per):
                        dev = t * per + i

                        @pl.when(dev != m)
                        def _():
                            dw_copy(dev).start()

                return 0

            lax.fori_loop(0, width // pair, body, 0)

        for h in (0, 1):
            total = part[c, h]
            for d in (0, 1):
                for q in (2 * h, 2 * h + 1):
                    rs(d, hops, q, piece(sums.at[d, hops - 1], q)).wait_recv()
                total += sums[d, hops - 1, h]
            thin[h] = total.astype(BF16)

            def send_rows(dev, _):
                @pl.when(dev != m)
                def _():
                    kv_copy(dev).start()

                return 0

            lax.fori_loop(h * n // 2, (h + 1) * n // 2, send_rows, 0)
            key_grads(h)
        kv_rows[m] = tokens_of(m)[...]
        dx_pairs(7, chips)

        def rows_arrived(dev, _):
            @pl.when(dev != m)
            def _():
                kv_copy(dev).wait_send()
                remote(kv_rows.at[dev], kv_rows.at[dev], kv_s.at[dev], kv_r.at[dev], mate).wait_recv()

            return 0

        lax.fori_loop(0, n, rows_arrived, 0)
        own_kv = kv_rows[...].reshape(2 * dim, rows).T
        wait_sends(RY)
        for t in range(spare):
            at = pl.ds(t * pair, pair)
            add = dot_nt(own_kv, wqkv[at, pl.ds(dim, 2 * dim)])
            dy_all[0, pl.ds(0, rows), at] = (st[t, pl.ds(0, rows), :] + add).astype(BF16)
        dx_out = local(dy_all.at[0, pl.ds(0, rows), :], dx_hbm, 4)
        dx_out.start()
        dw_in[m] = dw_out[m]

        def arrived(dev, _):
            @pl.when(dev != m)
            def _():
                dw_copy(dev).wait_send()
                remote(dw_in.at[dev], dw_in.at[dev], dw_s.at[dev], dw_r.at[dev], mate).wait_recv()

            return 0

        lax.fori_loop(0, n, arrived, 0)
        turned = dw_in[...].reshape(2 * dim, cols)
        dw_t[0] = turned[:dim].T
        dw_t[1] = turned[dim:].T
        outs = [local(dw_t.at[0], dwk_hbm, 2), local(dw_t.at[1], dwv_hbm, 3)]
        for out in outs:
            out.start()
        for out in (dwo_out, *dwq_out, dx_out, *outs):
            out.wait()

        for r in (RX, RW):
            wait_sends(r)
        for i in range(1, groups):
            peer(i).wait_send()
        for i in range(chips):
            px(i).wait_send()
        for copy in sent:
            copy.wait_send()

        def sent_dq(h, _):
            @pl.when(h != m)
            def _():
                remote(dq_in.at[h], dq_in.at[h], dq_s.at[h], dq_r.at[h], h).wait_send()

            return 0

        lax.fori_loop(0, n, sent_dq, 0)

    return kernel


def hand_on(*refs):
    count = (len(refs) - 2) // 3
    srcs, dsts, bufs = refs[:count], refs[count : 2 * count], refs[2 * count : 3 * count]
    sems_in, sems_out = refs[3 * count :]
    pieces = []
    for src, dst, buf in zip(srcs, dsts, bufs):
        parts = max(1, src.shape[0] * src.shape[1] // (1 << 17))
        size = src.shape[0] // parts
        for i in range(parts):
            at = pl.ds(i * size, size)
            pieces.append((src.at[at, :], buf.at[at, :], dst.at[at, :]))
    ins = [pltpu.make_async_copy(a, b, sems_in.at[i]) for i, (a, b, _) in enumerate(pieces)]
    outs = [pltpu.make_async_copy(b, c, sems_out.at[i]) for i, (_, b, c) in enumerate(pieces)]
    for copy in ins:
        copy.start()
    for got, put in zip(ins, outs):
        got.wait()
        put.start()
    for put in outs:
        put.wait()


def solution(mesh):
    n = mesh.shape["model"]
    groups = mesh.shape["data"]
    chips = n // 2
    hops = chips // 2
    tok_spec = P(("data", "model"), None)

    def local_step(x_loc, dy_loc, wq_loc, w_key, w_value, wo_loc):
        rows, width = x_loc.shape
        dim = w_key.shape[1]
        cols = width // n
        sds = jax.ShapeDtypeStruct
        vmem = pltpu.VMEM
        dma = pltpu.SemaphoreType.DMA
        arrivals = 2 * hops - 1
        slim = 2 * dim // n
        outs = pl.pallas_call(
            make_kernel(n, groups),
            name="mqa_backward",
            out_shape=(
                sds((rows, width), BF16),
                sds((width, dim), F32),
                sds((cols, dim), F32),
                sds((cols, dim), F32),
                sds((dim, width), F32),
                sds((n, width, dim), BF16),
            ),
            in_specs=[pl.BlockSpec(memory_space=pl.ANY)] * 6,
            out_specs=[pl.BlockSpec(memory_space=pl.ANY)] * 6,
            scratch_shapes=[
                vmem((chips, 2 * rows, width), BF16),
                vmem((chips, 2 * rows, width), BF16),
                vmem((chips, 2 * rows, dim), BF16),
                vmem((2, chips, 2 * rows, dim), BF16),
                vmem((chips, dim, 2 * rows), BF16),
                vmem((chips, dim, 2 * rows), BF16),
                vmem((chips, 2, 8, 2 * rows), F32),
                vmem((width, 3 * dim), BF16),
                vmem((width, dim), BF16),
                vmem((2, 2, hops, dim, 2 * rows), F32),
                vmem((chips, 2, hops, slim, 2 * rows), F32),
                vmem((2, hops, 2, hops, slim, 2 * rows), F32),
                vmem((n, rows, dim), BF16),
                vmem((dim, width), F32),
                vmem((dim, width), F32),
                vmem((chips, 2 * rows, 2 * rows), F32),
                vmem((2, width, 2 * dim), BF16),
                vmem((dim, 2 * rows), F32),
                vmem((dim, 2 * rows), BF16),
                vmem((dim, 2 * rows), BF16),
                vmem((2, hops, slim, 2 * rows), BF16),
                vmem((n, slim, rows), BF16),
                vmem((n, slim, cols), F32),
                vmem((n, slim, cols), F32),
                vmem((2, cols, dim), F32),
                dma((3, 2, arrivals)),
                dma((3, 2, arrivals)),
                dma((3, 2 + 2 * arrivals)),
                dma((3, 2 + 2 * arrivals)),
                dma((n,)),
                dma((n,)),
                dma((chips,)),
                dma((chips,)),
                dma((2, hops, 4)),
                dma((2, hops, 4)),
                dma((n,)),
                dma((n,)),
                dma((n,)),
                dma((n,)),
                dma((groups,)),
                dma((groups,)),
                dma((6 + width // (2 * rows),)),
            ],
            compiler_params=pltpu.CompilerParams(
                collective_id=0, has_side_effects=True, vmem_limit_bytes=67043328
            ),
        )(
            x_loc,
            dy_loc,
            wq_loc.reshape(width, dim),
            w_key,
            w_value,
            wo_loc.reshape(dim, width),
        )
        results = outs[:5]
        any_spec = [pl.BlockSpec(memory_space=pl.ANY)] * 5
        dx, dwq, dwk, dwv, dwo = pl.pallas_call(
            hand_on,
            name="hand_on",
            out_shape=tuple(sds(o.shape, o.dtype) for o in results),
            in_specs=any_spec,
            out_specs=any_spec,
            scratch_shapes=[vmem(o.shape, o.dtype) for o in results] + [dma((64,)), dma((64,))],
        )(*results)
        return dx, dwq.reshape(width, 1, dim), dwk, dwv, dwo.reshape(1, dim, width)

    return jax.shard_map(
        local_step,
        mesh=mesh,
        in_specs=(tok_spec, tok_spec, P(None, "model", None), P(None, None), P(None, None), P("model", None, None)),
        out_specs=(tok_spec, P("data", "model", None), tok_spec, tok_spec, P(("data", "model"), None, None)),
        check_vma=False,
    )
```

```python
import math

import jax
import jax.numpy as jnp
from jax import lax
from jax.experimental import pallas as pl
from jax.experimental.pallas import tpu as pltpu
from jax.sharding import PartitionSpec as P

BF16 = jnp.bfloat16
F32 = jnp.float32
MESH = pl.DeviceIdType.MESH
RX, RY, RW = range(3)


def dot(a, b):
    return jnp.dot(a, b, preferred_element_type=F32)


def dot_nt(a, b):
    return lax.dot_general(a, b, (((1,), (1,)), ((), ())), preferred_element_type=F32)


def dot_tn(a, b):
    return lax.dot_general(a, b, (((0,), (0,)), ((), ())), preferred_element_type=F32)


def rowfold(x, op):
    y = x.reshape(x.shape[0] // 8, 8, x.shape[1])
    return jnp.max(y, axis=0) if op == "max" else jnp.sum(y, axis=0)


def make_kernel(n, groups):
    chips = n // 2
    hops = chips // 2
    last = 2 * (hops - 1)
    arrivals = last + 1

    def kernel(
        x_hbm, dy_hbm, wq_hbm, wk_hbm, wv_hbm, wo_hbm,
        dx_hbm, dwq_hbm, dwk_hbm, dwv_hbm, dwo_hbm, wq_all,
        x_all, dy_all, q_all, kv_all, kt_all, vo_all, soft, wqkv, wot,
        dkv, part, sums, dq_in, dwqt, dwo_acc, st, wq_st,
        dqt, dot_s, qt_s, thin, kv_rows, dw_out, dw_in, dw_t,
        ring_r, ring_s, pair_r, pair_s, dq_r, dq_s, px_r, px_s, rs_r, rs_s,
        kv_r, kv_s, dw_r, dw_s, peer_r, peer_s, loc,
    ):
        rows, width = x_hbm.shape
        dim = wk_hbm.shape[1]
        cols = width // n
        slim = 2 * dim // n
        quarter = chips // 2
        scale = 1.0 / math.sqrt(dim)
        m = lax.axis_index("model")
        g = lax.axis_index("data")
        share = width // groups
        c = lax.div(m, 2)
        k = lax.rem(m, 2)
        mate = m + 1 - 2 * k
        nbr = (lax.rem(m + 2, n), lax.rem(m + n - 2, n))

        def remote(src, dst, ssem, rsem, dev):
            return pltpu.make_async_remote_copy(
                src_ref=src, dst_ref=dst, send_sem=ssem, recv_sem=rsem,
                device_id={"model": dev}, device_id_type=MESH,
            )

        bufs = (x_all, dy_all)
        owns = (x_hbm, dy_hbm, wq_hbm)

        def half(ref, h, size, base=0):
            return ref.at[pl.ds(pl.multiple_of(base + h * size, size), size), :]

        def chunk_at(r, blk, h):
            chip = lax.div(blk, 2)
            base = lax.rem(blk, 2) * rows
            if r == RW:
                return half(wq_all.at[blk], h, share // 2, g * share)
            return half(bufs[r].at[chip], h, rows // 2, base)

        def own_at(r, h):
            if r == RW:
                return half(wq_hbm, h, share // 2, g * share)
            return half(owns[r], h, owns[r].shape[0] // 2)

        def start_own(r):
            for p in (0, 1):
                for d in (0, 1):
                    h = p if d == 0 else 1 - p
                    remote(own_at(r, h), chunk_at(r, m, h), ring_s.at[r, d, p], ring_r.at[r, d, p], nbr[d]).start()
            for h in (0, 1):
                remote(own_at(r, h), chunk_at(r, m, h), pair_s.at[r, h], pair_r.at[r, h], mate).start()

        def service(r, a):
            step = lax.div(a, 2) + 1
            p = lax.rem(a, 2)
            for d in (0, 1):
                blk = lax.rem(m + (n - 2 * step if d == 0 else 2 * step), n)
                chunk = chunk_at(r, blk, p if d == 0 else 1 - p)
                remote(chunk, chunk, ring_s.at[r, d, 0], ring_r.at[r, d, a], nbr[d]).wait_recv()

                @pl.when(a <= last - 2)
                def _():
                    remote(chunk, chunk, ring_s.at[r, d, 2 + a], ring_r.at[r, d, a + 2], nbr[d]).start()

                i = 2 + d * arrivals + a
                remote(chunk, chunk, pair_s.at[r, i], pair_r.at[r, i], mate).start()

        def chip_at(u):
            step = lax.div(u + 1, 2)
            odd = lax.rem(u, 2)
            return lax.rem(c + odd * (chips - step) + (1 - odd) * step, chips)

        def wait_pair(r, u):
            blk = 2 * chip_at(u) + 1 - k

            def wait(h, i):
                chunk = chunk_at(r, blk, h)
                remote(chunk, chunk, pair_s.at[r, 0], pair_r.at[r, i], mate).wait_recv()

            @pl.when(u == 0)
            def _():
                wait(0, 0)
                wait(1, 1)

            @pl.when(u > 0)
            def _():
                d = 1 - lax.rem(u, 2)
                i = 2 + d * arrivals + 2 * (lax.div(u + 1, 2) - 1)
                wait(d, i)
                wait(1 - d, i + 1 + lax.div(u, chips - 1) * last)

        def wait_sends(r):
            chunk = own_at(r, 0)
            for d in (0, 1):
                for i in range(last + 1):
                    remote(chunk, chunk, ring_s.at[r, d, i], ring_r.at[r, d, 0], nbr[d]).wait_send()
            for i in range(2 + 2 * arrivals):
                remote(chunk, chunk, pair_s.at[r, i], pair_r.at[r, 0], mate).wait_send()

        def local(src, dst, i):
            return pltpu.make_async_copy(src, dst, loc.at[i])

        own_rows = pl.ds(pl.multiple_of(k * rows, rows), rows)
        loads = [
            local(x_hbm, x_all.at[c, own_rows, :], 0),
            local(wq_hbm, wqkv.at[:, pl.ds(0, dim)], 1),
            local(wk_hbm, wqkv.at[:, pl.ds(dim, dim)], 2),
            local(wv_hbm, wqkv.at[:, pl.ds(2 * dim, dim)], 3),
            local(dy_hbm, dy_all.at[c, own_rows, :], 5),
        ]
        pair = 2 * rows
        for t in range(width // pair):
            loads.append(local(wo_hbm.at[:, pl.ds(t * pair, pair)], vo_all.at[t], 6 + t))
        for load in loads:
            load.start()
        barrier = pltpu.get_barrier_semaphore()
        for dev in (*nbr, mate):
            pl.semaphore_signal(barrier, inc=1, device_id={"model": dev}, device_id_type=MESH)
        for i in range(1, groups):
            pl.semaphore_signal(barrier, inc=1, device_id={"data": lax.rem(g + i, groups), "model": m}, device_id_type=MESH)
        pl.semaphore_wait(barrier, 2 + groups)
        start_own(RW)
        start_own(RX)
        dwqt[...] = jnp.zeros_like(dwqt)
        dwo_acc[...] = jnp.zeros_like(dwo_acc)

        def clear(j, _):
            for kind in (0, 1):
                for hi in (0, 1):
                    dkv[kind, hi, j] = jnp.zeros(dkv.shape[3:], F32)
            return 0

        lax.fori_loop(0, quarter, clear, 0)
        for load in loads:
            load.wait()
        for t in range(width // pair):
            wot[pl.ds(t * pair, pair), :] = vo_all[t].T

        def rows_at(group):
            return wq_all.at[:, pl.ds(pl.multiple_of(group * share, share), share), :]

        def peer(i):
            there = rows_at(g)
            return pltpu.make_async_remote_copy(
                src_ref=there, dst_ref=there, send_sem=peer_s.at[i], recv_sem=peer_r.at[i],
                device_id={"data": lax.rem(g + i, groups), "model": m}, device_id_type=MESH,
            )

        mine = pl.ds(pl.multiple_of(g * share, share), share)
        own_rows_out = local(wqkv.at[mine, pl.ds(0, dim)], wq_all.at[m, mine, :], 1)
        own_rows_out.start()

        def spread():
            def waited(u, _):
                wait_pair(RW, u)
                return 0

            lax.fori_loop(0, chips, waited, 0)
            own_rows_out.wait()
            for i in range(1, groups):
                peer(i).start()

        def gathered_weights():
            for i in range(1, groups):
                there = rows_at(lax.rem(g + groups - i, groups))
                pltpu.make_async_remote_copy(
                    src_ref=there, dst_ref=there, send_sem=peer_s.at[i], recv_sem=peer_r.at[i],
                    device_id={"data": lax.rem(g + i, groups), "model": m}, device_id_type=MESH,
                ).wait_recv()

        def project(ch):
            qkv = dot(x_all[ch], wqkv[...]).astype(BF16)
            q_all[ch] = qkv[:, :dim]
            kv_all[0, ch] = qkv[:, dim : 2 * dim]
            kv_all[1, ch] = qkv[:, 2 * dim :]
            kt_all[ch] = qkv[:, dim : 2 * dim].T
            vo_all[ch] = qkv[:, 2 * dim :].T

        def gathered(u, _):
            @pl.when(u == 1)
            def _():
                service(RX, 0)

            @pl.when((u >= 1) & (u < hops))
            def _():
                service(RW, 2 * u - 2)
                service(RW, 2 * u - 1)

            @pl.when(u == hops)
            def _():
                service(RW, last)
                spread()

            @pl.when((u >= 1) & (u <= last))
            def _():
                service(RX, u)

            @pl.when(u == last - 2)
            def _():
                start_own(RY)

            wait_pair(RX, u)
            project(chip_at(u))
            return 0

        lax.fori_loop(0, chips, gathered, 0)

        factor = scale * math.log2(math.e)
        halves = [pl.ds(i * rows, rows) for i in (0, 1)]

        def causal(i):
            key = lax.broadcasted_iota(jnp.int32, (rows, pair), 0) + i * rows
            return key <= lax.broadcasted_iota(jnp.int32, (rows, pair), 1)

        def forward(ch):
            qt_s[...] = q_all[ch].T

            def scores(j, top):
                for at in halves:
                    s = dot(kv_all[0, j, at, :], qt_s[...])
                    st[j, at, :] = s
                    top = jnp.maximum(top, rowfold(s, "max"))
                return top

            top = lax.fori_loop(0, ch, scores, jnp.full((8, pair), -jnp.inf, F32))
            for i in (0, 1):
                s = dot(kv_all[0, ch, halves[i], :], qt_s[...])
                s = jnp.where(causal(i), s, -jnp.inf)
                st[ch, halves[i], :] = s
                top = jnp.maximum(top, rowfold(s, "max"))
            top = jnp.max(top, axis=0, keepdims=True)

            def weights(j, total):
                for at in halves:
                    p = jnp.exp2((st[j, at, :] - top) * factor)
                    st[j, at, :] = p
                    total += rowfold(p, "sum")
                return total

            total = lax.fori_loop(0, ch + 1, weights, jnp.zeros((8, pair), F32))
            total = jnp.sum(total, axis=0, keepdims=True)
            inv = 1.0 / total
            soft[ch, 0] = jnp.broadcast_to(top, (8, pair))
            soft[ch, 1] = jnp.broadcast_to(inv, (8, pair))
            dqt[...] = jnp.zeros_like(dqt)

            def outputs(j, _):
                dqt[...] += dot(vo_all[j], (st[j] * inv).astype(BF16))
                return 0

            lax.fori_loop(0, ch + 1, outputs, 0)
            vo_all[ch] = dqt[...].astype(BF16)

        def forwarded(u, _):
            @pl.when(u == 2)
            def _():
                service(RY, 0)

            @pl.when(u == chips - 2)
            def _():
                service(RY, 1)

            forward(chips - 1 - u)
            return 0

        lax.fori_loop(0, chips, forwarded, 0)

        def attend(ch):
            dot_s[...] = dot(dy_all[ch], wot[...]).astype(BF16).T
            qt_s[...] = q_all[ch].T
            row = jnp.sum(dot_s[...].astype(F32) * vo_all[ch].astype(F32), axis=0, keepdims=True)
            top, inv = soft[ch, 0, 0:1, :], soft[ch, 1, 0:1, :]
            dqt[...] = jnp.zeros_like(dqt)

            def tile(j, masked):
                add_q = []
                hi, lo = lax.div(j, quarter), lax.rem(j, quarter)
                step = rows // 2
                for i in (0, 1):
                    first = i * rows if masked else 0
                    ask = pl.ds(first, pair - first)
                    ps, gs = [], []
                    for b in (0, 1):
                        at = pl.ds(i * rows + b * step, step)
                        s = dot(kv_all[0, j, at, :], qt_s[:, ask])
                        dp = dot(kv_all[1, j, at, :], dot_s[:, ask])
                        p = jnp.exp2((s - top[:, first:]) * factor) * inv[:, first:]
                        if masked:
                            p = jnp.where(causal(0)[b * step : (b + 1) * step, : pair - first], p, 0.0)
                        ps.append(p.astype(BF16))
                        gs.append((p * (dp - row[:, first:]) * scale).astype(BF16))
                    at = halves[i]
                    g = jnp.concatenate(gs, axis=0)
                    dkv[1, hi, lo, :, at] += dot_nt(dot_s[:, ask], jnp.concatenate(ps, axis=0))
                    dkv[0, hi, lo, :, at] += dot_nt(qt_s[:, ask], g)
                    add_q.append(dot(kt_all[j, :, at], g))
                if masked:
                    dqt[...] += add_q[0]
                    dqt[:, halves[1]] += add_q[1]
                else:
                    dqt[...] += add_q[0] + add_q[1]

            def grads(j, _):
                tile(j, False)
                return 0

            lax.fori_loop(0, ch, grads, 0)
            tile(ch, True)
            q_all[ch] = dqt[...].astype(BF16).T

        def weight_grads(ch):
            dq = dqt[...].astype(BF16)
            for t in range(width // pair):
                at = pl.ds(t * pair, pair)
                dwqt[:, at] += dot(dq, x_all[ch, :, at])
                dwo_acc[:, at] += dot(vo_all[ch], dy_all[ch, :, at])

        def send_dq(u, i):
            ch = chip_at(u)
            blk = 2 * ch + i

            @pl.when(blk != m)
            def _():
                remote(q_all.at[ch, halves[i], :], dq_in.at[m], dq_s.at[blk], dq_r.at[m], blk).start()

            @pl.when(blk == m)
            def _():
                dq_in[m] = q_all[ch, halves[i], :]

        spare = width // pair

        def fetch(u, i):
            slot = lax.rem(u, 2)
            dst = wq_st.at[slot, :, pl.ds(i * dim, dim)]
            return local(wq_all.at[2 * chip_at(u) + i], dst, 2 + 2 * slot + i)

        def dx_start(u):
            fetch(u, 0).start()
            fetch(u, 1).start()

        def dx_pair(u):
            dq = []
            for i in (0, 1):
                h = 2 * chip_at(u) + i
                fetch(u, i).wait()

                @pl.when(h != m)
                def _():
                    remote(dq_in.at[h], dq_in.at[h], dq_s.at[h], dq_r.at[h], mate).wait_recv()

                dq.append(dq_in[h])
            dq = jnp.concatenate(dq, axis=1)
            for t in range(spare):
                at = pl.ds(t * pair, pair)
                st[t, pl.ds(0, rows), :] += dot_nt(dq, wq_st[lax.rem(u, 2), at, :])

        def dx_pairs(lo, hi):
            def body(u, _):
                @pl.when(u + 1 < chips)
                def _():
                    dx_start(u + 1)

                dx_pair(u)
                return 0

            lax.fori_loop(lo, hi, body, 0)

        def attended(u, _):
            @pl.when((u >= 2) & (u < last))
            def _():
                service(RY, u)

            @pl.when(u == chips - 1)
            def _():
                service(RY, last)
                send_dq(chips - 3, 0)
                send_dq(chips - 3, 1)

            wait_pair(RY, u)
            attend(chip_at(u))

            @pl.when(u != chips - 3)
            def _():
                send_dq(u, 0)
                send_dq(u, 1)

            @pl.when(u < chips - 1)
            def _():
                weight_grads(chip_at(u))

            return 0

        lax.fori_loop(0, chips, attended, 0)

        order = [hops]
        for step in range(hops - 1, 0, -1):
            order += [step, -step]
        order.append(0)

        def chip_off(off):
            return lax.rem(c + off + chips, chips)

        def slice_of(dev):
            row = pl.multiple_of(lax.rem(dev, chips) * slim, slim)
            return dkv.at[lax.div(dev, chips), :, :, pl.ds(row, slim), :]

        def px(i):
            chip = chip_off(order[i])
            return remote(slice_of(2 * chip + 1 - k), part.at[chip], px_s.at[i], px_r.at[i], mate)

        for i in range(chips):
            px(i).start()

        def gather(i):
            px(i).wait_recv()
            chip = chip_off(order[i])
            part[chip] += slice_of(2 * chip + k)[...]

        few = quarter // 2

        def piece(ref, q):
            return ref.at[q // 2, pl.ds(q % 2 * few, few)]

        def rs(d, t, q, src):
            return remote(src, piece(sums.at[d, t - 1], q), rs_s.at[d, t - 1, q], rs_r.at[d, t - 1, q], nbr[d])

        sent = []

        def hop(t):
            for q in range(4):
                for d in (0, 1):
                    chip = chip_off((hops + 1 - t) * (1 - 2 * d))
                    if t == 1 and q // 2 != d:
                        continue
                    if t == 1 or (t == 2 and q // 2 != d):
                        copy = rs(d, t, q, piece(part.at[chip], q))
                    else:
                        held = piece(sums.at[d, t - 2], q)
                        rs(d, t - 1, q, held).wait_recv()
                        held[...] += piece(part.at[chip], q)[...]
                        copy = rs(d, t, q, held)
                    copy.start()
                    sent.append(copy)

        gather(0)
        hop(1)
        gathered_weights()
        for t in range(spare):
            st[t, pl.ds(0, rows), :] = jnp.zeros((rows, pair), F32)
        dx_start(0)
        dx_pairs(0, 5)
        for i in range(1, chips):
            gather(i)
        hop(2)
        weight_grads(chip_at(chips - 1))
        dx_pairs(5, 6)
        hop(hops - 1)
        dx_pairs(6, 7)
        hop(hops)
        dwo_out = local(dwo_acc, dwo_hbm, 0)
        dwo_out.start()
        dwq_out = []
        for t in range(spare):
            at = pl.ds(t * pair, pair)
            staged = st.at[spare + t, :, pl.ds(0, dim)]
            staged[...] = dwqt[:, at].T
            out = local(staged, dwq_hbm.at[at, :], 6 + t)
            out.start()
            dwq_out.append(out)

        dx_pairs(7, 7)

        def tokens_of(dev):
            chip = lax.div(dev, 2)
            at = pl.ds(pl.multiple_of(lax.rem(dev, 2) * rows, rows), rows)
            return thin.at[lax.div(chip, quarter), lax.rem(chip, quarter), :, at]

        def kv_copy(dev):
            return remote(tokens_of(dev), kv_rows.at[m], kv_s.at[dev], kv_r.at[m], dev)

        def dw_copy(dev):
            return remote(dw_out.at[dev], dw_in.at[m], dw_s.at[dev], dw_r.at[m], dev)

        per = pair // cols

        def key_grads(h):
            def body(t, _):
                at = pl.ds(pl.multiple_of(t * pair, pair), pair)
                add = dot(thin[h, 0], x_all[h * quarter, :, at])
                for j in range(1, quarter):
                    add += dot(thin[h, j], x_all[h * quarter + j, :, at])
                for i in range(per):
                    dev = t * per + i
                    piece = add[:, i * cols : (i + 1) * cols]
                    dw_out[dev] = piece if h == 0 else dw_out[dev] + piece
                if h == 1:
                    for i in range(per):
                        dev = t * per + i

                        @pl.when(dev != m)
                        def _():
                            dw_copy(dev).start()

                return 0

            lax.fori_loop(0, width // pair, body, 0)

        for h in (0, 1):
            total = part[c, h]
            for d in (0, 1):
                for q in (2 * h, 2 * h + 1):
                    rs(d, hops, q, piece(sums.at[d, hops - 1], q)).wait_recv()
                total += sums[d, hops - 1, h]
            thin[h] = total.astype(BF16)

            def send_rows(dev, _):
                @pl.when(dev != m)
                def _():
                    kv_copy(dev).start()

                return 0

            lax.fori_loop(h * n // 2, (h + 1) * n // 2, send_rows, 0)
            key_grads(h)
        kv_rows[m] = tokens_of(m)[...]
        dx_pairs(7, chips)

        def rows_arrived(dev, _):
            @pl.when(dev != m)
            def _():
                kv_copy(dev).wait_send()
                remote(kv_rows.at[dev], kv_rows.at[dev], kv_s.at[dev], kv_r.at[dev], mate).wait_recv()

            return 0

        lax.fori_loop(0, n, rows_arrived, 0)
        own_kv = kv_rows[...].reshape(2 * dim, rows).T
        wait_sends(RY)
        for t in range(spare):
            at = pl.ds(t * pair, pair)
            add = dot_nt(own_kv, wqkv[at, pl.ds(dim, 2 * dim)])
            dy_all[0, pl.ds(0, rows), at] = (st[t, pl.ds(0, rows), :] + add).astype(BF16)
        dx_out = local(dy_all.at[0, pl.ds(0, rows), :], dx_hbm, 4)
        dx_out.start()
        dw_in[m] = dw_out[m]

        def arrived(dev, _):
            @pl.when(dev != m)
            def _():
                dw_copy(dev).wait_send()
                remote(dw_in.at[dev], dw_in.at[dev], dw_s.at[dev], dw_r.at[dev], mate).wait_recv()

            return 0

        lax.fori_loop(0, n, arrived, 0)
        turned = dw_in[...].reshape(2 * dim, cols)
        dw_t[0] = turned[:dim].T
        dw_t[1] = turned[dim:].T
        outs = [local(dw_t.at[0], dwk_hbm, 2), local(dw_t.at[1], dwv_hbm, 3)]
        for out in outs:
            out.start()
        for out in (dwo_out, *dwq_out, dx_out, *outs):
            out.wait()

        for r in (RX, RW):
            wait_sends(r)
        for i in range(1, groups):
            peer(i).wait_send()
        for i in range(chips):
            px(i).wait_send()
        for copy in sent:
            copy.wait_send()

        def sent_dq(h, _):
            @pl.when(h != m)
            def _():
                remote(dq_in.at[h], dq_in.at[h], dq_s.at[h], dq_r.at[h], h).wait_send()

            return 0

        lax.fori_loop(0, n, sent_dq, 0)

    return kernel


def hand_on(*refs):
    count = (len(refs) - 2) // 3
    srcs, dsts, bufs = refs[:count], refs[count : 2 * count], refs[2 * count : 3 * count]
    sems_in, sems_out = refs[3 * count :]
    pieces = []
    for src, dst, buf in zip(srcs, dsts, bufs):
        parts = max(1, src.shape[0] * src.shape[1] // (1 << 17))
        size = src.shape[0] // parts
        for i in range(parts):
            at = pl.ds(i * size, size)
            pieces.append((src.at[at, :], buf.at[at, :], dst.at[at, :]))
    ins = [pltpu.make_async_copy(a, b, sems_in.at[i]) for i, (a, b, _) in enumerate(pieces)]
    outs = [pltpu.make_async_copy(b, c, sems_out.at[i]) for i, (_, b, c) in enumerate(pieces)]
    for copy in ins:
        copy.start()
    for got, put in zip(ins, outs):
        got.wait()
        put.start()
    for put in outs:
        put.wait()


def solution(mesh):
    n = mesh.shape["model"]
    groups = mesh.shape["data"]
    chips = n // 2
    hops = chips // 2
    tok_spec = P(("data", "model"), None)

    def local_step(x_loc, dy_loc, wq_loc, w_key, w_value, wo_loc):
        rows, width = x_loc.shape
        dim = w_key.shape[1]
        cols = width // n
        sds = jax.ShapeDtypeStruct
        vmem = pltpu.VMEM
        dma = pltpu.SemaphoreType.DMA
        arrivals = 2 * hops - 1
        slim = 2 * dim // n
        outs = pl.pallas_call(
            make_kernel(n, groups),
            name="mqa_backward",
            out_shape=(
                sds((rows, width), BF16),
                sds((width, dim), F32),
                sds((cols, dim), F32),
                sds((cols, dim), F32),
                sds((dim, width), F32),
                sds((n, width, dim), BF16),
            ),
            in_specs=[pl.BlockSpec(memory_space=pl.ANY)] * 6,
            out_specs=[pl.BlockSpec(memory_space=pl.ANY)] * 6,
            scratch_shapes=[
                vmem((chips, 2 * rows, width), BF16),
                vmem((chips, 2 * rows, width), BF16),
                vmem((chips, 2 * rows, dim), BF16),
                vmem((2, chips, 2 * rows, dim), BF16),
                vmem((chips, dim, 2 * rows), BF16),
                vmem((chips, dim, 2 * rows), BF16),
                vmem((chips, 2, 8, 2 * rows), F32),
                vmem((width, 3 * dim), BF16),
                vmem((width, dim), BF16),
                vmem((2, 2, hops, dim, 2 * rows), F32),
                vmem((chips, 2, hops, slim, 2 * rows), F32),
                vmem((2, hops, 2, hops, slim, 2 * rows), F32),
                vmem((n, rows, dim), BF16),
                vmem((dim, width), F32),
                vmem((dim, width), F32),
                vmem((chips, 2 * rows, 2 * rows), F32),
                vmem((2, width, 2 * dim), BF16),
                vmem((dim, 2 * rows), F32),
                vmem((dim, 2 * rows), BF16),
                vmem((dim, 2 * rows), BF16),
                vmem((2, hops, slim, 2 * rows), BF16),
                vmem((n, slim, rows), BF16),
                vmem((n, slim, cols), F32),
                vmem((n, slim, cols), F32),
                vmem((2, cols, dim), F32),
                dma((3, 2, arrivals)),
                dma((3, 2, arrivals)),
                dma((3, 2 + 2 * arrivals)),
                dma((3, 2 + 2 * arrivals)),
                dma((n,)),
                dma((n,)),
                dma((chips,)),
                dma((chips,)),
                dma((2, hops, 4)),
                dma((2, hops, 4)),
                dma((n,)),
                dma((n,)),
                dma((n,)),
                dma((n,)),
                dma((groups,)),
                dma((groups,)),
                dma((6 + width // (2 * rows),)),
            ],
            compiler_params=pltpu.CompilerParams(
                collective_id=0, has_side_effects=True, vmem_limit_bytes=67043328
            ),
        )(
            x_loc,
            dy_loc,
            wq_loc.reshape(width, dim),
            w_key,
            w_value,
            wo_loc.reshape(dim, width),
        )
        results = outs[:5]
        any_spec = [pl.BlockSpec(memory_space=pl.ANY)] * 5
        dx, dwq, dwk, dwv, dwo = pl.pallas_call(
            hand_on,
            name="hand_on",
            out_shape=tuple(sds(o.shape, o.dtype) for o in results),
            in_specs=any_spec,
            out_specs=any_spec,
            scratch_shapes=[vmem(o.shape, o.dtype) for o in results] + [dma((64,)), dma((64,))],
        )(*results)
        return dx, dwq.reshape(width, 1, dim), dwk, dwv, dwo.reshape(1, dim, width)

    return jax.shard_map(
        local_step,
        mesh=mesh,
        in_specs=(tok_spec, tok_spec, P(None, "model", None), P(None, None), P(None, None), P("model", None, None)),
        out_specs=(tok_spec, P("data", "model", None), tok_spec, tok_spec, P(("data", "model"), None, None)),
        check_vma=False,
    )
```
